32 devices in a mesh: tm: 8 (over z, core), block: 4 (over y, x).
Axes of the slice: x: 2, y: 2, z: 4, core: 2. Of those that a mesh axis runs over, the one named last changes fastest.
Arguments:
- state: float32 [16, 4, 256, 512], P('tm', None, None, 'block'), may hold values from -6 to 6
- far_field: float32 [16, 4, 512], P('tm', None, 'block'), may hold values from -6 to 6
- face_index: int32 [16, 512], P('tm', 'block'), may hold values from 0 to 255, as said below
- face_weight: float32 [16, 4, 512], P('tm', None, 'block'), may hold values from 0.05 to 0.45
- mean_flow: float32 [2, 2], replicated, may hold values from -0.6 to 0.6
Outputs:
- new_state: float32 [16, 4, 256, 512], P('tm', None, None, 'block')
The draws below stay inside these ranges and needn't reach their ends.
Inputs may be any that keep to these rules, and one draw needn't show every extreme that they name: `face_index`: each face's index points into the opposite row's 2 * 128 interface faces laid end to end; the 4 faces read wrap around that cycle. At each level, the faces of one blade row take distinct first indices, every face of the opposite row exactly once.
All inputs are finite; a program needn't handle non-finite values.
Results may differ from the reference program's by a relative error of at most 0.00016.
Values sent between devices are 32-bit elements; how exact they have to be, the bound alone decides.
A program may use at most 64 MiB of HBM per device.

```python
import jax
import jax.numpy as jnp
from jax import lax

NT = 16
NI = 256
NJ = 128
K = 4
BLOCKS = 4
HALF = 2


def draw_face_index(key, part):
    base = jax.random.fold_in(key, 7)
    cycle_size = HALF * NJ
    level_keys = jax.random.split(base, NT * 2)
    orders = jax.vmap(lambda single: jax.random.permutation(single, cycle_size))(level_keys)
    column = jnp.arange(BLOCKS * NJ)
    block_number = column // NJ
    side = block_number // HALF
    place = block_number % HALF * NJ + column % NJ
    flat = orders.reshape(NT, 2 * cycle_size)
    return jnp.take(flat, side * cycle_size + place, axis=1).astype(jnp.int32)


def block_levels(stream_key, shape, cuts, smallest, top_value):
    level = 1.0
    for axis_at, blocks in cuts:
        draws = jax.random.uniform(jax.random.fold_in(jax.random.fold_in(stream_key, 6), axis_at), (blocks,), jnp.float32, smallest / len(cuts), top_value / len(cuts))
        level = level * jnp.repeat(jnp.exp(draws), shape[axis_at] // blocks).reshape((-1,) + (1,) * (len(shape) - 1 - axis_at))
    return level


def centred(own_key, extent, deviation, limit, cuts=(), held_as=jnp.bfloat16):
    factor_of = block_levels(own_key, extent, cuts, -0.22, 0.18) if cuts else 1.0
    entries = jax.random.normal(own_key, extent, jnp.float32) * deviation * factor_of
    return jnp.minimum(jnp.maximum(entries, -limit), limit).astype(held_as)


def setup_inputs(seed: int = 0) -> dict:
    keys = jax.random.split(jax.random.key(seed), 6)
    state = centred(keys[0], (NT, 4, NI, BLOCKS * NJ), 1.0, 6.0, ((0, 8), (3, 4)), jnp.float32)
    far_field = centred(keys[1], (NT, 4, BLOCKS * NJ), 1.0, 6.0, ((0, 8), (2, 4)), jnp.float32)
    face_index = draw_face_index(jax.random.fold_in(keys[5], 71), 0)
    face_weight = jnp.clip(0.05 + 0.39999999 * jax.random.uniform(keys[3], (NT, K, BLOCKS * NJ), jnp.float32) ** block_levels(keys[3], (NT, K, BLOCKS * NJ), ((0, 8), (2, 4)), -0.2, 0.2), 0.05, 0.45)
    mean_flow = jnp.clip(jax.random.uniform(keys[4], (2, 2), jnp.float32, -0.6, 0.6), -0.6, 0.6)
    return {"state": state, "far_field": far_field, "face_index": face_index, "face_weight": face_weight, "mean_flow": mean_flow}


SECTION_FACTORS = (0.075, 0.05, 0.1125, 0.15, 0.3)
OMEGA = 1.0
DISSIPATION = 0.2


def derivative_matrix(count):
    index = jnp.arange(count)
    offsets = index[:, None] - index[None, :]
    angle = jnp.pi * offsets.astype(jnp.float32) / count
    parity_sign = 1.0 - 2.0 * (offsets % 2).astype(jnp.float32)
    safe_angle = jnp.where(offsets == 0, 0.5 * jnp.pi, angle)
    cotangent = jnp.cos(safe_angle) / jnp.sin(safe_angle)
    return jnp.where(offsets == 0, 0.0, 0.5 * parity_sign * cotangent).astype(jnp.float32)


def interpolate(faces, table, weight):
    cycle_size = faces.shape[2]
    total = jnp.zeros(faces.shape, jnp.float32)
    for offset in range(weight.shape[1]):
        source = ((table + offset) % cycle_size).astype(jnp.int32)
        picked = jnp.take_along_axis(faces, jnp.broadcast_to(source[:, None, :], faces.shape), axis=2)
        total = total + weight[:, offset][:, None, :] * picked
    return total


def residual(field, lower_ghost, upper_ghost, lower_col, upper_col, speed_u, speed_v):
    padded_i = jnp.concatenate([lower_ghost[:, :, None], field, upper_ghost[:, :, None]], axis=2)
    padded_j = jnp.concatenate([lower_col, field, upper_col], axis=3)
    diff_i = padded_i[:, :, 2:] - padded_i[:, :, :-2]
    diff_j = padded_j[..., 2:] - padded_j[..., :-2]
    laplace = (padded_i[:, :, 2:] - 2.0 * field + padded_i[:, :, :-2]) + (padded_j[..., 2:] - 2.0 * field + padded_j[..., :-2])
    flux_i = jnp.stack([speed_u * diff_i[:, 0] + diff_i[:, 1], speed_u * diff_i[:, 1] + diff_i[:, 3],
                        speed_u * diff_i[:, 2], speed_u * diff_i[:, 3] + diff_i[:, 1]], axis=1)
    flux_j = jnp.stack([speed_v * diff_j[:, 0] + diff_j[:, 2], speed_v * diff_j[:, 1],
                        speed_v * diff_j[:, 2] + diff_j[:, 3], speed_v * diff_j[:, 3] + diff_j[:, 2]], axis=1)
    return 0.5 * (flux_i + flux_j) - DISSIPATION * laplace


def reference(state, far_field, face_index, face_weight, mean_flow):
    half = BLOCKS // 2
    spectral = derivative_matrix(NT)
    far_rows = far_field.reshape(NT, 4, 2, half * NJ)
    tables = face_index.reshape(NT, 2, half * NJ)
    weights = face_weight.reshape(NT, K, 2, half * NJ)
    field = state
    for factor in SECTION_FACTORS:
        blocked = field.reshape(NT, 4, NI, 2, half * NJ)
        pieces = []
        for side in (0, 1):
            part = blocked[:, :, :, side]
            other = blocked[:, :, :, 1 - side]
            other_face = other[:, :, 0] if side == 0 else other[:, :, NI - 1]
            ghost = interpolate(other_face, tables[:, side], weights[:, :, side])
            far_side = far_rows[:, :, side]
            if side == 0:
                lower_ghost, upper_ghost = far_side, ghost
            else:
                lower_ghost, upper_ghost = ghost, far_side
            flux = residual(part, lower_ghost, upper_ghost, part[..., -1:], part[..., :1],
                            mean_flow[side, 0], mean_flow[side, 1])
            pieces.append(flux)
        flux_all = jnp.stack(pieces, axis=3).reshape(NT, 4, NI, BLOCKS * NJ)
        deriv = jnp.einsum('nm,mvij->nvij', spectral, field, precision=lax.Precision.HIGHEST)
        field = state - factor * (flux_all + OMEGA * deriv)
    return field
```

```python
import functools
import math

import jax
import jax.numpy as jnp
from jax import lax
from jax.experimental import pallas as pl
from jax.experimental.pallas import tpu as pltpu
from jax.sharding import PartitionSpec as P

SECTION_FACTORS = (0.075, 0.05, 0.1125, 0.15, 0.3)
OMEGA = 1.0
DISSIPATION = 0.2
PAD = 8
MESH = pl.DeviceIdType.MESH


def split_coefficients(count, scale):
    half = count // 2
    d = [0.0] + [0.5 * (-1) ** k / math.tan(math.pi * k / count) for k in range(1, half)] + [0.0]
    even = [0.5 * scale * (d[m] - d[half - m]) for m in range(half)]
    odd = [0.5 * scale * (d[m] + d[half - m]) for m in range(half)]
    even[0] = odd[0] = 0.0
    return even, odd


def time_term(q, even, odd):
    half = len(q) // 2
    quarter = half // 2
    e = [q[n] + q[n + half] for n in range(half)]
    o = [q[n] - q[n + half] for n in range(half)]

    def odd_at(n):
        return (o[n % half], -1.0 if (n // half) % 2 else 1.0)

    low, high = [], []
    for n in range(half):
        ev = None
        od = None
        for m in range(1, quarter):
            term = even[m] * (e[(n - m) % half] - e[(n + m) % half])
            ev = term if ev is None else ev + term
            (a, sa), (b, sb) = odd_at(n - m), odd_at(n + m)
            pair = a - b if sa == sb else a + b
            term = (odd[m] * sa) * pair
            od = term if od is None else od + term
        a, sa = odd_at(n - quarter)
        od = od + (odd[quarter] * sa) * a
        low.append(ev + od)
        high.append(ev - od)
    return low + high


def kernel(dims, state, far, fidx, fw, mf, out, x0, qa, qb, ef, el, rl, ru, cs, cl, cu,
           face, ff, wts, fi, lane_ix, blk_ix, ww, gh,
           in_s, in_r, out_s, out_r, p_s, p_r, h_s, h_r, f_s, f_r, loc):
    tm_n, half, L, R, K = dims
    NT = tm_n * L
    cycle = half * 128
    tiles = R // 8
    nsec = len(SECTION_FACTORS)
    me = lax.axis_index("tm")
    blk = lax.axis_index("block")
    side = lax.div(blk, half)
    place = lax.rem(blk, half)
    row0 = side * half
    lower_b = row0 + lax.rem(place + half - 1, half)
    upper_b = row0 + lax.rem(place + 1, half)
    other0 = (1 - side) * half
    step = 1 - 2 * side
    is_last = me == tm_n - 1
    is_far = me == 0
    rchunk = side * (tm_n - 1) + step * me
    has_lower = rchunk > 0
    has_upper = rchunk < tm_n - 1
    ghost_row = jnp.where(side == 0, PAD + R, PAD - 1)
    far_row = jnp.where(side == 0, PAD - 1, PAD + R)

    def rc(src, dst, ss, rs, dev):
        return pltpu.make_async_remote_copy(src_ref=src, dst_ref=dst, send_sem=ss, recv_sem=rs,
                                            device_id=dev, device_id_type=MESH)

    def rows(p):
        return pl.ds(pl.multiple_of((side * (tm_n - 1) + step * p) * R, R), R)

    def lev(p):
        return pl.ds(p * L, L)

    def peer(t):
        return lax.rem(me + 1 + t, tm_n)

    bar = pltpu.get_barrier_semaphore()

    @pl.loop(0, tm_n - 1)
    def _(t):
        pl.semaphore_signal(bar, inc=1, device_id={"tm": peer(t)}, device_id_type=MESH)

    pl.semaphore_signal(bar, inc=1, device_id={"block": lower_b}, device_id_type=MESH)
    pl.semaphore_signal(bar, inc=1, device_id={"block": upper_b}, device_id_type=MESH)

    @pl.when(is_last)
    def _():
        for h in range(half):
            pl.semaphore_signal(bar, inc=1, device_id={"block": other0 + h}, device_id_type=MESH)

    own = pltpu.make_async_copy(state.at[:, :, rows(me)], x0.at[lev(me)], loc.at[0])
    own.start()
    pl.semaphore_wait(bar, tm_n + 1 + jnp.where(is_last, half, 0))

    def in_copy(p, src_tm):
        return rc(state.at[:, :, rows(p)], x0.at[lev(src_tm)], in_s.at[p], in_r.at[src_tm], {"tm": p})

    @pl.loop(0, tm_n - 1)
    def _(t):
        p = peer(t)
        in_copy(p, me).start()

    def far_copy(src_tm):
        return rc(far, ff.at[lev(src_tm)], p_s.at[0], p_r.at[0, src_tm], {"tm": 0})

    def wt_copy(src_tm):
        return rc(fw, wts.at[lev(src_tm)], p_s.at[1], p_r.at[1, src_tm], {"tm": tm_n - 1})

    def ix_copy(src_tm):
        return rc(fidx, fi.at[src_tm], p_s.at[2], p_r.at[2, src_tm], {"tm": tm_n - 1})

    own_far = pltpu.make_async_copy(far, ff.at[lev(me)], loc.at[1])
    own_wt = pltpu.make_async_copy(fw, wts.at[lev(me)], loc.at[2])
    own_ix = pltpu.make_async_copy(fidx, fi.at[me], loc.at[3])

    @pl.when(is_far)
    def _():
        own_far.start()

    @pl.when(jnp.logical_not(is_far))
    def _():
        far_copy(me).start()

    @pl.when(is_last)
    def _():
        own_wt.start()
        own_ix.start()

    @pl.when(jnp.logical_not(is_last))
    def _():
        wt_copy(me).start()
        ix_copy(me).start()

    lane = lax.broadcasted_iota(jnp.int32, (8, 128), 1)
    lane_pair = jnp.bitwise_or(lane, 1)
    sub = lax.broadcasted_iota(jnp.int32, (8, 128), 0)

    def pack(acc, value, k):
        return jnp.where(lane_pair == k, pltpu.roll(value, k, 1), acc)

    def key(l, v):
        return 2 * (4 * l + v) + 1

    def halo_copies(s):
        low = rc(ef.at[s], ru.at[s], h_s.at[s, 0], h_r.at[s, 0], {"tm": me - step})
        up = rc(el.at[s], rl.at[s], h_s.at[s, 1], h_r.at[s, 1], {"tm": me + step})
        jl = rc(cs.at[s], cu.at[s], h_s.at[s, 2], h_r.at[s, 2], {"block": lower_b})
        ju = rc(cs.at[s], cl.at[s], h_s.at[s, 3], h_r.at[s, 3], {"block": upper_b})
        return low, up, jl, ju

    def face_copy(s, h, edge):
        return rc(edge.at[s], face.at[s, place], f_s.at[s, h], f_r.at[s, place], {"block": other0 + h})

    def face_wait(s, h):
        return rc(ef.at[s], face.at[s, h], f_s.at[s, h], f_r.at[s, h], {"block": other0 + h})

    def send_halos(s):
        low, up, jl, ju = halo_copies(s)

        @pl.when(is_last & (side == 0))
        def _():
            for h in range(half):
                face_copy(s, h, el).start()

        @pl.when(is_last & (side == 1))
        def _():
            for h in range(half):
                face_copy(s, h, ef).start()

        @pl.when(has_lower)
        def _():
            low.start()

        @pl.when(has_upper)
        def _():
            up.start()

        jl.start()
        ju.start()

    def take_level(l, accs):
        accs = list(accs)
        for v in range(4):
            for a in range(tiles):
                value = x0[l, v, pl.ds(8 * a, 8)]
                qa[l, v, pl.ds(PAD + 8 * a, 8)] = value
                accs[a] = pack(accs[a], value, key(l, v))
                if a == 0:
                    ef[0, pl.ds(4 * l + v, 1)] = value[0:1]
                if a == tiles - 1:
                    el[0, pl.ds(4 * l + v, 1)] = value[7:8]
        return tuple(accs)

    own.wait()
    accs = tuple(jnp.zeros((8, 128), jnp.float32) for _ in range(tiles))
    accs = lax.fori_loop(0, L, lambda j, c: take_level(me * L + j, c), accs)

    def arrive(t, c):
        p = peer(tm_n - 2 - t)
        in_copy(p, p).wait_recv()
        return lax.fori_loop(0, L, lambda j, d: take_level(p * L + j, d), c)

    accs = lax.fori_loop(0, tm_n - 1, arrive, accs)
    for a in range(tiles):
        cs[0, pl.ds(8 * a, 8)] = accs[a]
    send_halos(0)

    @pl.when(is_far)
    def _():
        own_far.wait()

        @pl.loop(1, tm_n)
        def _(p):
            far_copy(p).wait_recv()

        @pl.loop(0, NT)
        def _(l):
            for v in range(4):
                row = ff[l, pl.ds(v, 1)]
                qa[l, v, pl.ds(far_row, 1)] = row
                qb[l, v, pl.ds(far_row, 1)] = row

    @pl.when(is_last)
    def _():
        own_wt.wait()
        own_ix.wait()

        @pl.loop(0, tm_n - 1)
        def _(p):
            wt_copy(p).wait_recv()
            ix_copy(p).wait_recv()

        @pl.loop(0, NT // 2)
        def _(m):
            def ix(l):
                return jnp.broadcast_to(fi[lax.div(l, L), pl.ds(lax.rem(l, L), 1)], (8, 128))

            def wt(l, k):
                return jnp.broadcast_to(wts[l, pl.ds(k, 1)], (8, 128))

            start = jnp.where(sub < 4, ix(2 * m), ix(2 * m + 1))
            at = pl.ds(8 * m, 8)
            for k in range(K):
                src = start + k
                src = jnp.where(src >= cycle, src - cycle, src)
                lane_ix[k, at] = jnp.bitwise_and(src, 127)
                blk_ix[k, at] = lax.shift_right_logical(src, 7)
                ww[k, at] = jnp.where(sub < 4, wt(2 * m, k), wt(2 * m + 1, k))

    speed_u = jnp.where(side == 0, mf[0, 0], mf[1, 0])
    speed_v = jnp.where(side == 0, mf[0, 1], mf[1, 1])
    odd_lane = jnp.bitwise_and(lane, 1) == 1
    edge_lane = {0: lane == 0, 127: lane == 127}

    def install(dst, src, at):
        @pl.loop(0, NT)
        def _(l):
            for v in range(4):
                dst[l, v, pl.ds(at, 1)] = src[pl.ds(4 * l + v, 1)]

    def out_copy(q, p, src_tm):
        return rc(q.at[lev(p), :, pl.ds(PAD, R)], out.at[:, :, rows(src_tm)],
                  out_s.at[p], out_r.at[src_tm], {"tm": p})

    for s, factor in enumerate(SECTION_FACTORS):
        q, nq = (qa, qb) if s % 2 == 0 else (qb, qa)
        final = s == nsec - 1
        even, odd = split_coefficients(NT, OMEGA * factor)
        hu, hv, hh = (0.5 * factor) * speed_u, (0.5 * factor) * speed_v, 0.5 * factor

        @pl.loop(0, 4)
        def _(v):
            @pl.loop(0, tiles)
            def _(a):
                at = pl.ds(pl.multiple_of(PAD + 8 * a, 8), 8)
                xs = [q[l, v, at] for l in range(NT)]
                terms = time_term(xs, even, odd)
                for l in range(NT):
                    first = x0[l, v, pl.ds(pl.multiple_of(8 * a, 8), 8)]
                    nq[l, v, at] = first - (terms[l] + (4.0 * DISSIPATION * factor) * xs[l])

        low, up, jl, ju = halo_copies(s)
        jl.wait_recv()
        ju.wait_recv()
        mixed = []
        for a in range(tiles):
            at = pl.ds(8 * a, 8)
            mixed.append(jnp.where(odd_lane, pltpu.roll(cl[s, at], 1, 1), pltpu.roll(cu[s, at], 127, 1)))

        def level(l, accs, which):
            accs = list(accs)
            for slot, a in enumerate(which):
                base = PAD + 8 * a
                di, dj, near = [], [], []
                for v in range(4):
                    x = q[l, v, pl.ds(base, 8)]
                    upx = q[l, v, pl.ds(base + 1, 8)]
                    dnx = q[l, v, pl.ds(base - 1, 8)]
                    border = pltpu.roll(mixed[a], 128 - key(l, v), 1)
                    left = jnp.where(edge_lane[0], border, pltpu.roll(x, 1, 1))
                    right = jnp.where(edge_lane[127], border, pltpu.roll(x, 127, 1))
                    di.append(upx - dnx)
                    dj.append(right - left)
                    near.append((DISSIPATION * factor) * ((upx + dnx) + (right + left)))
                flux = [
                    hu * di[0] + hv * dj[0] + hh * (di[1] + dj[2]),
                    hu * di[1] + hv * dj[1] + hh * di[3],
                    hu * di[2] + hv * dj[2] + hh * dj[3],
                    hu * di[3] + hv * dj[3] + hh * (di[1] + dj[2]),
                ]
                for v in range(4):
                    new = nq[l, v, pl.ds(base, 8)] + (near[v] - flux[v])
                    nq[l, v, pl.ds(base, 8)] = new
                    if not final:
                        accs[slot] = pack(accs[slot], new, key(l, v))
                        if a == 0:
                            ef[s + 1, pl.ds(4 * l + v, 1)] = new[0:1]
                        if a == tiles - 1:
                            el[s + 1, pl.ds(4 * l + v, 1)] = new[7:8]
            return tuple(accs)

        def sweep(which):
            zero = tuple(jnp.zeros((8, 128), jnp.float32) for _ in which)
            step_by = 4 if NT % 4 == 0 else 1

            def several(g, c):
                for j in range(step_by):
                    c = level(step_by * g + j, c, which)
                return c

            accs = lax.fori_loop(0, NT // step_by, several, zero)
            if not final:
                for slot, a in enumerate(which):
                    cs[s + 1, pl.ds(8 * a, 8)] = accs[slot]

        inner = tuple(range(1, tiles - 1))
        outer = tuple(sorted({0, tiles - 1}))
        if inner:
            sweep(inner)

        @pl.when(has_lower)
        def _():
            up.wait_recv()
            install(q, rl.at[s], PAD - 1)

        @pl.when(has_upper)
        def _():
            low.wait_recv()
            install(q, ru.at[s], PAD + R)

        @pl.when(is_last)
        def _():
            for h in range(half):
                face_wait(s, h).wait_recv()

            @pl.loop(0, NT // 2)
            def _(m):
                at = pl.ds(8 * m, 8)
                total = jnp.zeros((8, 128), jnp.float32)
                for k in range(K):
                    picked = jnp.zeros((8, 128), jnp.float32)
                    for h in range(half):
                        got = jnp.take_along_axis(face[s, h, at], lane_ix[k, at], axis=1)
                        picked = jnp.where(blk_ix[k, at] == h, got, picked)
                    total = total + ww[k, at] * picked
                gh[at] = total

            install(q, gh, ghost_row)

        if not final:
            sweep(outer)
            send_halos(s + 1)
        else:
            def finish(t, c):
                p = peer(t)
                for j in range(L):
                    level(p * L + j, (None,) * len(outer), outer)

                @pl.when(t < tm_n - 1)
                def _():
                    out_copy(nq, p, me).start()

                return c

            lax.fori_loop(0, tm_n, finish, 0)
            own_out = pltpu.make_async_copy(nq.at[lev(me), :, pl.ds(PAD, R)], out.at[:, :, rows(me)], loc.at[4])
            own_out.start()

            @pl.loop(0, tm_n - 1)
            def _(t):
                p = peer(t)
                out_copy(nq, p, p).wait_recv()

            own_out.wait()

            @pl.loop(0, tm_n - 1)
            def _(t):
                p = peer(t)
                out_copy(nq, p, me).wait_send()

    @pl.loop(0, tm_n - 1)
    def _(t):
        p = peer(t)
        in_copy(p, me).wait_send()

    @pl.when(jnp.logical_not(is_far))
    def _():
        far_copy(me).wait_send()

    @pl.when(jnp.logical_not(is_last))
    def _():
        wt_copy(me).wait_send()
        ix_copy(me).wait_send()

    for s in range(nsec):
        low, up, jl, ju = halo_copies(s)

        @pl.when(has_lower)
        def _():
            low.wait_send()

        @pl.when(has_upper)
        def _():
            up.wait_send()

        jl.wait_send()
        ju.wait_send()

        @pl.when(is_last)
        def _():
            for h in range(half):
                face_wait(s, h).wait_send()


def shards(dims, state, far_field, face_index, face_weight, mean_flow):
    tm_n, half = dims
    L, _, rows, width = state.shape
    K = face_weight.shape[1]
    R = rows // tm_n
    NT = L * tm_n
    assert width == 128 and NT % 4 == 0 and R % 8 == 0 and 8 * NT <= width
    n = len(SECTION_FACTORS)
    f32 = jnp.float32
    hbm = pl.BlockSpec(memory_space=pl.ANY)
    dma = pltpu.SemaphoreType.DMA
    V = pltpu.VMEM
    return pl.pallas_call(
        functools.partial(kernel, (tm_n, half, L, R, K)),
        out_shape=jax.ShapeDtypeStruct(state.shape, f32),
        in_specs=[hbm, hbm, hbm, hbm, pl.BlockSpec(memory_space=pltpu.SMEM)],
        out_specs=hbm,
        scratch_shapes=[
            V((NT, 4, R, width), f32),
            V((NT, 4, R + 2 * PAD, width), f32),
            V((NT, 4, R + 2 * PAD, width), f32),
            V((n, 4 * NT, width), f32),
            V((n, 4 * NT, width), f32),
            V((n, 4 * NT, width), f32),
            V((n, 4 * NT, width), f32),
            V((n, R, width), f32),
            V((n, R, width), f32),
            V((n, R, width), f32),
            V((n, half, 4 * NT, width), f32),
            V((NT, 4, width), f32),
            V((NT, K, width), f32),
            V((tm_n, L, width), jnp.int32),
            V((K, 4 * NT, width), jnp.int32),
            V((K, 4 * NT, width), jnp.int32),
            V((K, 4 * NT, width), f32),
            V((4 * NT, width), f32),
            dma((tm_n,)), dma((tm_n,)), dma((tm_n,)), dma((tm_n,)),
            dma((3,)), dma((3, tm_n)),
            dma((n, 4)), dma((n, 4)),
            dma((n, half)), dma((n, half)),
            dma((5,)),
        ],
        compiler_params=pltpu.CompilerParams(
            collective_id=0, has_side_effects=True, vmem_limit_bytes=40 * 1024 * 1024),
    )(state, far_field, face_index, face_weight, mean_flow)


def skew_part(o, coef):
    half = len(o)
    quarter = half // 2

    def at(n):
        return o[n % half], -1.0 if (n // half) % 2 else 1.0

    res = []
    for n in range(half):
        total = None
        for m in range(1, quarter):
            (a, sa), (b, sb) = at(n - m), at(n + m)
            term = (coef[m] * sa) * (a - b if sa == sb else a + b)
            total = term if total is None else total + term
        a, sa = at(n - quarter)
        term = (coef[quarter] * sa) * a
        res.append(term if total is None else total + term)
    return res


def cyclic_part(e, coef):
    half = len(e)
    res = []
    for n in range(half):
        total = None
        for m in range(1, half // 2):
            term = coef[m] * (e[(n - m) % half] - e[(n + m) % half])
            total = term if total is None else total + term
        res.append(total)
    return res


def time_term_split(q, even, odd):
    half = len(q) // 2
    quarter = half // 2
    e = [q[n] + q[n + half] for n in range(half)]
    o = [q[n] - q[n + half] for n in range(half)]
    ee = [e[n] + e[n + quarter] for n in range(quarter)]
    eo = [e[n] - e[n + quarter] for n in range(quarter)]
    low = [0.0] + [0.5 * (even[m] - even[quarter - m]) for m in range(1, quarter)]
    high = [0.0] + [0.5 * (even[m] + even[quarter - m]) for m in range(1, quarter)]
    cyc = cyclic_part(ee, low)
    skw = skew_part(eo, high)
    ev = [cyc[n] + skw[n] for n in range(quarter)] + [cyc[n] - skw[n] for n in range(quarter)]
    od = skew_part(o, odd)
    return [ev[n] + od[n] for n in range(half)] + [ev[n] - od[n] for n in range(half)]


def ring_kernel(dims, state, far, fidx, fw, mf, out, q, tt, ff, wts, fi, lane_ix, blk_ix, ww, gg, fo, fg, mfs,
                in_s, in_r, out_s, out_r, p_s, p_r, h_s, h_r, f_s, f_r, loc):
    tm_n, half, L, R, K = dims
    NT = tm_n * L
    G = tm_n * half
    cycle = half * 128
    nsec = len(SECTION_FACTORS)
    groups = 4 * NT // 8
    me = lax.axis_index("tm")
    blk = lax.axis_index("block")
    side = lax.div(blk, half)
    place = lax.rem(blk, half)
    row0 = side * half

    def slab(t, b):
        return b * tm_n + jnp.where(lax.rem(b, 2) == 0, t, tm_n - 1 - t)

    def owner(g):
        b = lax.div(g, tm_n)
        t = lax.rem(g, tm_n)
        return jnp.where(lax.rem(b, 2) == 0, t, tm_n - 1 - t), b

    g = slab(me, place)
    seam = g == G - 1
    prev_t, prev_b = owner(lax.rem(g + G - 1, G))
    prev_dev = {"tm": prev_t, "block": row0 + prev_b}
    seam_dev = {"tm": 0, "block": row0 + half - 1}
    other_dev = {"block": (1 - side) * half + place}
    here = me * half + place

    def peer(t):
        return lax.rem(here + 1 + t, G)

    def dev(j):
        return {"tm": lax.div(j, half), "block": row0 + lax.rem(j, half)}

    def rows(j):
        return pl.multiple_of(slab(lax.div(j, half), lax.rem(j, half)) * R, R)

    def lev(t):
        return pl.ds(t * L, L)

    def rc(src, dst, ss, rs, to):
        return pltpu.make_async_remote_copy(src_ref=src, dst_ref=dst, send_sem=ss, recv_sem=rs,
                                            device_id=to, device_id_type=MESH)

    bar = pltpu.get_barrier_semaphore()

    @pl.loop(0, G - 1)
    def _(t):
        pl.semaphore_signal(bar, inc=1, device_id=dev(peer(t)), device_id_type=MESH)

    @pl.when(seam)
    def _():
        pl.semaphore_signal(bar, inc=1, device_id=other_dev, device_id_type=MESH)

    own = pltpu.make_async_copy(state.at[:, :, pl.ds(rows(here), R)], q.at[0, place, lev(me), :, pl.ds(0, R)], loc.at[0])
    own.start()
    own_mf = pltpu.make_async_copy(mf, mfs, loc.at[4])
    own_mf.start()
    pl.semaphore_wait(bar, G - 1 + jnp.where(seam, 1, 0))

    def far_copy(j):
        return rc(far, ff.at[lax.rem(j, half), lev(lax.div(j, half))], p_s.at[0], p_r.at[0, j], seam_dev)

    def wt_copy(j):
        return rc(fw, wts.at[lax.rem(j, half), lev(lax.div(j, half))], p_s.at[1], p_r.at[1, j], seam_dev)

    def ix_copy(j):
        return rc(fidx, fi.at[lax.rem(j, half), lax.div(j, half)], p_s.at[2], p_r.at[2, j], seam_dev)

    own_far = pltpu.make_async_copy(far, ff.at[place, lev(me)], loc.at[1])
    own_wt = pltpu.make_async_copy(fw, wts.at[place, lev(me)], loc.at[2])
    own_ix = pltpu.make_async_copy(fidx, fi.at[place, me], loc.at[3])

    @pl.when(seam)
    def _():
        own_far.start()
        own_wt.start()
        own_ix.start()

    @pl.when(jnp.logical_not(seam))
    def _():
        far_copy(here).start()
        wt_copy(here).start()
        ix_copy(here).start()

    def in_copy(j, src):
        return rc(state.at[:, :, pl.ds(rows(j), R)],
                  q.at[0, lax.rem(src, half), lev(lax.div(src, half)), :, pl.ds(0, R)],
                  in_s.at[j], in_r.at[src], dev(j))

    @pl.loop(0, G - 1)
    def _(t):
        in_copy(peer(t), here).start()

    lane = lax.broadcasted_iota(jnp.int32, (8, 128), 1)
    sub = lax.broadcasted_iota(jnp.int32, (8, 128), 0)
    first_lane, last_lane = lane == 0, lane == 127

    @pl.when(seam)
    def _():
        own_far.wait()
        own_wt.wait()
        own_ix.wait()

        @pl.loop(0, G - 1)
        def _(t):
            j = peer(t)
            far_copy(j).wait_recv()
            wt_copy(j).wait_recv()
            ix_copy(j).wait_recv()

        for b in range(half):
            @pl.loop(0, NT)
            def _(l):
                for v in range(4):
                    gg[1, b, pl.ds(4 * l + v, 1)] = ff[b, l, pl.ds(v, 1)]

            @pl.loop(0, NT // 2)
            def _(m):
                def ix(l):
                    return jnp.broadcast_to(fi[b, lax.div(l, L), pl.ds(lax.rem(l, L), 1)], (8, 128))

                def wt(l, k):
                    return jnp.broadcast_to(wts[b, l, pl.ds(k, 1)], (8, 128))

                start = jnp.where(sub < 4, ix(2 * m), ix(2 * m + 1))
                at = pl.ds(8 * m, 8)
                for k in range(K):
                    src = start + k
                    src = jnp.where(src >= cycle, src - cycle, src)
                    lane_ix[k, b, at] = jnp.bitwise_and(src, 127)
                    blk_ix[k, b, at] = lax.shift_right_logical(src, 7)
                    ww[k, b, at] = jnp.where(sub < 4, wt(2 * m, k), wt(2 * m + 1, k))

    own_mf.wait()
    speed_u = jnp.where(side == 0, mfs[0, 0], mfs[1, 0])
    speed_v = jnp.where(side == 0, mfs[0, 1], mfs[1, 1])

    def trail(i):
        s, lo, n = ([(0, 0, 2), (0, 2, 3)] + [(s, s, 2) for s in range(1, nsec)])[i]
        return rc(q.at[s, :, :, :, pl.ds(lo, n)], q.at[s, :, :, :, pl.ds(R + lo, n)], h_s.at[i], h_r.at[i], prev_dev)

    def face_copy(s):
        return rc(fo.at[side, s], fg.at[s], f_s.at[s], f_r.at[s], other_dev)

    def time_pass(s, w):
        c = SECTION_FACTORS[s - 1]
        even, odd = split_coefficients(NT, -OMEGA * c)
        at = pl.ds(w, 8)

        @pl.loop(0, 4)
        def _(v):
            for b in range(half):
                xs = [q[s - 1, b, l, v, at] for l in range(NT)]
                terms = time_term_split(xs, even, odd)
                for l in range(NT):
                    tt[b, l, v] = (q[0, b, l, v, at] + terms[l]) - (4.0 * DISSIPATION * c) * xs[l]

    def space_pass(s, w, lo, hi, ghosts):
        c = SECTION_FACTORS[s - 1]
        hh = 0.5 * c
        hu, hv = hh * speed_u, hh * speed_v
        near = DISSIPATION * c
        cu, cd, cr, cl = near - hu, near + hu, near - hv, near + hv
        span = range(half)
        if ghosts:
            up_at = sub == jnp.where(seam, R - 1 - w, 8)
            dn_at = sub == jnp.where(seam, R - w, 8)

        def level(l):
            di, dj, acc = [[], []], [[], []], [[], []]
            di = [[None] * half for _ in range(4)]
            dj = [[None] * half for _ in range(4)]
            acc = [[None] * half for _ in range(4)]
            for v in range(4):
                x = [q[s - 1, b, l, v, pl.ds(w, 8)] for b in span]
                rr = [pltpu.roll(x[b], 127, 1) for b in span]
                rl = [pltpu.roll(x[b], 1, 1) for b in span]
                for b in span:
                    up = q[s - 1, b, l, v, pl.ds(w + 1, 8)]
                    dn = q[s - 1, b, l, v, pl.ds(w - 1, 8)]
                    if ghosts:
                        at = pl.ds(4 * l + v, 1)
                        up = jnp.where(up_at, jnp.broadcast_to(gg[side, b, at], (8, 128)), up)
                        dn = jnp.where(dn_at, jnp.broadcast_to(gg[1 - side, b, at], (8, 128)), dn)
                    right = jnp.where(last_lane, rr[(b + 1) % half], rr[b])
                    left = jnp.where(first_lane, rl[(b - 1) % half], rl[b])
                    acc[v][b] = (tt[b, l, v] + (cu * up + cd * dn)) + (cr * right + cl * left)
                    if v in (1, 3):
                        di[v][b] = up - dn
                    if v in (2, 3):
                        dj[v][b] = right - left
            for b in span:
                cross = hh * (di[1][b] + dj[2][b])
                new = [acc[0][b] - cross, acc[1][b] - hh * di[3][b], acc[2][b] - hh * dj[3][b], acc[3][b] - cross]
                for v in range(4):
                    q[s, b, l, v, pl.ds(w + lo, hi - lo)] = new[v][lo:hi]
                    if ghosts and s < nsec:
                        for k in range(2):
                            row = R - 1 + k - w
                            fo[k, s, b, pl.ds(4 * l + v, 1)] = new[v][row:row + 1]

        @pl.loop(0, NT // 2)
        def _(i):
            for j in range(2):
                level(2 * i + j)

    own.wait()

    @pl.loop(0, G - 1)
    def _(t):
        j = peer(G - 2 - t)
        in_copy(j, j).wait_recv()

    trail(0).start()
    trail(1).start()

    def rise(s):
        if 2 * s + 8 < R:
            windows = [(s, 0, 8), (R - 8 - s, 0, 8)]
        else:
            w = (R - 8) // 2
            windows = [(w, s - w, R - s - w)]
        for w, lo, hi in windows:
            time_pass(s, w)
            space_pass(s, w, lo, hi, False)

    def fall(s):
        if s < nsec:
            windows = [(R - 8 + s, 8 - 2 * s, 8)]
        else:
            windows = [(R - s, 0, 8), (R + s - 8, 16 - 2 * s, 8)]
        for w, lo, hi in windows:
            time_pass(s, w)
            space_pass(s, w, lo, hi, True)

    def out_copy(i, j, src):
        lo, n = [(nsec, R - 2 * nsec), (R - nsec, nsec), (R, nsec)][i]
        g_src = slab(lax.div(src, half), lax.rem(src, half))
        to = g_src * R + lo if i < 2 else lax.rem(g_src + 1, G) * R
        return rc(q.at[nsec, lax.rem(j, half), lev(lax.div(j, half)), :, pl.ds(lo, n)],
                  out.at[:, :, pl.ds(to, n)], out_s.at[i, j], out_r.at[i, src], dev(j))

    def own_out(i):
        lo, n = [(nsec, R - 2 * nsec), (R - nsec, nsec), (R, nsec)][i]
        to = g * R + lo if i < 2 else lax.rem(g + 1, G) * R
        return pltpu.make_async_copy(q.at[nsec, place, lev(me), :, pl.ds(lo, n)], out.at[:, :, pl.ds(to, n)], loc.at[5 + i])

    def send_out(i):
        @pl.loop(0, G - 1)
        def _(t):
            out_copy(i, peer(t), here).start()

        own_out(i).start()

    for s in range(1, nsec + 1):
        rise(s)
        if s < nsec:
            trail(s + 1).start()
        if s == 3:
            trail(0).wait_recv()

            @pl.when(seam)
            def _():
                @pl.loop(0, NT)
                def _(l):
                    for b in range(half):
                        for v in range(4):
                            for k in range(2):
                                fo[k, 0, b, pl.ds(4 * l + v, 1)] = q[0, b, l, v, pl.ds(R - 1 + k, 1)]

                face_copy(0).start()
    send_out(0)

    for s in range(1, nsec + 1):
        if s > 1:
            trail(s).wait_recv()
        if s == 2:
            trail(1).wait_recv()

        @pl.when(seam)
        def _():
            face_copy(s - 1).wait_recv()

            @pl.loop(0, groups)
            def _(m):
                at = pl.ds(8 * m, 8)
                for b in range(half):
                    total = jnp.zeros((8, 128), jnp.float32)
                    for k in range(K):
                        picked = jnp.zeros((8, 128), jnp.float32)
                        for h in range(half):
                            got = jnp.take_along_axis(fg[s - 1, h, at], lane_ix[k, b, at], axis=1)
                            picked = jnp.where(blk_ix[k, b, at] == h, got, picked)
                        total = total + ww[k, b, at] * picked
                    gg[0, b, at] = total

        fall(s)
        if s < nsec:
            @pl.when(seam)
            def _():
                face_copy(s).start()
    send_out(1)
    send_out(2)

    for i in range(3):
        @pl.loop(0, G - 1)
        def _(t):
            j = peer(t)
            out_copy(i, j, j).wait_recv()

        own_out(i).wait()

    @pl.loop(0, G - 1)
    def _(t):
        j = peer(t)
        in_copy(j, here).wait_send()
        for i in range(3):
            out_copy(i, j, here).wait_send()

    for i in range(nsec + 1):
        trail(i).wait_send()

    @pl.when(jnp.logical_not(seam))
    def _():
        far_copy(here).wait_send()
        wt_copy(here).wait_send()
        ix_copy(here).wait_send()

    @pl.when(seam)
    def _():
        for s in range(nsec):
            face_copy(s).wait_send()


def ring_shards(dims, state, far_field, face_index, face_weight, mean_flow):
    tm_n, half = dims
    L, _, rows, width = state.shape
    K = face_weight.shape[1]
    G = tm_n * half
    R = rows // G
    NT = L * tm_n
    n = len(SECTION_FACTORS)
    f32 = jnp.float32
    hbm = pl.BlockSpec(memory_space=pl.ANY)
    dma = pltpu.SemaphoreType.DMA
    V = pltpu.VMEM
    args = [pltpu.with_memory_space_constraint(a, pltpu.HBM)
            for a in (state, far_field, face_index, face_weight, mean_flow)]
    return pl.pallas_call(
        functools.partial(ring_kernel, (tm_n, half, L, R, K)),
        out_shape=jax.ShapeDtypeStruct(state.shape, f32),
        in_specs=[hbm] * 5,
        out_specs=hbm,
        scratch_shapes=[
            V((n + 1, half, NT, 4, R + 8, width), f32),
            V((half, NT, 4, 8, width), f32),
            V((half, NT, 4, width), f32),
            V((half, NT, K, width), f32),
            V((half, tm_n, L, width), jnp.int32),
            V((K, half, 4 * NT, width), jnp.int32),
            V((K, half, 4 * NT, width), jnp.int32),
            V((K, half, 4 * NT, width), f32),
            V((2, half, 4 * NT, width), f32),
            V((2, n, half, 4 * NT, width), f32),
            V((n, half, 4 * NT, width), f32),
            pltpu.SMEM((2, 2), f32),
            dma((G,)), dma((G,)), dma((3, G)), dma((3, G)),
            dma((3,)), dma((3, G)),
            dma((n + 1,)), dma((n + 1,)),
            dma((n,)), dma((n,)),
            dma((8,)),
        ],
        compiler_params=pltpu.CompilerParams(
            collective_id=0, has_side_effects=True, vmem_limit_bytes=48 * 1024 * 1024),
    )(*args)


def solution(mesh):
    dims = (mesh.shape["tm"], mesh.shape["block"] // 2)
    in_specs = (
        P("tm", None, None, "block"),
        P("tm", None, "block"),
        P("tm", "block"),
        P("tm", None, "block"),
        P(),
    )
    out_specs = P("tm", None, None, "block")

    def body(state, *rest):
        ring = dims[0] * dims[1]
        levels = state.shape[0] * dims[0]
        fits = state.shape[2] == 16 * ring and state.shape[3] == 128 and dims[1] % 2 == 0 and levels % 8 == 0
        return (ring_shards if fits else shards)(dims, state, *rest)

    return jax.shard_map(body, mesh=mesh, in_specs=in_specs, out_specs=out_specs, check_vma=False)
```

```python
import functools
import math

import jax
import jax.numpy as jnp
from jax import lax
from jax.experimental import pallas as pl
from jax.experimental.pallas import tpu as pltpu
from jax.sharding import PartitionSpec as P

SECTION_FACTORS = (0.075, 0.05, 0.1125, 0.15, 0.3)
OMEGA = 1.0
DISSIPATION = 0.2
PAD = 8
MESH = pl.DeviceIdType.MESH


def split_coefficients(count, scale):
    half = count // 2
    d = [0.0] + [0.5 * (-1) ** k / math.tan(math.pi * k / count) for k in range(1, half)] + [0.0]
    even = [0.5 * scale * (d[m] - d[half - m]) for m in range(half)]
    odd = [0.5 * scale * (d[m] + d[half - m]) for m in range(half)]
    even[0] = odd[0] = 0.0
    return even, odd


def time_term(q, even, odd):
    half = len(q) // 2
    quarter = half // 2
    e = [q[n] + q[n + half] for n in range(half)]
    o = [q[n] - q[n + half] for n in range(half)]

    def odd_at(n):
        return (o[n % half], -1.0 if (n // half) % 2 else 1.0)

    low, high = [], []
    for n in range(half):
        ev = None
        od = None
        for m in range(1, quarter):
            term = even[m] * (e[(n - m) % half] - e[(n + m) % half])
            ev = term if ev is None else ev + term
            (a, sa), (b, sb) = odd_at(n - m), odd_at(n + m)
            pair = a - b if sa == sb else a + b
            term = (odd[m] * sa) * pair
            od = term if od is None else od + term
        a, sa = odd_at(n - quarter)
        od = od + (odd[quarter] * sa) * a
        low.append(ev + od)
        high.append(ev - od)
    return low + high


def kernel(dims, state, far, fidx, fw, mf, out, x0, qa, qb, ef, el, rl, ru, cs, cl, cu,
           face, ff, wts, fi, lane_ix, blk_ix, ww, gh,
           in_s, in_r, out_s, out_r, p_s, p_r, h_s, h_r, f_s, f_r, loc):
    tm_n, half, L, R, K = dims
    NT = tm_n * L
    cycle = half * 128
    tiles = R // 8
    nsec = len(SECTION_FACTORS)
    me = lax.axis_index("tm")
    blk = lax.axis_index("block")
    side = lax.div(blk, half)
    place = lax.rem(blk, half)
    row0 = side * half
    lower_b = row0 + lax.rem(place + half - 1, half)
    upper_b = row0 + lax.rem(place + 1, half)
    other0 = (1 - side) * half
    step = 1 - 2 * side
    is_last = me == tm_n - 1
    is_far = me == 0
    rchunk = side * (tm_n - 1) + step * me
    has_lower = rchunk > 0
    has_upper = rchunk < tm_n - 1
    ghost_row = jnp.where(side == 0, PAD + R, PAD - 1)
    far_row = jnp.where(side == 0, PAD - 1, PAD + R)

    def rc(src, dst, ss, rs, dev):
        return pltpu.make_async_remote_copy(src_ref=src, dst_ref=dst, send_sem=ss, recv_sem=rs,
                                            device_id=dev, device_id_type=MESH)

    def rows(p):
        return pl.ds(pl.multiple_of((side * (tm_n - 1) + step * p) * R, R), R)

    def lev(p):
        return pl.ds(p * L, L)

    def peer(t):
        return lax.rem(me + 1 + t, tm_n)

    bar = pltpu.get_barrier_semaphore()

    @pl.loop(0, tm_n - 1)
    def _(t):
        pl.semaphore_signal(bar, inc=1, device_id={"tm": peer(t)}, device_id_type=MESH)

    pl.semaphore_signal(bar, inc=1, device_id={"block": lower_b}, device_id_type=MESH)
    pl.semaphore_signal(bar, inc=1, device_id={"block": upper_b}, device_id_type=MESH)

    @pl.when(is_last)
    def _():
        for h in range(half):
            pl.semaphore_signal(bar, inc=1, device_id={"block": other0 + h}, device_id_type=MESH)

    own = pltpu.make_async_copy(state.at[:, :, rows(me)], x0.at[lev(me)], loc.at[0])
    own.start()
    pl.semaphore_wait(bar, tm_n + 1 + jnp.where(is_last, half, 0))

    def in_copy(p, src_tm):
        return rc(state.at[:, :, rows(p)], x0.at[lev(src_tm)], in_s.at[p], in_r.at[src_tm], {"tm": p})

    @pl.loop(0, tm_n - 1)
    def _(t):
        p = peer(t)
        in_copy(p, me).start()

    def far_copy(src_tm):
        return rc(far, ff.at[lev(src_tm)], p_s.at[0], p_r.at[0, src_tm], {"tm": 0})

    def wt_copy(src_tm):
        return rc(fw, wts.at[lev(src_tm)], p_s.at[1], p_r.at[1, src_tm], {"tm": tm_n - 1})

    def ix_copy(src_tm):
        return rc(fidx, fi.at[src_tm], p_s.at[2], p_r.at[2, src_tm], {"tm": tm_n - 1})

    own_far = pltpu.make_async_copy(far, ff.at[lev(me)], loc.at[1])
    own_wt = pltpu.make_async_copy(fw, wts.at[lev(me)], loc.at[2])
    own_ix = pltpu.make_async_copy(fidx, fi.at[me], loc.at[3])

    @pl.when(is_far)
    def _():
        own_far.start()

    @pl.when(jnp.logical_not(is_far))
    def _():
        far_copy(me).start()

    @pl.when(is_last)
    def _():
        own_wt.start()
        own_ix.start()

    @pl.when(jnp.logical_not(is_last))
    def _():
        wt_copy(me).start()
        ix_copy(me).start()

    lane = lax.broadcasted_iota(jnp.int32, (8, 128), 1)
    lane_pair = jnp.bitwise_or(lane, 1)
    sub = lax.broadcasted_iota(jnp.int32, (8, 128), 0)

    def pack(acc, value, k):
        return jnp.where(lane_pair == k, pltpu.roll(value, k, 1), acc)

    def key(l, v):
        return 2 * (4 * l + v) + 1

    def halo_copies(s):
        low = rc(ef.at[s], ru.at[s], h_s.at[s, 0], h_r.at[s, 0], {"tm": me - step})
        up = rc(el.at[s], rl.at[s], h_s.at[s, 1], h_r.at[s, 1], {"tm": me + step})
        jl = rc(cs.at[s], cu.at[s], h_s.at[s, 2], h_r.at[s, 2], {"block": lower_b})
        ju = rc(cs.at[s], cl.at[s], h_s.at[s, 3], h_r.at[s, 3], {"block": upper_b})
        return low, up, jl, ju

    def face_copy(s, h, edge):
        return rc(edge.at[s], face.at[s, place], f_s.at[s, h], f_r.at[s, place], {"block": other0 + h})

    def face_wait(s, h):
        return rc(ef.at[s], face.at[s, h], f_s.at[s, h], f_r.at[s, h], {"block": other0 + h})

    def send_halos(s):
        low, up, jl, ju = halo_copies(s)

        @pl.when(is_last & (side == 0))
        def _():
            for h in range(half):
                face_copy(s, h, el).start()

        @pl.when(is_last & (side == 1))
        def _():
            for h in range(half):
                face_copy(s, h, ef).start()

        @pl.when(has_lower)
        def _():
            low.start()

        @pl.when(has_upper)
        def _():
            up.start()

        jl.start()
        ju.start()

    def take_level(l, accs):
        accs = list(accs)
        for v in range(4):
            for a in range(tiles):
                value = x0[l, v, pl.ds(8 * a, 8)]
                qa[l, v, pl.ds(PAD + 8 * a, 8)] = value
                accs[a] = pack(accs[a], value, key(l, v))
                if a == 0:
                    ef[0, pl.ds(4 * l + v, 1)] = value[0:1]
                if a == tiles - 1:
                    el[0, pl.ds(4 * l + v, 1)] = value[7:8]
        return tuple(accs)

    own.wait()
    accs = tuple(jnp.zeros((8, 128), jnp.float32) for _ in range(tiles))
    accs = lax.fori_loop(0, L, lambda j, c: take_level(me * L + j, c), accs)

    def arrive(t, c):
        p = peer(tm_n - 2 - t)
        in_copy(p, p).wait_recv()
        return lax.fori_loop(0, L, lambda j, d: take_level(p * L + j, d), c)

    accs = lax.fori_loop(0, tm_n - 1, arrive, accs)
    for a in range(tiles):
        cs[0, pl.ds(8 * a, 8)] = accs[a]
    send_halos(0)

    @pl.when(is_far)
    def _():
        own_far.wait()

        @pl.loop(1, tm_n)
        def _(p):
            far_copy(p).wait_recv()

        @pl.loop(0, NT)
        def _(l):
            for v in range(4):
                row = ff[l, pl.ds(v, 1)]
                qa[l, v, pl.ds(far_row, 1)] = row
                qb[l, v, pl.ds(far_row, 1)] = row

    @pl.when(is_last)
    def _():
        own_wt.wait()
        own_ix.wait()

        @pl.loop(0, tm_n - 1)
        def _(p):
            wt_copy(p).wait_recv()
            ix_copy(p).wait_recv()

        @pl.loop(0, NT // 2)
        def _(m):
            def ix(l):
                return jnp.broadcast_to(fi[lax.div(l, L), pl.ds(lax.rem(l, L), 1)], (8, 128))

            def wt(l, k):
                return jnp.broadcast_to(wts[l, pl.ds(k, 1)], (8, 128))

            start = jnp.where(sub < 4, ix(2 * m), ix(2 * m + 1))
            at = pl.ds(8 * m, 8)
            for k in range(K):
                src = start + k
                src = jnp.where(src >= cycle, src - cycle, src)
                lane_ix[k, at] = jnp.bitwise_and(src, 127)
                blk_ix[k, at] = lax.shift_right_logical(src, 7)
                ww[k, at] = jnp.where(sub < 4, wt(2 * m, k), wt(2 * m + 1, k))

    speed_u = jnp.where(side == 0, mf[0, 0], mf[1, 0])
    speed_v = jnp.where(side == 0, mf[0, 1], mf[1, 1])
    odd_lane = jnp.bitwise_and(lane, 1) == 1
    edge_lane = {0: lane == 0, 127: lane == 127}

    def install(dst, src, at):
        @pl.loop(0, NT)
        def _(l):
            for v in range(4):
                dst[l, v, pl.ds(at, 1)] = src[pl.ds(4 * l + v, 1)]

    def out_copy(q, p, src_tm):
        return rc(q.at[lev(p), :, pl.ds(PAD, R)], out.at[:, :, rows(src_tm)],
                  out_s.at[p], out_r.at[src_tm], {"tm": p})

    for s, factor in enumerate(SECTION_FACTORS):
        q, nq = (qa, qb) if s % 2 == 0 else (qb, qa)
        final = s == nsec - 1
        even, odd = split_coefficients(NT, OMEGA * factor)
        hu, hv, hh = (0.5 * factor) * speed_u, (0.5 * factor) * speed_v, 0.5 * factor

        @pl.loop(0, 4)
        def _(v):
            @pl.loop(0, tiles)
            def _(a):
                at = pl.ds(pl.multiple_of(PAD + 8 * a, 8), 8)
                xs = [q[l, v, at] for l in range(NT)]
                terms = time_term(xs, even, odd)
                for l in range(NT):
                    first = x0[l, v, pl.ds(pl.multiple_of(8 * a, 8), 8)]
                    nq[l, v, at] = first - (terms[l] + (4.0 * DISSIPATION * factor) * xs[l])

        low, up, jl, ju = halo_copies(s)
        jl.wait_recv()
        ju.wait_recv()
        mixed = []
        for a in range(tiles):
            at = pl.ds(8 * a, 8)
            mixed.append(jnp.where(odd_lane, pltpu.roll(cl[s, at], 1, 1), pltpu.roll(cu[s, at], 127, 1)))

        def level(l, accs, which):
            accs = list(accs)
            for slot, a in enumerate(which):
                base = PAD + 8 * a
                di, dj, near = [], [], []
                for v in range(4):
                    x = q[l, v, pl.ds(base, 8)]
                    upx = q[l, v, pl.ds(base + 1, 8)]
                    dnx = q[l, v, pl.ds(base - 1, 8)]
                    border = pltpu.roll(mixed[a], 128 - key(l, v), 1)
                    left = jnp.where(edge_lane[0], border, pltpu.roll(x, 1, 1))
                    right = jnp.where(edge_lane[127], border, pltpu.roll(x, 127, 1))
                    di.append(upx - dnx)
                    dj.append(right - left)
                    near.append((DISSIPATION * factor) * ((upx + dnx) + (right + left)))
                flux = [
                    hu * di[0] + hv * dj[0] + hh * (di[1] + dj[2]),
                    hu * di[1] + hv * dj[1] + hh * di[3],
                    hu * di[2] + hv * dj[2] + hh * dj[3],
                    hu * di[3] + hv * dj[3] + hh * (di[1] + dj[2]),
                ]
                for v in range(4):
                    new = nq[l, v, pl.ds(base, 8)] + (near[v] - flux[v])
                    nq[l, v, pl.ds(base, 8)] = new
                    if not final:
                        accs[slot] = pack(accs[slot], new, key(l, v))
                        if a == 0:
                            ef[s + 1, pl.ds(4 * l + v, 1)] = new[0:1]
                        if a == tiles - 1:
                            el[s + 1, pl.ds(4 * l + v, 1)] = new[7:8]
            return tuple(accs)

        def sweep(which):
            zero = tuple(jnp.zeros((8, 128), jnp.float32) for _ in which)
            step_by = 4 if NT % 4 == 0 else 1

            def several(g, c):
                for j in range(step_by):
                    c = level(step_by * g + j, c, which)
                return c

            accs = lax.fori_loop(0, NT // step_by, several, zero)
            if not final:
                for slot, a in enumerate(which):
                    cs[s + 1, pl.ds(8 * a, 8)] = accs[slot]

        inner = tuple(range(1, tiles - 1))
        outer = tuple(sorted({0, tiles - 1}))
        if inner:
            sweep(inner)

        @pl.when(has_lower)
        def _():
            up.wait_recv()
            install(q, rl.at[s], PAD - 1)

        @pl.when(has_upper)
        def _():
            low.wait_recv()
            install(q, ru.at[s], PAD + R)

        @pl.when(is_last)
        def _():
            for h in range(half):
                face_wait(s, h).wait_recv()

            @pl.loop(0, NT // 2)
            def _(m):
                at = pl.ds(8 * m, 8)
                total = jnp.zeros((8, 128), jnp.float32)
                for k in range(K):
                    picked = jnp.zeros((8, 128), jnp.float32)
                    for h in range(half):
                        got = jnp.take_along_axis(face[s, h, at], lane_ix[k, at], axis=1)
                        picked = jnp.where(blk_ix[k, at] == h, got, picked)
                    total = total + ww[k, at] * picked
                gh[at] = total

            install(q, gh, ghost_row)

        if not final:
            sweep(outer)
            send_halos(s + 1)
        else:
            def finish(t, c):
                p = peer(t)
                for j in range(L):
                    level(p * L + j, (None,) * len(outer), outer)

                @pl.when(t < tm_n - 1)
                def _():
                    out_copy(nq, p, me).start()

                return c

            lax.fori_loop(0, tm_n, finish, 0)
            own_out = pltpu.make_async_copy(nq.at[lev(me), :, pl.ds(PAD, R)], out.at[:, :, rows(me)], loc.at[4])
            own_out.start()

            @pl.loop(0, tm_n - 1)
            def _(t):
                p = peer(t)
                out_copy(nq, p, p).wait_recv()

            own_out.wait()

            @pl.loop(0, tm_n - 1)
            def _(t):
                p = peer(t)
                out_copy(nq, p, me).wait_send()

    @pl.loop(0, tm_n - 1)
    def _(t):
        p = peer(t)
        in_copy(p, me).wait_send()

    @pl.when(jnp.logical_not(is_far))
    def _():
        far_copy(me).wait_send()

    @pl.when(jnp.logical_not(is_last))
    def _():
        wt_copy(me).wait_send()
        ix_copy(me).wait_send()

    for s in range(nsec):
        low, up, jl, ju = halo_copies(s)

        @pl.when(has_lower)
        def _():
            low.wait_send()

        @pl.when(has_upper)
        def _():
            up.wait_send()

        jl.wait_send()
        ju.wait_send()

        @pl.when(is_last)
        def _():
            for h in range(half):
                face_wait(s, h).wait_send()


def shards(dims, state, far_field, face_index, face_weight, mean_flow):
    tm_n, half = dims
    L, _, rows, width = state.shape
    K = face_weight.shape[1]
    R = rows // tm_n
    NT = L * tm_n
    assert width == 128 and NT % 4 == 0 and R % 8 == 0 and 8 * NT <= width
    n = len(SECTION_FACTORS)
    f32 = jnp.float32
    hbm = pl.BlockSpec(memory_space=pl.ANY)
    dma = pltpu.SemaphoreType.DMA
    V = pltpu.VMEM
    return pl.pallas_call(
        functools.partial(kernel, (tm_n, half, L, R, K)),
        out_shape=jax.ShapeDtypeStruct(state.shape, f32),
        in_specs=[hbm, hbm, hbm, hbm, pl.BlockSpec(memory_space=pltpu.SMEM)],
        out_specs=hbm,
        scratch_shapes=[
            V((NT, 4, R, width), f32),
            V((NT, 4, R + 2 * PAD, width), f32),
            V((NT, 4, R + 2 * PAD, width), f32),
            V((n, 4 * NT, width), f32),
            V((n, 4 * NT, width), f32),
            V((n, 4 * NT, width), f32),
            V((n, 4 * NT, width), f32),
            V((n, R, width), f32),
            V((n, R, width), f32),
            V((n, R, width), f32),
            V((n, half, 4 * NT, width), f32),
            V((NT, 4, width), f32),
            V((NT, K, width), f32),
            V((tm_n, L, width), jnp.int32),
            V((K, 4 * NT, width), jnp.int32),
            V((K, 4 * NT, width), jnp.int32),
            V((K, 4 * NT, width), f32),
            V((4 * NT, width), f32),
            dma((tm_n,)), dma((tm_n,)), dma((tm_n,)), dma((tm_n,)),
            dma((3,)), dma((3, tm_n)),
            dma((n, 4)), dma((n, 4)),
            dma((n, half)), dma((n, half)),
            dma((5,)),
        ],
        compiler_params=pltpu.CompilerParams(
            collective_id=0, has_side_effects=True, vmem_limit_bytes=40 * 1024 * 1024),
    )(state, far_field, face_index, face_weight, mean_flow)


def skew_part(o, coef):
    half = len(o)
    quarter = half // 2

    def at(n):
        return o[n % half], -1.0 if (n // half) % 2 else 1.0

    res = []
    for n in range(half):
        total = None
        for m in range(1, quarter):
            (a, sa), (b, sb) = at(n - m), at(n + m)
            term = (coef[m] * sa) * (a - b if sa == sb else a + b)
            total = term if total is None else total + term
        a, sa = at(n - quarter)
        term = (coef[quarter] * sa) * a
        res.append(term if total is None else total + term)
    return res


def cyclic_part(e, coef):
    half = len(e)
    res = []
    for n in range(half):
        total = None
        for m in range(1, half // 2):
            term = coef[m] * (e[(n - m) % half] - e[(n + m) % half])
            total = term if total is None else total + term
        res.append(total)
    return res


def time_term_split(q, even, odd):
    half = len(q) // 2
    quarter = half // 2
    e = [q[n] + q[n + half] for n in range(half)]
    o = [q[n] - q[n + half] for n in range(half)]
    ee = [e[n] + e[n + quarter] for n in range(quarter)]
    eo = [e[n] - e[n + quarter] for n in range(quarter)]
    low = [0.0] + [0.5 * (even[m] - even[quarter - m]) for m in range(1, quarter)]
    high = [0.0] + [0.5 * (even[m] + even[quarter - m]) for m in range(1, quarter)]
    cyc = cyclic_part(ee, low)
    skw = skew_part(eo, high)
    ev = [cyc[n] + skw[n] for n in range(quarter)] + [cyc[n] - skw[n] for n in range(quarter)]
    od = skew_part(o, odd)
    return [ev[n] + od[n] for n in range(half)] + [ev[n] - od[n] for n in range(half)]


def ring_kernel(dims, state, far, fidx, fw, mf, out, q, tt, ff, wts, fi, lane_ix, blk_ix, ww, gg, fo, mfs,
                in_s, in_r, dup_s, dup_r, out_s, out_r, p_s, p_r, h_s, h_r, loc):
    tm_n, half, L, R, K = dims
    NT = tm_n * L
    G = tm_n * half
    Z = tm_n // 2
    cycle = half * 128
    nsec = len(SECTION_FACTORS)
    reach = 2 * nsec
    groups = 4 * NT // 8
    me = lax.axis_index("tm")
    blk = lax.axis_index("block")
    side = lax.div(blk, half)
    place = lax.rem(blk, half)

    def slab(t, b, sd):
        z = lax.div(t, 2)
        c = lax.rem(t, 2)
        zo = jnp.where(sd == 0, z, Z - 1 - z)
        return 4 * zo + jnp.where(lax.rem(b + zo, 2) == 0, c, 3 - c)

    def owner(g, sd):
        zo = g // 4 if isinstance(g, int) else lax.div(g, 4)
        k = g % 4 if isinstance(g, int) else lax.rem(g, 4)
        xo = jnp.where(k >= 2, 1, 0)
        c = jnp.where(k >= 2, 3 - k, k)
        b = lax.rem(xo + zo, 2)
        return 2 * jnp.where(sd == 0, zo, Z - 1 - zo) + c, b

    def device(g, sd):
        t, b = owner(g, sd)
        return {"tm": t, "block": sd * half + b}

    g = slab(me, place, side)
    here = me * half + place
    seam = g == G - 1
    mixes = seam & (side == 0)
    ends = seam & (side == 1)
    mix_dev = device(G - 1, 0)
    end_dev = device(G - 1, 1)
    dup_list = [4 * z + 3 for z in range(1, Z - 1)]

    def is_dup(x):
        hit = x < -1
        for d in dup_list:
            hit = hit | (x == d)
        return hit

    takes_dup = is_dup(g)
    feeds_prev = jnp.logical_not(is_dup(g - 1))
    prev_side = jnp.where(g == 0, 1 - side, side)
    prev_dev = device(lax.rem(g + G - 1, G), prev_side)
    next_side = jnp.where(seam, 1 - side, side)

    def peer(t):
        return lax.rem(here + 1 + t, G)

    def dev(j, sd):
        return {"tm": lax.div(j, half), "block": sd * half + lax.rem(j, half)}

    def slab_of(j):
        return slab(lax.div(j, half), lax.rem(j, half), side)

    def lev(t):
        return pl.ds(t * L, L)

    def rc(src, dst, ss, rs, to):
        return pltpu.make_async_remote_copy(src_ref=src, dst_ref=dst, send_sem=ss, recv_sem=rs,
                                            device_id=to, device_id_type=MESH)

    bar = pltpu.get_barrier_semaphore()

    @pl.loop(0, G - 1)
    def _(t):
        pl.semaphore_signal(bar, inc=1, device_id=dev(peer(t), side), device_id_type=MESH)

    @pl.when(seam)
    def _():
        @pl.loop(0, G)
        def _(j):
            pl.semaphore_signal(bar, inc=1, device_id=dev(j, 1 - side), device_id_type=MESH)

    @pl.when(jnp.logical_not(seam))
    def _():
        pl.semaphore_signal(bar, inc=1, device_id=device(G - 1, 1 - side), device_id_type=MESH)

    own = pltpu.make_async_copy(state.at[:, :, pl.ds(pl.multiple_of(g * R, R), R)],
                                q.at[0, place, lev(me), :, pl.ds(0, R)], loc.at[0])
    own.start()
    own_mf = pltpu.make_async_copy(mf, mfs, loc.at[4])
    own_mf.start()

    def ahead_rows(d):
        return state.at[:, :, pl.ds((d + 1) * R, reach)]

    def ahead_spot(j):
        return q.at[0, lax.rem(j, half), lev(lax.div(j, half)), :, pl.ds(R, reach)]

    def dup_copy(i, j):
        return rc(ahead_rows(dup_list[i]), ahead_spot(j), dup_s.at[i], dup_r.at[j], device(dup_list[i], side))

    def own_dup(i):
        return pltpu.make_async_copy(ahead_rows(dup_list[i]), ahead_spot(here), loc.at[5])

    for i, d in enumerate(dup_list):
        @pl.when(g == d)
        def _():
            own_dup(i).start()

    pl.semaphore_wait(bar, G + jnp.where(seam, G - 1, 0))

    def far_copy(j, sd):
        return rc(far, ff.at[sd, lax.rem(j, half), lev(lax.div(j, half))], p_s.at[0], p_r.at[0, sd * G + j], end_dev)

    def wt_copy(j, sd):
        return rc(fw, wts.at[sd, lax.rem(j, half), lev(lax.div(j, half))], p_s.at[1], p_r.at[1, sd * G + j], mix_dev)

    def ix_copy(j, sd):
        return rc(fidx, fi.at[sd, lax.rem(j, half), lax.div(j, half)], p_s.at[2], p_r.at[2, sd * G + j], mix_dev)

    own_far = pltpu.make_async_copy(far, ff.at[side, place, lev(me)], loc.at[1])
    own_wt = pltpu.make_async_copy(fw, wts.at[side, place, lev(me)], loc.at[2])
    own_ix = pltpu.make_async_copy(fidx, fi.at[side, place, me], loc.at[3])

    @pl.when(ends)
    def _():
        own_far.start()

    @pl.when(jnp.logical_not(ends))
    def _():
        far_copy(here, side).start()

    @pl.when(mixes)
    def _():
        own_wt.start()
        own_ix.start()

    @pl.when(jnp.logical_not(mixes))
    def _():
        wt_copy(here, side).start()
        ix_copy(here, side).start()

    parts = ((0, reach), (reach, R - reach))

    def in_copy(i, j, src):
        lo, n = parts[i]
        return rc(state.at[:, :, pl.ds(slab_of(j) * R + lo, n)],
                  q.at[0, lax.rem(src, half), lev(lax.div(src, half)), :, pl.ds(lo, n)],
                  in_s.at[i, j], in_r.at[i, src], dev(j, side))

    @pl.loop(0, G - 1)
    def _(t):
        in_copy(0, peer(t), here).start()

    for i, d in enumerate(dup_list):
        @pl.when(g != d)
        def _():
            dup_copy(i, here).start()

    @pl.loop(0, G - 1)
    def _(t):
        in_copy(1, peer(t), here).start()

    lane = lax.broadcasted_iota(jnp.int32, (8, 128), 1)
    sub = lax.broadcasted_iota(jnp.int32, (8, 128), 0)
    first_lane, last_lane = lane == 0, lane == 127

    def others(sd):
        def each(body):
            @pl.loop(0, G - 1)
            def _(t):
                body(peer(t), sd)

            @pl.loop(0, G)
            def _(j):
                body(j, 1 - sd)
        return each

    @pl.when(ends)
    def _():
        own_far.wait()

        @others(1)
        def _(j, sd):
            far_copy(j, sd).wait_recv()

        for k in range(2):
            for b in range(half):
                @pl.loop(0, NT)
                def _(l):
                    for v in range(4):
                        gg[k, b, pl.ds(4 * l + v, 1)] = ff[1 - k, b, l, pl.ds(v, 1)]

    @pl.when(mixes)
    def _():
        own_wt.wait()
        own_ix.wait()

        @others(0)
        def _(j, sd):
            wt_copy(j, sd).wait_recv()
            ix_copy(j, sd).wait_recv()

        for r in range(2):
            for b in range(half):
                @pl.loop(0, NT // 2)
                def _(m):
                    def ix(l):
                        return jnp.broadcast_to(fi[r, b, lax.div(l, L), pl.ds(lax.rem(l, L), 1)], (8, 128))

                    def wt(l, k):
                        return jnp.broadcast_to(wts[r, b, l, pl.ds(k, 1)], (8, 128))

                    start = jnp.where(sub < 4, ix(2 * m), ix(2 * m + 1))
                    at = pl.ds(8 * m, 8)
                    for k in range(K):
                        src = start + k
                        src = jnp.where(src >= cycle, src - cycle, src)
                        lane_ix[r, k, b, at] = jnp.bitwise_and(src, 127)
                        blk_ix[r, k, b, at] = lax.shift_right_logical(src, 7)
                        ww[r, k, b, at] = jnp.where(sub < 4, wt(2 * m, k), wt(2 * m + 1, k))

    own_mf.wait()

    def speeds(sd):
        return jnp.where(sd == 0, mfs[0, 0], mfs[1, 0]), jnp.where(sd == 0, mfs[0, 1], mfs[1, 1])

    own_speed = speeds(side)
    next_speed = speeds(next_side)

    def feed():
        return rc(q.at[0, :, :, :, pl.ds(0, reach)], q.at[0, :, :, :, pl.ds(R, reach)], h_s.at[0], h_r.at[0], prev_dev)

    def time_pass(s, w):
        c = SECTION_FACTORS[s - 1]
        even, odd = split_coefficients(NT, -OMEGA * c)
        at = pl.ds(w, 8)

        @pl.loop(0, 4)
        def _(v):
            for b in range(half):
                xs = [q[s - 1, b, l, v, at] for l in range(NT)]
                terms = time_term_split(xs, even, odd)
                for l in range(NT):
                    tt[b, l, v] = (q[0, b, l, v, at] + terms[l]) - (4.0 * DISSIPATION * c) * xs[l]

    def space_pass(s, w, lo, hi, ghosts=False, border=False):
        c = SECTION_FACTORS[s - 1]
        hh = 0.5 * c
        near = DISSIPATION * c

        def weights(uv):
            return near - hh * uv[0], near + hh * uv[0], near - hh * uv[1], near + hh * uv[1]

        cu, cd, cr, cl = weights(own_speed)
        if border:
            beyond = sub >= R - w
            cu, cd, cr, cl = [jnp.where(beyond, n, o) for n, o in zip(weights(next_speed), (cu, cd, cr, cl))]
        span = range(half)
        if ghosts:
            up_at = sub == jnp.where(seam, R - 1 - w, 8)
            dn_at = sub == jnp.where(seam, R - w, 8)

        def level(l):
            di = [[None] * half for _ in range(4)]
            dj = [[None] * half for _ in range(4)]
            acc = [[None] * half for _ in range(4)]
            for v in range(4):
                x = [q[s - 1, b, l, v, pl.ds(w, 8)] for b in span]
                rr = [pltpu.roll(x[b], 127, 1) for b in span]
                rl = [pltpu.roll(x[b], 1, 1) for b in span]
                for b in span:
                    up = q[s - 1, b, l, v, pl.ds(w + 1, 8)]
                    dn = q[s - 1, b, l, v, pl.ds(w - 1, 8)]
                    if ghosts:
                        at = pl.ds(4 * l + v, 1)
                        up = jnp.where(up_at, jnp.broadcast_to(gg[0, b, at], (8, 128)), up)
                        dn = jnp.where(dn_at, jnp.broadcast_to(gg[1, b, at], (8, 128)), dn)
                    right = jnp.where(last_lane, rr[(b + 1) % half], rr[b])
                    left = jnp.where(first_lane, rl[(b - 1) % half], rl[b])
                    acc[v][b] = (tt[b, l, v] + (cu * up + cd * dn)) + (cr * right + cl * left)
                    if v in (1, 3):
                        di[v][b] = up - dn
                    if v in (2, 3):
                        dj[v][b] = right - left
            for b in span:
                cross = hh * (di[1][b] + dj[2][b])
                new = [acc[0][b] - cross, acc[1][b] - hh * di[3][b], acc[2][b] - hh * dj[3][b], acc[3][b] - cross]
                for v in range(4):
                    q[s, b, l, v, pl.ds(w + lo, hi - lo)] = new[v][lo:hi]
                    if ghosts and s < nsec:
                        for k in range(2):
                            row = R - 1 + k - w
                            fo[k, b, pl.ds(4 * l + v, 1)] = new[v][row:row + 1]

        @pl.loop(0, NT // 4)
        def _(i):
            for j in range(4):
                level(4 * i + j)

    own.wait()

    @pl.loop(0, G - 1)
    def _(t):
        j = peer(G - 2 - t)
        in_copy(0, j, j).wait_recv()

    @pl.when(feeds_prev)
    def _():
        feed().start()

    for s in range(1, 4):
        w = min(s, reach - 8)
        time_pass(s, w)
        space_pass(s, w, s - w, reach - s - w)

    @pl.loop(0, G - 1)
    def _(t):
        j = peer(G - 2 - t)
        in_copy(1, j, j).wait_recv()

    for s in range(1, nsec + 1):
        if s < 4:
            w = R - 8 - s
            lo, hi = reach - s - w, 8
        else:
            w = (R - 8) // 2
            lo, hi = s - w, R - s - w
        time_pass(s, w)
        space_pass(s, w, lo, hi)

    spans = ((nsec, R - 2 * nsec), (R - nsec, nsec), (R, nsec))

    def result(i, j):
        lo, n = spans[i]
        return q.at[nsec, lax.rem(j, half), lev(lax.div(j, half)), :, pl.ds(lo, n)]

    def spot(i, gs):
        lo, n = spans[i]
        return out.at[:, :, pl.ds(gs * R + (lo if i < 2 else 0), n)]

    def out_copy(i, j, gs):
        return rc(result(i, j), spot(i, gs), out_s.at[i, j], out_r.at[i, gs], dev(j, side if i < 2 else next_side))

    def own_out(i, gs):
        return pltpu.make_async_copy(result(i, here), spot(i, gs), loc.at[5 + i])

    following = lax.rem(g + 1, G)
    takes_own = jnp.logical_not(seam)

    @pl.loop(0, G - 1)
    def _(t):
        out_copy(0, peer(t), g).start()

    for i, d in enumerate(dup_list):
        @pl.when(g == d)
        def _():
            own_dup(i).wait()

    @pl.when(takes_dup)
    def _():
        @pl.loop(0, G - 1)
        def _(t):
            dup_copy(0, peer(t)).wait_recv()

    @pl.when(jnp.logical_not(takes_dup))
    def _():
        feed().wait_recv()

    own_out(0, g).start()

    @pl.when(mixes)
    def _():
        @pl.loop(0, NT)
        def _(l):
            for b in range(half):
                for v in range(4):
                    for k in range(2):
                        fo[k, b, pl.ds(4 * l + v, 1)] = q[0, b, l, v, pl.ds(R - 1 + k, 1)]

    for s in range(1, nsec + 1):
        @pl.when(mixes)
        def _():
            @pl.loop(0, groups)
            def _(m):
                at = pl.ds(pl.multiple_of(8 * m, 8), 8)
                for r in range(2):
                    for b in range(half):
                        total = jnp.zeros((8, 128), jnp.float32)
                        for k in range(K):
                            picked = jnp.zeros((8, 128), jnp.float32)
                            for h in range(half):
                                got = jnp.take_along_axis(fo[1 - r, h, at], lane_ix[r, k, b, at], axis=1)
                                picked = jnp.where(blk_ix[r, k, b, at] == h, got, picked)
                            total = total + ww[r, k, b, at] * picked
                        gg[r, b, at] = total

        time_pass(s, R - s)
        space_pass(s, R - s, 0, 8, True, True)
        time_pass(s, R + 2 - s)
        space_pass(s, R + 2 - s, 6, 8, False, True)

    @pl.loop(0, G - 1)
    def _(t):
        out_copy(1, peer(t), g).start()
        out_copy(2, peer(t), following).start()

    own_out(1, g).start()

    @pl.when(takes_own)
    def _():
        own_out(2, following).start()

    @pl.when(seam)
    def _():
        out_copy(2, here, following).start()

    @pl.loop(0, G - 1)
    def _(t):
        gs = lax.rem(g + 1 + t, G)
        out_copy(0, here, gs).wait_recv()
        out_copy(1, here, gs).wait_recv()
        out_copy(2, here, lax.rem(gs + 1, G)).wait_recv()

    @pl.when(takes_own)
    def _():
        own_out(2, following).wait()

    @pl.when(seam)
    def _():
        out_copy(2, here, following).wait_recv()
        out_copy(2, here, following).wait_send()

    own_out(0, g).wait()
    own_out(1, g).wait()

    @pl.loop(0, G - 1)
    def _(t):
        j = peer(t)
        in_copy(0, j, here).wait_send()
        in_copy(1, j, here).wait_send()
        for i in range(3):
            out_copy(i, j, g).wait_send()

    for i, d in enumerate(dup_list):
        @pl.when(g != d)
        def _():
            dup_copy(i, here).wait_send()

    @pl.when(feeds_prev)
    def _():
        feed().wait_send()

    @pl.when(jnp.logical_not(ends))
    def _():
        far_copy(here, side).wait_send()

    @pl.when(jnp.logical_not(mixes))
    def _():
        wt_copy(here, side).wait_send()
        ix_copy(here, side).wait_send()


def ring_shards(dims, state, far_field, face_index, face_weight, mean_flow):
    tm_n, half = dims
    L, _, rows, width = state.shape
    K = face_weight.shape[1]
    G = tm_n * half
    R = rows // G
    NT = L * tm_n
    n = len(SECTION_FACTORS)
    f32 = jnp.float32
    hbm = pl.BlockSpec(memory_space=pl.ANY)
    dma = pltpu.SemaphoreType.DMA
    V = pltpu.VMEM
    args = [pltpu.with_memory_space_constraint(a, pltpu.HBM)
            for a in (state, far_field, face_index, face_weight, mean_flow)]
    return pl.pallas_call(
        functools.partial(ring_kernel, (tm_n, half, L, R, K)),
        out_shape=jax.ShapeDtypeStruct(state.shape, f32),
        in_specs=[hbm] * 5,
        out_specs=hbm,
        scratch_shapes=[
            V((n + 1, half, NT, 4, R + 16, width), f32),
            V((half, NT, 4, 8, width), f32),
            V((2, half, NT, 4, width), f32),
            V((2, half, NT, K, width), f32),
            V((2, half, tm_n, L, width), jnp.int32),
            V((2, K, half, 4 * NT, width), jnp.int32),
            V((2, K, half, 4 * NT, width), jnp.int32),
            V((2, K, half, 4 * NT, width), f32),
            V((2, half, 4 * NT, width), f32),
            V((2, half, 4 * NT, width), f32),
            pltpu.SMEM((2, 2), f32),
            dma((2, G)), dma((2, G)),
            dma((tm_n,)), dma((G,)),
            dma((3, G)), dma((3, G)),
            dma((3,)), dma((3, 2 * G)),
            dma((1,)), dma((1,)),
            dma((8,)),
        ],
        compiler_params=pltpu.CompilerParams(
            collective_id=0, has_side_effects=True, vmem_limit_bytes=48 * 1024 * 1024),
    )(*args)


def solution(mesh):
    dims = (mesh.shape["tm"], mesh.shape["block"] // 2)
    in_specs = (
        P("tm", None, None, "block"),
        P("tm", None, "block"),
        P("tm", "block"),
        P("tm", None, "block"),
        P(),
    )
    out_specs = P("tm", None, None, "block")

    def body(state, *rest):
        tm_n, half = dims
        fits = (half == 2 and tm_n % 2 == 0 and tm_n >= 4 and state.shape[2] == 16 * tm_n * half
                and state.shape[3] == 128 and state.shape[0] * tm_n % 8 == 0)
        return (ring_shards if fits else shards)(dims, state, *rest)

    return jax.shard_map(body, mesh=mesh, in_specs=in_specs, out_specs=out_specs, check_vma=False)
```

```python
import functools
import math

import jax
import jax.numpy as jnp
from jax import lax
from jax.experimental import pallas as pl
from jax.experimental.pallas import tpu as pltpu
from jax.sharding import PartitionSpec as P

SECTION_FACTORS = (0.075, 0.05, 0.1125, 0.15, 0.3)
OMEGA = 1.0
DISSIPATION = 0.2
PAD = 8
FIRST_ROWS = 11
MESH = pl.DeviceIdType.MESH


def split_coefficients(count, scale):
    half = count // 2
    d = [0.0] + [0.5 * (-1) ** k / math.tan(math.pi * k / count) for k in range(1, half)] + [0.0]
    even = [0.5 * scale * (d[m] - d[half - m]) for m in range(half)]
    odd = [0.5 * scale * (d[m] + d[half - m]) for m in range(half)]
    even[0] = odd[0] = 0.0
    return even, odd


def time_term(q, even, odd):
    half = len(q) // 2
    quarter = half // 2
    e = [q[n] + q[n + half] for n in range(half)]
    o = [q[n] - q[n + half] for n in range(half)]

    def odd_at(n):
        return (o[n % half], -1.0 if (n // half) % 2 else 1.0)

    low, high = [], []
    for n in range(half):
        ev = None
        od = None
        for m in range(1, quarter):
            term = even[m] * (e[(n - m) % half] - e[(n + m) % half])
            ev = term if ev is None else ev + term
            (a, sa), (b, sb) = odd_at(n - m), odd_at(n + m)
            pair = a - b if sa == sb else a + b
            term = (odd[m] * sa) * pair
            od = term if od is None else od + term
        a, sa = odd_at(n - quarter)
        od = od + (odd[quarter] * sa) * a
        low.append(ev + od)
        high.append(ev - od)
    return low + high


def kernel(dims, state, far, fidx, fw, mf, out, x0, qa, qb, ef, el, rl, ru, cs, cl, cu,
           face, ff, wts, fi, lane_ix, blk_ix, ww, gh,
           in_s, in_r, out_s, out_r, p_s, p_r, h_s, h_r, f_s, f_r, loc):
    tm_n, half, L, R, K = dims
    NT = tm_n * L
    cycle = half * 128
    tiles = R // 8
    nsec = len(SECTION_FACTORS)
    me = lax.axis_index("tm")
    blk = lax.axis_index("block")
    side = lax.div(blk, half)
    place = lax.rem(blk, half)
    row0 = side * half
    lower_b = row0 + lax.rem(place + half - 1, half)
    upper_b = row0 + lax.rem(place + 1, half)
    other0 = (1 - side) * half
    step = 1 - 2 * side
    is_last = me == tm_n - 1
    is_far = me == 0
    rchunk = side * (tm_n - 1) + step * me
    has_lower = rchunk > 0
    has_upper = rchunk < tm_n - 1
    ghost_row = jnp.where(side == 0, PAD + R, PAD - 1)
    far_row = jnp.where(side == 0, PAD - 1, PAD + R)

    def rc(src, dst, ss, rs, dev):
        return pltpu.make_async_remote_copy(src_ref=src, dst_ref=dst, send_sem=ss, recv_sem=rs,
                                            device_id=dev, device_id_type=MESH)

    def rows(p):
        return pl.ds(pl.multiple_of((side * (tm_n - 1) + step * p) * R, R), R)

    def lev(p):
        return pl.ds(p * L, L)

    def peer(t):
        return lax.rem(me + 1 + t, tm_n)

    bar = pltpu.get_barrier_semaphore()

    @pl.loop(0, tm_n - 1)
    def _(t):
        pl.semaphore_signal(bar, inc=1, device_id={"tm": peer(t)}, device_id_type=MESH)

    pl.semaphore_signal(bar, inc=1, device_id={"block": lower_b}, device_id_type=MESH)
    pl.semaphore_signal(bar, inc=1, device_id={"block": upper_b}, device_id_type=MESH)

    @pl.when(is_last)
    def _():
        for h in range(half):
            pl.semaphore_signal(bar, inc=1, device_id={"block": other0 + h}, device_id_type=MESH)

    own = pltpu.make_async_copy(state.at[:, :, rows(me)], x0.at[lev(me)], loc.at[0])
    own.start()
    pl.semaphore_wait(bar, tm_n + 1 + jnp.where(is_last, half, 0))

    def in_copy(p, src_tm):
        return rc(state.at[:, :, rows(p)], x0.at[lev(src_tm)], in_s.at[p], in_r.at[src_tm], {"tm": p})

    @pl.loop(0, tm_n - 1)
    def _(t):
        p = peer(t)
        in_copy(p, me).start()

    def far_copy(src_tm):
        return rc(far, ff.at[lev(src_tm)], p_s.at[0], p_r.at[0, src_tm], {"tm": 0})

    def wt_copy(src_tm):
        return rc(fw, wts.at[lev(src_tm)], p_s.at[1], p_r.at[1, src_tm], {"tm": tm_n - 1})

    def ix_copy(src_tm):
        return rc(fidx, fi.at[src_tm], p_s.at[2], p_r.at[2, src_tm], {"tm": tm_n - 1})

    own_far = pltpu.make_async_copy(far, ff.at[lev(me)], loc.at[1])
    own_wt = pltpu.make_async_copy(fw, wts.at[lev(me)], loc.at[2])
    own_ix = pltpu.make_async_copy(fidx, fi.at[me], loc.at[3])

    @pl.when(is_far)
    def _():
        own_far.start()

    @pl.when(jnp.logical_not(is_far))
    def _():
        far_copy(me).start()

    @pl.when(is_last)
    def _():
        own_wt.start()
        own_ix.start()

    @pl.when(jnp.logical_not(is_last))
    def _():
        wt_copy(me).start()
        ix_copy(me).start()

    lane = lax.broadcasted_iota(jnp.int32, (8, 128), 1)
    lane_pair = jnp.bitwise_or(lane, 1)
    sub = lax.broadcasted_iota(jnp.int32, (8, 128), 0)

    def pack(acc, value, k):
        return jnp.where(lane_pair == k, pltpu.roll(value, k, 1), acc)

    def key(l, v):
        return 2 * (4 * l + v) + 1

    def halo_copies(s):
        low = rc(ef.at[s], ru.at[s], h_s.at[s, 0], h_r.at[s, 0], {"tm": me - step})
        up = rc(el.at[s], rl.at[s], h_s.at[s, 1], h_r.at[s, 1], {"tm": me + step})
        jl = rc(cs.at[s], cu.at[s], h_s.at[s, 2], h_r.at[s, 2], {"block": lower_b})
        ju = rc(cs.at[s], cl.at[s], h_s.at[s, 3], h_r.at[s, 3], {"block": upper_b})
        return low, up, jl, ju

    def face_copy(s, h, edge):
        return rc(edge.at[s], face.at[s, place], f_s.at[s, h], f_r.at[s, place], {"block": other0 + h})

    def face_wait(s, h):
        return rc(ef.at[s], face.at[s, h], f_s.at[s, h], f_r.at[s, h], {"block": other0 + h})

    def send_halos(s):
        low, up, jl, ju = halo_copies(s)

        @pl.when(is_last & (side == 0))
        def _():
            for h in range(half):
                face_copy(s, h, el).start()

        @pl.when(is_last & (side == 1))
        def _():
            for h in range(half):
                face_copy(s, h, ef).start()

        @pl.when(has_lower)
        def _():
            low.start()

        @pl.when(has_upper)
        def _():
            up.start()

        jl.start()
        ju.start()

    def take_level(l, accs):
        accs = list(accs)
        for v in range(4):
            for a in range(tiles):
                value = x0[l, v, pl.ds(8 * a, 8)]
                qa[l, v, pl.ds(PAD + 8 * a, 8)] = value
                accs[a] = pack(accs[a], value, key(l, v))
                if a == 0:
                    ef[0, pl.ds(4 * l + v, 1)] = value[0:1]
                if a == tiles - 1:
                    el[0, pl.ds(4 * l + v, 1)] = value[7:8]
        return tuple(accs)

    own.wait()
    accs = tuple(jnp.zeros((8, 128), jnp.float32) for _ in range(tiles))
    accs = lax.fori_loop(0, L, lambda j, c: take_level(me * L + j, c), accs)

    def arrive(t, c):
        p = peer(tm_n - 2 - t)
        in_copy(p, p).wait_recv()
        return lax.fori_loop(0, L, lambda j, d: take_level(p * L + j, d), c)

    accs = lax.fori_loop(0, tm_n - 1, arrive, accs)
    for a in range(tiles):
        cs[0, pl.ds(8 * a, 8)] = accs[a]
    send_halos(0)

    @pl.when(is_far)
    def _():
        own_far.wait()

        @pl.loop(1, tm_n)
        def _(p):
            far_copy(p).wait_recv()

        @pl.loop(0, NT)
        def _(l):
            for v in range(4):
                row = ff[l, pl.ds(v, 1)]
                qa[l, v, pl.ds(far_row, 1)] = row
                qb[l, v, pl.ds(far_row, 1)] = row

    @pl.when(is_last)
    def _():
        own_wt.wait()
        own_ix.wait()

        @pl.loop(0, tm_n - 1)
        def _(p):
            wt_copy(p).wait_recv()
            ix_copy(p).wait_recv()

        @pl.loop(0, NT // 2)
        def _(m):
            def ix(l):
                return jnp.broadcast_to(fi[lax.div(l, L), pl.ds(lax.rem(l, L), 1)], (8, 128))

            def wt(l, k):
                return jnp.broadcast_to(wts[l, pl.ds(k, 1)], (8, 128))

            start = jnp.where(sub < 4, ix(2 * m), ix(2 * m + 1))
            at = pl.ds(8 * m, 8)
            for k in range(K):
                src = start + k
                src = jnp.where(src >= cycle, src - cycle, src)
                lane_ix[k, at] = jnp.bitwise_and(src, 127)
                blk_ix[k, at] = lax.shift_right_logical(src, 7)
                ww[k, at] = jnp.where(sub < 4, wt(2 * m, k), wt(2 * m + 1, k))

    speed_u = jnp.where(side == 0, mf[0, 0], mf[1, 0])
    speed_v = jnp.where(side == 0, mf[0, 1], mf[1, 1])
    odd_lane = jnp.bitwise_and(lane, 1) == 1
    edge_lane = {0: lane == 0, 127: lane == 127}

    def install(dst, src, at):
        @pl.loop(0, NT)
        def _(l):
            for v in range(4):
                dst[l, v, pl.ds(at, 1)] = src[pl.ds(4 * l + v, 1)]

    def out_copy(q, p, src_tm):
        return rc(q.at[lev(p), :, pl.ds(PAD, R)], out.at[:, :, rows(src_tm)],
                  out_s.at[p], out_r.at[src_tm], {"tm": p})

    for s, factor in enumerate(SECTION_FACTORS):
        q, nq = (qa, qb) if s % 2 == 0 else (qb, qa)
        final = s == nsec - 1
        even, odd = split_coefficients(NT, OMEGA * factor)
        hu, hv, hh = (0.5 * factor) * speed_u, (0.5 * factor) * speed_v, 0.5 * factor

        @pl.loop(0, 4)
        def _(v):
            @pl.loop(0, tiles)
            def _(a):
                at = pl.ds(pl.multiple_of(PAD + 8 * a, 8), 8)
                xs = [q[l, v, at] for l in range(NT)]
                terms = time_term(xs, even, odd)
                for l in range(NT):
                    first = x0[l, v, pl.ds(pl.multiple_of(8 * a, 8), 8)]
                    nq[l, v, at] = first - (terms[l] + (4.0 * DISSIPATION * factor) * xs[l])

        low, up, jl, ju = halo_copies(s)
        jl.wait_recv()
        ju.wait_recv()
        mixed = []
        for a in range(tiles):
            at = pl.ds(8 * a, 8)
            mixed.append(jnp.where(odd_lane, pltpu.roll(cl[s, at], 1, 1), pltpu.roll(cu[s, at], 127, 1)))

        def level(l, accs, which):
            accs = list(accs)
            for slot, a in enumerate(which):
                base = PAD + 8 * a
                di, dj, near = [], [], []
                for v in range(4):
                    x = q[l, v, pl.ds(base, 8)]
                    upx = q[l, v, pl.ds(base + 1, 8)]
                    dnx = q[l, v, pl.ds(base - 1, 8)]
                    border = pltpu.roll(mixed[a], 128 - key(l, v), 1)
                    left = jnp.where(edge_lane[0], border, pltpu.roll(x, 1, 1))
                    right = jnp.where(edge_lane[127], border, pltpu.roll(x, 127, 1))
                    di.append(upx - dnx)
                    dj.append(right - left)
                    near.append((DISSIPATION * factor) * ((upx + dnx) + (right + left)))
                flux = [
                    hu * di[0] + hv * dj[0] + hh * (di[1] + dj[2]),
                    hu * di[1] + hv * dj[1] + hh * di[3],
                    hu * di[2] + hv * dj[2] + hh * dj[3],
                    hu * di[3] + hv * dj[3] + hh * (di[1] + dj[2]),
                ]
                for v in range(4):
                    new = nq[l, v, pl.ds(base, 8)] + (near[v] - flux[v])
                    nq[l, v, pl.ds(base, 8)] = new
                    if not final:
                        accs[slot] = pack(accs[slot], new, key(l, v))
                        if a == 0:
                            ef[s + 1, pl.ds(4 * l + v, 1)] = new[0:1]
                        if a == tiles - 1:
                            el[s + 1, pl.ds(4 * l + v, 1)] = new[7:8]
            return tuple(accs)

        def sweep(which):
            zero = tuple(jnp.zeros((8, 128), jnp.float32) for _ in which)
            step_by = 4 if NT % 4 == 0 else 1

            def several(g, c):
                for j in range(step_by):
                    c = level(step_by * g + j, c, which)
                return c

            accs = lax.fori_loop(0, NT // step_by, several, zero)
            if not final:
                for slot, a in enumerate(which):
                    cs[s + 1, pl.ds(8 * a, 8)] = accs[slot]

        inner = tuple(range(1, tiles - 1))
        outer = tuple(sorted({0, tiles - 1}))
        if inner:
            sweep(inner)

        @pl.when(has_lower)
        def _():
            up.wait_recv()
            install(q, rl.at[s], PAD - 1)

        @pl.when(has_upper)
        def _():
            low.wait_recv()
            install(q, ru.at[s], PAD + R)

        @pl.when(is_last)
        def _():
            for h in range(half):
                face_wait(s, h).wait_recv()

            @pl.loop(0, NT // 2)
            def _(m):
                at = pl.ds(8 * m, 8)
                total = jnp.zeros((8, 128), jnp.float32)
                for k in range(K):
                    picked = jnp.zeros((8, 128), jnp.float32)
                    for h in range(half):
                        got = jnp.take_along_axis(face[s, h, at], lane_ix[k, at], axis=1)
                        picked = jnp.where(blk_ix[k, at] == h, got, picked)
                    total = total + ww[k, at] * picked
                gh[at] = total

            install(q, gh, ghost_row)

        if not final:
            sweep(outer)
            send_halos(s + 1)
        else:
            def finish(t, c):
                p = peer(t)
                for j in range(L):
                    level(p * L + j, (None,) * len(outer), outer)

                @pl.when(t < tm_n - 1)
                def _():
                    out_copy(nq, p, me).start()

                return c

            lax.fori_loop(0, tm_n, finish, 0)
            own_out = pltpu.make_async_copy(nq.at[lev(me), :, pl.ds(PAD, R)], out.at[:, :, rows(me)], loc.at[4])
            own_out.start()

            @pl.loop(0, tm_n - 1)
            def _(t):
                p = peer(t)
                out_copy(nq, p, p).wait_recv()

            own_out.wait()

            @pl.loop(0, tm_n - 1)
            def _(t):
                p = peer(t)
                out_copy(nq, p, me).wait_send()

    @pl.loop(0, tm_n - 1)
    def _(t):
        p = peer(t)
        in_copy(p, me).wait_send()

    @pl.when(jnp.logical_not(is_far))
    def _():
        far_copy(me).wait_send()

    @pl.when(jnp.logical_not(is_last))
    def _():
        wt_copy(me).wait_send()
        ix_copy(me).wait_send()

    for s in range(nsec):
        low, up, jl, ju = halo_copies(s)

        @pl.when(has_lower)
        def _():
            low.wait_send()

        @pl.when(has_upper)
        def _():
            up.wait_send()

        jl.wait_send()
        ju.wait_send()

        @pl.when(is_last)
        def _():
            for h in range(half):
                face_wait(s, h).wait_send()


def shards(dims, state, far_field, face_index, face_weight, mean_flow):
    tm_n, half = dims
    L, _, rows, width = state.shape
    K = face_weight.shape[1]
    R = rows // tm_n
    NT = L * tm_n
    assert width == 128 and NT % 4 == 0 and R % 8 == 0 and 8 * NT <= width
    n = len(SECTION_FACTORS)
    f32 = jnp.float32
    hbm = pl.BlockSpec(memory_space=pl.ANY)
    dma = pltpu.SemaphoreType.DMA
    V = pltpu.VMEM
    return pl.pallas_call(
        functools.partial(kernel, (tm_n, half, L, R, K)),
        out_shape=jax.ShapeDtypeStruct(state.shape, f32),
        in_specs=[hbm, hbm, hbm, hbm, pl.BlockSpec(memory_space=pltpu.SMEM)],
        out_specs=hbm,
        scratch_shapes=[
            V((NT, 4, R, width), f32),
            V((NT, 4, R + 2 * PAD, width), f32),
            V((NT, 4, R + 2 * PAD, width), f32),
            V((n, 4 * NT, width), f32),
            V((n, 4 * NT, width), f32),
            V((n, 4 * NT, width), f32),
            V((n, 4 * NT, width), f32),
            V((n, R, width), f32),
            V((n, R, width), f32),
            V((n, R, width), f32),
            V((n, half, 4 * NT, width), f32),
            V((NT, 4, width), f32),
            V((NT, K, width), f32),
            V((tm_n, L, width), jnp.int32),
            V((K, 4 * NT, width), jnp.int32),
            V((K, 4 * NT, width), jnp.int32),
            V((K, 4 * NT, width), f32),
            V((4 * NT, width), f32),
            dma((tm_n,)), dma((tm_n,)), dma((tm_n,)), dma((tm_n,)),
            dma((3,)), dma((3, tm_n)),
            dma((n, 4)), dma((n, 4)),
            dma((n, half)), dma((n, half)),
            dma((5,)),
        ],
        compiler_params=pltpu.CompilerParams(
            collective_id=0, has_side_effects=True, vmem_limit_bytes=40 * 1024 * 1024),
    )(state, far_field, face_index, face_weight, mean_flow)


def skew_part(o, coef):
    half = len(o)
    quarter = half // 2

    def at(n):
        return o[n % half], -1.0 if (n // half) % 2 else 1.0

    res = []
    for n in range(half):
        total = None
        for m in range(1, quarter):
            (a, sa), (b, sb) = at(n - m), at(n + m)
            term = (coef[m] * sa) * (a - b if sa == sb else a + b)
            total = term if total is None else total + term
        a, sa = at(n - quarter)
        term = (coef[quarter] * sa) * a
        res.append(term if total is None else total + term)
    return res


def cyclic_part(e, coef):
    half = len(e)
    res = []
    for n in range(half):
        total = None
        for m in range(1, half // 2):
            term = coef[m] * (e[(n - m) % half] - e[(n + m) % half])
            total = term if total is None else total + term
        res.append(total)
    return res


def time_term_split(q, even, odd):
    half = len(q) // 2
    quarter = half // 2
    e = [q[n] + q[n + half] for n in range(half)]
    o = [q[n] - q[n + half] for n in range(half)]
    ee = [e[n] + e[n + quarter] for n in range(quarter)]
    eo = [e[n] - e[n + quarter] for n in range(quarter)]
    low = [0.0] + [0.5 * (even[m] - even[quarter - m]) for m in range(1, quarter)]
    high = [0.0] + [0.5 * (even[m] + even[quarter - m]) for m in range(1, quarter)]
    cyc = cyclic_part(ee, low)
    skw = skew_part(eo, high)
    ev = [cyc[n] + skw[n] for n in range(quarter)] + [cyc[n] - skw[n] for n in range(quarter)]
    od = skew_part(o, odd)
    return [ev[n] + od[n] for n in range(half)] + [ev[n] - od[n] for n in range(half)]


def ring_kernel(dims, state, far, fidx, fw, mf, out, q, tt, ff, wts, fi, lane_ix, blk_ix, ww, gg, fo, mfs,
                in_s, in_r, dup_s, dup_r, out_s, out_r, p_s, p_r, h_s, h_r, loc):
    tm_n, half, L, R, K = dims
    NT = tm_n * L
    G = tm_n * half
    Z = tm_n // 2
    cycle = half * 128
    nsec = len(SECTION_FACTORS)
    reach = 2 * nsec
    groups = 4 * NT // 8
    me = lax.axis_index("tm")
    blk = lax.axis_index("block")
    side = lax.div(blk, half)
    place = lax.rem(blk, half)

    def slab(t, b, sd):
        z = lax.div(t, 2)
        c = lax.rem(t, 2)
        zo = jnp.where(sd == 0, z, Z - 1 - z)
        return 4 * zo + jnp.where(lax.rem(b + zo, 2) == 0, c, 3 - c)

    def owner(g, sd):
        zo = g // 4 if isinstance(g, int) else lax.div(g, 4)
        k = g % 4 if isinstance(g, int) else lax.rem(g, 4)
        xo = jnp.where(k >= 2, 1, 0)
        c = jnp.where(k >= 2, 3 - k, k)
        b = lax.rem(xo + zo, 2)
        return 2 * jnp.where(sd == 0, zo, Z - 1 - zo) + c, b

    def device(g, sd):
        t, b = owner(g, sd)
        return {"tm": t, "block": sd * half + b}

    g = slab(me, place, side)
    here = me * half + place
    seam = g == G - 1
    mixes = seam & (side == 0)
    ends = seam & (side == 1)
    mix_dev = device(G - 1, 0)
    end_dev = device(G - 1, 1)
    dup_list = [4 * z + 3 for z in range(1, Z - 1)]

    def is_dup(x):
        hit = x < -1
        for d in dup_list:
            hit = hit | (x == d)
        return hit

    takes_dup = is_dup(g)
    feeds_prev = jnp.logical_not(is_dup(g - 1))
    prev_side = jnp.where(g == 0, 1 - side, side)
    prev_dev = device(lax.rem(g + G - 1, G), prev_side)
    next_side = jnp.where(seam, 1 - side, side)

    def peer(t):
        return lax.rem(here + 1 + t, G)

    def dev(j, sd):
        return {"tm": lax.div(j, half), "block": sd * half + lax.rem(j, half)}

    def slab_of(j):
        return slab(lax.div(j, half), lax.rem(j, half), side)

    def lev(t):
        return pl.ds(t * L, L)

    def rc(src, dst, ss, rs, to):
        return pltpu.make_async_remote_copy(src_ref=src, dst_ref=dst, send_sem=ss, recv_sem=rs,
                                            device_id=to, device_id_type=MESH)

    def gather_of(n, whole=False):
        return q.at[0, :, pl.ds(0, NT if whole else NT - L // half), :, pl.ds(0, n)]

    def received(view, sem):
        rc(view, view, p_s.at[0], sem, end_dev).wait_recv()

    def sent(view, sem):
        rc(view, view, sem, p_r.at[0], end_dev).wait_send()

    bar = pltpu.get_barrier_semaphore()

    @pl.loop(0, G - 1)
    def _(t):
        pl.semaphore_signal(bar, inc=1, device_id=dev(peer(t), side), device_id_type=MESH)

    @pl.when(seam)
    def _():
        @pl.loop(0, G)
        def _(j):
            pl.semaphore_signal(bar, inc=1, device_id=dev(j, 1 - side), device_id_type=MESH)

    @pl.when(jnp.logical_not(seam))
    def _():
        pl.semaphore_signal(bar, inc=1, device_id=device(G - 1, 1 - side), device_id_type=MESH)

    own = pltpu.make_async_copy(state.at[:, :, pl.ds(pl.multiple_of(g * R, R), R)],
                                q.at[0, place, lev(me), :, pl.ds(0, R)], loc.at[0])
    own.start()
    own_mf = pltpu.make_async_copy(mf, mfs, loc.at[4])
    own_mf.start()

    first = FIRST_ROWS
    parts = ((0, first), (first, R - first))
    ahead = ((0, first - 8), (first - 8, reach + 8 - first), (0, reach))

    def ahead_rows(d, k):
        lo, n = ahead[k]
        return state.at[:, :, pl.ds((d + 1) * R + lo, n)]

    def ahead_spot(j, k):
        lo, n = ahead[k]
        return q.at[0, lax.rem(j, half), lev(lax.div(j, half)), :, pl.ds(R + lo, n)]

    def dup_copy(i, k, j):
        return rc(ahead_rows(dup_list[i], k), ahead_spot(j, k), dup_s.at[i, k], dup_r.at[k],
                  device(dup_list[i], side))

    def own_dup(i):
        return pltpu.make_async_copy(ahead_rows(dup_list[i], 2), ahead_spot(here, 2), loc.at[5])

    def send_dup(k):
        for i, d in enumerate(dup_list):
            @pl.when(g != d)
            def _():
                dup_copy(i, k, here).start()

    for i, d in enumerate(dup_list):
        @pl.when(g == d)
        def _():
            own_dup(i).start()

    pl.semaphore_wait(bar, G + jnp.where(seam, G - 1, 0))

    def far_copy(j, sd):
        return rc(far, ff.at[sd, lax.rem(j, half), lev(lax.div(j, half))], p_s.at[0], p_r.at[0], end_dev)

    def wt_copy(j, sd):
        return rc(fw, wts.at[sd, lax.rem(j, half), lev(lax.div(j, half))], p_s.at[1], p_r.at[1], mix_dev)

    def ix_copy(j, sd):
        return rc(fidx, fi.at[sd, lax.rem(j, half), lax.div(j, half)], p_s.at[2], p_r.at[2], mix_dev)

    own_far = pltpu.make_async_copy(far, ff.at[side, place, lev(me)], loc.at[1])
    own_wt = pltpu.make_async_copy(fw, wts.at[side, place, lev(me)], loc.at[2])
    own_ix = pltpu.make_async_copy(fidx, fi.at[side, place, me], loc.at[3])

    @pl.when(ends)
    def _():
        own_far.start()

    @pl.when(jnp.logical_not(ends))
    def _():
        far_copy(here, side).start()

    @pl.when(mixes)
    def _():
        own_wt.start()
        own_ix.start()

    @pl.when(jnp.logical_not(mixes))
    def _():
        wt_copy(here, side).start()
        ix_copy(here, side).start()

    def in_copy(i, j, src):
        lo, n = parts[i]
        return rc(state.at[:, :, pl.ds(slab_of(j) * R + lo, n)],
                  q.at[0, lax.rem(src, half), lev(lax.div(src, half)), :, pl.ds(lo, n)],
                  in_s.at[i], in_r.at[i], dev(j, side))

    def send_in(i):
        @pl.loop(0, G - 1)
        def _(t):
            in_copy(i, peer(t), here).start()

    send_in(0)
    send_dup(0)
    send_in(1)
    send_dup(1)

    lane = lax.broadcasted_iota(jnp.int32, (8, 128), 1)
    sub = lax.broadcasted_iota(jnp.int32, (8, 128), 0)
    first_lane, last_lane = lane == 0, lane == 127

    @pl.when(ends)
    def _():
        own_far.wait()

        received(q.at[0, :, pl.ds(0, L // half), :, pl.ds(0, 2 * G - 1)], p_r.at[0])

        for k in range(2):
            for b in range(half):
                @pl.loop(0, NT)
                def _(l):
                    for v in range(4):
                        gg[k, b, pl.ds(4 * l + v, 1)] = ff[1 - k, b, l, pl.ds(v, 1)]

    @pl.when(mixes)
    def _():
        own_wt.wait()
        own_ix.wait()

        received(q.at[0, :, pl.ds(0, L // half), :, pl.ds(0, 2 * G - 1)], p_r.at[1])
        received(q.at[0, 0, 0, pl.ds(0, L), pl.ds(0, 2 * G - 1)], p_r.at[2])

        for r in range(2):
            for b in range(half):
                @pl.loop(0, NT // 2)
                def _(m):
                    def ix(l):
                        return jnp.broadcast_to(fi[r, b, lax.div(l, L), pl.ds(lax.rem(l, L), 1)], (8, 128))

                    def wt(l, k):
                        return jnp.broadcast_to(wts[r, b, l, pl.ds(k, 1)], (8, 128))

                    start = jnp.where(sub < 4, ix(2 * m), ix(2 * m + 1))
                    at = pl.ds(8 * m, 8)
                    for k in range(K):
                        src = start + k
                        src = jnp.where(src >= cycle, src - cycle, src)
                        lane_ix[r, k, b, at] = jnp.bitwise_and(src, 127)
                        blk_ix[r, k, b, at] = lax.shift_right_logical(src, 7)
                        ww[r, k, b, at] = jnp.where(sub < 4, wt(2 * m, k), wt(2 * m + 1, k))

    own_mf.wait()

    def speeds(sd):
        return jnp.where(sd == 0, mfs[0, 0], mfs[1, 0]), jnp.where(sd == 0, mfs[0, 1], mfs[1, 1])

    own_speed = speeds(side)
    next_speed = speeds(next_side)

    def feed(k):
        lo, n = ahead[k]
        return rc(q.at[0, :, :, :, pl.ds(lo, n)], q.at[0, :, :, :, pl.ds(R + lo, n)], h_s.at[k], h_r.at[k], prev_dev)

    def wait_ahead(k):
        @pl.when(takes_dup)
        def _():
            received(gather_of(ahead[k][1]), dup_r.at[k])

        @pl.when(jnp.logical_not(takes_dup))
        def _():
            feed(k).wait_recv()

    def time_pass(s, w):
        c = SECTION_FACTORS[s - 1]
        even, odd = split_coefficients(NT, -OMEGA * c)
        at = pl.ds(w, 8)

        @pl.loop(0, 4)
        def _(v):
            for b in range(half):
                xs = [q[s - 1, b, l, v, at] for l in range(NT)]
                terms = time_term_split(xs, even, odd)
                for l in range(NT):
                    tt[b, l, v] = (q[0, b, l, v, at] + terms[l]) - (4.0 * DISSIPATION * c) * xs[l]

    def space_pass(s, w, lo, hi):
        up_row, dn_row = w + lo <= R - 1 < w + hi, w + lo <= R < w + hi
        border = w + hi > R
        c = SECTION_FACTORS[s - 1]
        hh = 0.5 * c
        near = DISSIPATION * c

        def weights(uv):
            return near - hh * uv[0], near + hh * uv[0], near - hh * uv[1], near + hh * uv[1]

        cu, cd, cr, cl = weights(own_speed)
        if border:
            beyond = sub >= R - w
            cu, cd, cr, cl = [jnp.where(beyond, n, o) for n, o in zip(weights(next_speed), (cu, cd, cr, cl))]
        span = range(half)
        up_at = sub == jnp.where(seam, R - 1 - w, 8)
        dn_at = sub == jnp.where(seam, R - w, 8)

        def level(l):
            di = [[None] * half for _ in range(4)]
            dj = [[None] * half for _ in range(4)]
            acc = [[None] * half for _ in range(4)]
            for v in range(4):
                x = [q[s - 1, b, l, v, pl.ds(w, 8)] for b in span]
                rr = [pltpu.roll(x[b], 127, 1) for b in span]
                rl = [pltpu.roll(x[b], 1, 1) for b in span]
                for b in span:
                    up = q[s - 1, b, l, v, pl.ds(w + 1, 8)]
                    dn = q[s - 1, b, l, v, pl.ds(w - 1, 8)]
                    at = pl.ds(4 * l + v, 1)
                    if up_row:
                        up = jnp.where(up_at, jnp.broadcast_to(gg[0, b, at], (8, 128)), up)
                    if dn_row:
                        dn = jnp.where(dn_at, jnp.broadcast_to(gg[1, b, at], (8, 128)), dn)
                    right = jnp.where(last_lane, rr[(b + 1) % half], rr[b])
                    left = jnp.where(first_lane, rl[(b - 1) % half], rl[b])
                    acc[v][b] = (tt[b, l, v] + (cu * up + cd * dn)) + (cr * right + cl * left)
                    if v in (1, 3):
                        di[v][b] = up - dn
                    if v in (2, 3):
                        dj[v][b] = right - left
            for b in span:
                cross = hh * (di[1][b] + dj[2][b])
                new = [acc[0][b] - cross, acc[1][b] - hh * di[3][b], acc[2][b] - hh * dj[3][b], acc[3][b] - cross]
                for v in range(4):
                    q[s, b, l, v, pl.ds(w + lo, hi - lo)] = new[v][lo:hi]
                    for k, hit in enumerate((up_row, dn_row)):
                        if hit and s < nsec:
                            row = R - 1 + k - w
                            fo[k, b, pl.ds(4 * l + v, 1)] = new[v][row:row + 1]

        @pl.loop(0, NT // 4)
        def _(i):
            for j in range(4):
                level(4 * i + j)

    own.wait()

    received(gather_of(parts[0][1]), in_r.at[0])

    @pl.when(feeds_prev)
    def _():
        feed(0).start()
        feed(1).start()

    early = first - reach
    following = lax.rem(g + 1, G)
    takes_own = jnp.logical_not(seam)
    turn = nsec + early + 8
    spans = [(nsec, early), (nsec + early, 8), (turn, R - turn), (R, nsec)]
    spans = [(lo, n) for lo, n in spans if n > 0]
    last = len(spans) - 1
    inner = 1 if early else 0

    def result(i, j):
        lo, n = spans[i]
        return q.at[nsec, lax.rem(j, half), lev(lax.div(j, half)), :, pl.ds(lo, n)]

    def spot(i, gs):
        lo, n = spans[i]
        return out.at[:, :, pl.ds(gs * R + (lo if i < last else 0), n)]

    def out_copy(i, j, gs):
        return rc(result(i, j), spot(i, gs), out_s.at[i], out_r.at[i], dev(j, side if i < last else next_side))

    def own_out(i, gs):
        return pltpu.make_async_copy(result(i, here), spot(i, gs), loc.at[6 + i])

    def send_out(i):
        @pl.loop(0, G - 1)
        def _(t):
            out_copy(i, peer(t), g).start()

        own_out(i, g).start()

    def window(s, w, lo, hi):
        time_pass(s, w)
        space_pass(s, w, lo - w, hi - w)

    for s in range(1, nsec + 1):
        lo, hi = s, first - s
        if hi - lo > 8:
            window(s, lo, lo, lo + 8)
            window(s, hi - 8, lo + 8, hi)
        elif hi > lo:
            window(s, min(lo, first - 8 - (s == 1)), lo, hi)
    if early:
        send_out(0)

    received(gather_of(parts[1][1]), in_r.at[1])

    for i, d in enumerate(dup_list):
        @pl.when(g == d)
        def _():
            own_dup(i).wait()

    wait_ahead(0)

    @pl.when(mixes)
    def _():
        @pl.loop(0, NT)
        def _(l):
            for b in range(half):
                for v in range(4):
                    for k in range(2):
                        fo[k, b, pl.ds(4 * l + v, 1)] = q[0, b, l, v, pl.ds(R - 1 + k, 1)]

    def mix():
        @pl.when(mixes)
        def _():
            @pl.loop(0, groups)
            def _(m):
                at = pl.ds(pl.multiple_of(8 * m, 8), 8)
                for r in range(2):
                    for b in range(half):
                        total = jnp.zeros((8, 128), jnp.float32)
                        for k in range(K):
                            picked = jnp.zeros((8, 128), jnp.float32)
                            for h in range(half):
                                got = jnp.take_along_axis(fo[1 - r, h, at], lane_ix[r, k, b, at], axis=1)
                                picked = jnp.where(blk_ix[r, k, b, at] == h, got, picked)
                            total = total + ww[r, k, b, at] * picked
                        gg[r, b, at] = total

    for s in range(1, nsec + 1):
        if s <= first - 8:
            mix()
        window(s, first - s, first - s, first - s + 8)
    send_out(inner)
    wait_ahead(1)

    for s in range(1, nsec + 1):
        if s > first - 8:
            mix()
        window(s, R + 2 - s, first + 8 - s, R + reach - s)

    @pl.loop(0, G - 1)
    def _(t):
        for i in range(inner + 1, last):
            out_copy(i, peer(t), g).start()
        out_copy(last, peer(t), following).start()

    for i in range(inner + 1, last):
        own_out(i, g).start()

    @pl.when(takes_own)
    def _():
        own_out(last, following).start()

    @pl.when(seam)
    def _():
        out_copy(last, here, following).start()

    for i in range(2):
        sent(gather_of(parts[i][1]), in_s.at[i])

    for i, d in enumerate(dup_list):
        @pl.when(g != d)
        def _():
            for k in range(2):
                dup_copy(i, k, here).wait_send()

    @pl.when(feeds_prev)
    def _():
        feed(0).wait_send()
        feed(1).wait_send()

    @pl.when(jnp.logical_not(ends))
    def _():
        far_copy(here, side).wait_send()

    @pl.when(jnp.logical_not(mixes))
    def _():
        wt_copy(here, side).wait_send()
        ix_copy(here, side).wait_send()

    for i in range(last):
        own_out(i, g).wait()
        sent(gather_of(spans[i][1]), out_s.at[i])
        received(gather_of(spans[i][1]), out_r.at[i])

    @pl.when(takes_own)
    def _():
        own_out(last, following).wait()
        sent(gather_of(nsec), out_s.at[last])
        received(gather_of(nsec), out_r.at[last])

    @pl.when(seam)
    def _():
        sent(gather_of(nsec, True), out_s.at[last])
        received(gather_of(nsec, True), out_r.at[last])


def ring_shards(dims, state, far_field, face_index, face_weight, mean_flow):
    tm_n, half = dims
    L, _, rows, width = state.shape
    K = face_weight.shape[1]
    G = tm_n * half
    R = rows // G
    NT = L * tm_n
    n = len(SECTION_FACTORS)
    f32 = jnp.float32
    hbm = pl.BlockSpec(memory_space=pl.ANY)
    dma = pltpu.SemaphoreType.DMA
    V = pltpu.VMEM
    args = [pltpu.with_memory_space_constraint(a, pltpu.HBM)
            for a in (state, far_field, face_index, face_weight, mean_flow)]
    return pl.pallas_call(
        functools.partial(ring_kernel, (tm_n, half, L, R, K)),
        out_shape=jax.ShapeDtypeStruct(state.shape, f32),
        in_specs=[hbm] * 5,
        out_specs=hbm,
        scratch_shapes=[
            V((n + 1, half, NT, 4, R + 16, width), f32),
            V((half, NT, 4, 8, width), f32),
            V((2, half, NT, 4, width), f32),
            V((2, half, NT, K, width), f32),
            V((2, half, tm_n, L, width), jnp.int32),
            V((2, K, half, 4 * NT, width), jnp.int32),
            V((2, K, half, 4 * NT, width), jnp.int32),
            V((2, K, half, 4 * NT, width), f32),
            V((2, half, 4 * NT, width), f32),
            V((2, half, 4 * NT, width), f32),
            pltpu.SMEM((2, 2), f32),
            dma((2,)), dma((2,)),
            dma((tm_n // 2 - 2, 2)), dma((2,)),
            dma((4,)), dma((4,)),
            dma((3,)), dma((3,)),
            dma((2,)), dma((2,)),
            dma((10,)),
        ],
        compiler_params=pltpu.CompilerParams(
            collective_id=0, has_side_effects=True, vmem_limit_bytes=48 * 1024 * 1024),
    )(*args)


def solution(mesh):
    dims = (mesh.shape["tm"], mesh.shape["block"] // 2)
    in_specs = (
        P("tm", None, None, "block"),
        P("tm", None, "block"),
        P("tm", "block"),
        P("tm", None, "block"),
        P(),
    )
    out_specs = P("tm", None, None, "block")

    def body(state, *rest):
        tm_n, half = dims
        fits = (half == 2 and tm_n in (6, 8) and state.shape[0] % 2 == 0 and state.shape[0] * tm_n % 8 == 0
                and rest[2].shape[1] == 4 and state.shape[2] == 16 * tm_n * half and state.shape[3] == 128)
        return (ring_shards if fits else shards)(dims, state, *rest)

    return jax.shard_map(body, mesh=mesh, in_specs=in_specs, out_specs=out_specs, check_vma=False)
```

```python
import functools
import math

import jax
import jax.numpy as jnp
from jax import lax
from jax.experimental import pallas as pl
from jax.experimental.pallas import tpu as pltpu
from jax.sharding import PartitionSpec as P

SECTION_FACTORS = (0.075, 0.05, 0.1125, 0.15, 0.3)
OMEGA = 1.0
DISSIPATION = 0.2
PAD = 8
FIRST_ROWS = 13
MESH = pl.DeviceIdType.MESH


def split_coefficients(count, scale):
    half = count // 2
    d = [0.0] + [0.5 * (-1) ** k / math.tan(math.pi * k / count) for k in range(1, half)] + [0.0]
    even = [0.5 * scale * (d[m] - d[half - m]) for m in range(half)]
    odd = [0.5 * scale * (d[m] + d[half - m]) for m in range(half)]
    even[0] = odd[0] = 0.0
    return even, odd


def time_term(q, even, odd):
    half = len(q) // 2
    quarter = half // 2
    e = [q[n] + q[n + half] for n in range(half)]
    o = [q[n] - q[n + half] for n in range(half)]

    def odd_at(n):
        return (o[n % half], -1.0 if (n // half) % 2 else 1.0)

    low, high = [], []
    for n in range(half):
        ev = None
        od = None
        for m in range(1, quarter):
            term = even[m] * (e[(n - m) % half] - e[(n + m) % half])
            ev = term if ev is None else ev + term
            (a, sa), (b, sb) = odd_at(n - m), odd_at(n + m)
            pair = a - b if sa == sb else a + b
            term = (odd[m] * sa) * pair
            od = term if od is None else od + term
        a, sa = odd_at(n - quarter)
        od = od + (odd[quarter] * sa) * a
        low.append(ev + od)
        high.append(ev - od)
    return low + high


def kernel(dims, state, far, fidx, fw, mf, out, x0, qa, qb, ef, el, rl, ru, cs, cl, cu,
           face, ff, wts, fi, lane_ix, blk_ix, ww, gh,
           in_s, in_r, out_s, out_r, p_s, p_r, h_s, h_r, f_s, f_r, loc):
    tm_n, half, L, R, K = dims
    NT = tm_n * L
    cycle = half * 128
    tiles = R // 8
    nsec = len(SECTION_FACTORS)
    me = lax.axis_index("tm")
    blk = lax.axis_index("block")
    side = lax.div(blk, half)
    place = lax.rem(blk, half)
    row0 = side * half
    lower_b = row0 + lax.rem(place + half - 1, half)
    upper_b = row0 + lax.rem(place + 1, half)
    other0 = (1 - side) * half
    step = 1 - 2 * side
    is_last = me == tm_n - 1
    is_far = me == 0
    rchunk = side * (tm_n - 1) + step * me
    has_lower = rchunk > 0
    has_upper = rchunk < tm_n - 1
    ghost_row = jnp.where(side == 0, PAD + R, PAD - 1)
    far_row = jnp.where(side == 0, PAD - 1, PAD + R)

    def rc(src, dst, ss, rs, dev):
        return pltpu.make_async_remote_copy(src_ref=src, dst_ref=dst, send_sem=ss, recv_sem=rs,
                                            device_id=dev, device_id_type=MESH)

    def rows(p):
        return pl.ds(pl.multiple_of((side * (tm_n - 1) + step * p) * R, R), R)

    def lev(p):
        return pl.ds(p * L, L)

    def peer(t):
        return lax.rem(me + 1 + t, tm_n)

    bar = pltpu.get_barrier_semaphore()

    @pl.loop(0, tm_n - 1)
    def _(t):
        pl.semaphore_signal(bar, inc=1, device_id={"tm": peer(t)}, device_id_type=MESH)

    pl.semaphore_signal(bar, inc=1, device_id={"block": lower_b}, device_id_type=MESH)
    pl.semaphore_signal(bar, inc=1, device_id={"block": upper_b}, device_id_type=MESH)

    @pl.when(is_last)
    def _():
        for h in range(half):
            pl.semaphore_signal(bar, inc=1, device_id={"block": other0 + h}, device_id_type=MESH)

    own = pltpu.make_async_copy(state.at[:, :, rows(me)], x0.at[lev(me)], loc.at[0])
    own.start()
    pl.semaphore_wait(bar, tm_n + 1 + jnp.where(is_last, half, 0))

    def in_copy(p, src_tm):
        return rc(state.at[:, :, rows(p)], x0.at[lev(src_tm)], in_s.at[p], in_r.at[src_tm], {"tm": p})

    @pl.loop(0, tm_n - 1)
    def _(t):
        p = peer(t)
        in_copy(p, me).start()

    def far_copy(src_tm):
        return rc(far, ff.at[lev(src_tm)], p_s.at[0], p_r.at[0, src_tm], {"tm": 0})

    def wt_copy(src_tm):
        return rc(fw, wts.at[lev(src_tm)], p_s.at[1], p_r.at[1, src_tm], {"tm": tm_n - 1})

    def ix_copy(src_tm):
        return rc(fidx, fi.at[src_tm], p_s.at[2], p_r.at[2, src_tm], {"tm": tm_n - 1})

    own_far = pltpu.make_async_copy(far, ff.at[lev(me)], loc.at[1])
    own_wt = pltpu.make_async_copy(fw, wts.at[lev(me)], loc.at[2])
    own_ix = pltpu.make_async_copy(fidx, fi.at[me], loc.at[3])

    @pl.when(is_far)
    def _():
        own_far.start()

    @pl.when(jnp.logical_not(is_far))
    def _():
        far_copy(me).start()

    @pl.when(is_last)
    def _():
        own_wt.start()
        own_ix.start()

    @pl.when(jnp.logical_not(is_last))
    def _():
        wt_copy(me).start()
        ix_copy(me).start()

    lane = lax.broadcasted_iota(jnp.int32, (8, 128), 1)
    lane_pair = jnp.bitwise_or(lane, 1)
    sub = lax.broadcasted_iota(jnp.int32, (8, 128), 0)

    def pack(acc, value, k):
        return jnp.where(lane_pair == k, pltpu.roll(value, k, 1), acc)

    def key(l, v):
        return 2 * (4 * l + v) + 1

    def halo_copies(s):
        low = rc(ef.at[s], ru.at[s], h_s.at[s, 0], h_r.at[s, 0], {"tm": me - step})
        up = rc(el.at[s], rl.at[s], h_s.at[s, 1], h_r.at[s, 1], {"tm": me + step})
        jl = rc(cs.at[s], cu.at[s], h_s.at[s, 2], h_r.at[s, 2], {"block": lower_b})
        ju = rc(cs.at[s], cl.at[s], h_s.at[s, 3], h_r.at[s, 3], {"block": upper_b})
        return low, up, jl, ju

    def face_copy(s, h, edge):
        return rc(edge.at[s], face.at[s, place], f_s.at[s, h], f_r.at[s, place], {"block": other0 + h})

    def face_wait(s, h):
        return rc(ef.at[s], face.at[s, h], f_s.at[s, h], f_r.at[s, h], {"block": other0 + h})

    def send_halos(s):
        low, up, jl, ju = halo_copies(s)

        @pl.when(is_last & (side == 0))
        def _():
            for h in range(half):
                face_copy(s, h, el).start()

        @pl.when(is_last & (side == 1))
        def _():
            for h in range(half):
                face_copy(s, h, ef).start()

        @pl.when(has_lower)
        def _():
            low.start()

        @pl.when(has_upper)
        def _():
            up.start()

        jl.start()
        ju.start()

    def take_level(l, accs):
        accs = list(accs)
        for v in range(4):
            for a in range(tiles):
                value = x0[l, v, pl.ds(8 * a, 8)]
                qa[l, v, pl.ds(PAD + 8 * a, 8)] = value
                accs[a] = pack(accs[a], value, key(l, v))
                if a == 0:
                    ef[0, pl.ds(4 * l + v, 1)] = value[0:1]
                if a == tiles - 1:
                    el[0, pl.ds(4 * l + v, 1)] = value[7:8]
        return tuple(accs)

    own.wait()
    accs = tuple(jnp.zeros((8, 128), jnp.float32) for _ in range(tiles))
    accs = lax.fori_loop(0, L, lambda j, c: take_level(me * L + j, c), accs)

    def arrive(t, c):
        p = peer(tm_n - 2 - t)
        in_copy(p, p).wait_recv()
        return lax.fori_loop(0, L, lambda j, d: take_level(p * L + j, d), c)

    accs = lax.fori_loop(0, tm_n - 1, arrive, accs)
    for a in range(tiles):
        cs[0, pl.ds(8 * a, 8)] = accs[a]
    send_halos(0)

    @pl.when(is_far)
    def _():
        own_far.wait()

        @pl.loop(1, tm_n)
        def _(p):
            far_copy(p).wait_recv()

        @pl.loop(0, NT)
        def _(l):
            for v in range(4):
                row = ff[l, pl.ds(v, 1)]
                qa[l, v, pl.ds(far_row, 1)] = row
                qb[l, v, pl.ds(far_row, 1)] = row

    @pl.when(is_last)
    def _():
        own_wt.wait()
        own_ix.wait()

        @pl.loop(0, tm_n - 1)
        def _(p):
            wt_copy(p).wait_recv()
            ix_copy(p).wait_recv()

        @pl.loop(0, NT // 2)
        def _(m):
            def ix(l):
                return jnp.broadcast_to(fi[lax.div(l, L), pl.ds(lax.rem(l, L), 1)], (8, 128))

            def wt(l, k):
                return jnp.broadcast_to(wts[l, pl.ds(k, 1)], (8, 128))

            start = jnp.where(sub < 4, ix(2 * m), ix(2 * m + 1))
            at = pl.ds(8 * m, 8)
            for k in range(K):
                src = start + k
                src = jnp.where(src >= cycle, src - cycle, src)
                lane_ix[k, at] = jnp.bitwise_and(src, 127)
                blk_ix[k, at] = lax.shift_right_logical(src, 7)
                ww[k, at] = jnp.where(sub < 4, wt(2 * m, k), wt(2 * m + 1, k))

    speed_u = jnp.where(side == 0, mf[0, 0], mf[1, 0])
    speed_v = jnp.where(side == 0, mf[0, 1], mf[1, 1])
    odd_lane = jnp.bitwise_and(lane, 1) == 1
    edge_lane = {0: lane == 0, 127: lane == 127}

    def install(dst, src, at):
        @pl.loop(0, NT)
        def _(l):
            for v in range(4):
                dst[l, v, pl.ds(at, 1)] = src[pl.ds(4 * l + v, 1)]

    def out_copy(q, p, src_tm):
        return rc(q.at[lev(p), :, pl.ds(PAD, R)], out.at[:, :, rows(src_tm)],
                  out_s.at[p], out_r.at[src_tm], {"tm": p})

    for s, factor in enumerate(SECTION_FACTORS):
        q, nq = (qa, qb) if s % 2 == 0 else (qb, qa)
        final = s == nsec - 1
        even, odd = split_coefficients(NT, OMEGA * factor)
        hu, hv, hh = (0.5 * factor) * speed_u, (0.5 * factor) * speed_v, 0.5 * factor

        @pl.loop(0, 4)
        def _(v):
            @pl.loop(0, tiles)
            def _(a):
                at = pl.ds(pl.multiple_of(PAD + 8 * a, 8), 8)
                xs = [q[l, v, at] for l in range(NT)]
                terms = time_term(xs, even, odd)
                for l in range(NT):
                    first = x0[l, v, pl.ds(pl.multiple_of(8 * a, 8), 8)]
                    nq[l, v, at] = first - (terms[l] + (4.0 * DISSIPATION * factor) * xs[l])

        low, up, jl, ju = halo_copies(s)
        jl.wait_recv()
        ju.wait_recv()
        mixed = []
        for a in range(tiles):
            at = pl.ds(8 * a, 8)
            mixed.append(jnp.where(odd_lane, pltpu.roll(cl[s, at], 1, 1), pltpu.roll(cu[s, at], 127, 1)))

        def level(l, accs, which):
            accs = list(accs)
            for slot, a in enumerate(which):
                base = PAD + 8 * a
                di, dj, near = [], [], []
                for v in range(4):
                    x = q[l, v, pl.ds(base, 8)]
                    upx = q[l, v, pl.ds(base + 1, 8)]
                    dnx = q[l, v, pl.ds(base - 1, 8)]
                    border = pltpu.roll(mixed[a], 128 - key(l, v), 1)
                    left = jnp.where(edge_lane[0], border, pltpu.roll(x, 1, 1))
                    right = jnp.where(edge_lane[127], border, pltpu.roll(x, 127, 1))
                    di.append(upx - dnx)
                    dj.append(right - left)
                    near.append((DISSIPATION * factor) * ((upx + dnx) + (right + left)))
                flux = [
                    hu * di[0] + hv * dj[0] + hh * (di[1] + dj[2]),
                    hu * di[1] + hv * dj[1] + hh * di[3],
                    hu * di[2] + hv * dj[2] + hh * dj[3],
                    hu * di[3] + hv * dj[3] + hh * (di[1] + dj[2]),
                ]
                for v in range(4):
                    new = nq[l, v, pl.ds(base, 8)] + (near[v] - flux[v])
                    nq[l, v, pl.ds(base, 8)] = new
                    if not final:
                        accs[slot] = pack(accs[slot], new, key(l, v))
                        if a == 0:
                            ef[s + 1, pl.ds(4 * l + v, 1)] = new[0:1]
                        if a == tiles - 1:
                            el[s + 1, pl.ds(4 * l + v, 1)] = new[7:8]
            return tuple(accs)

        def sweep(which):
            zero = tuple(jnp.zeros((8, 128), jnp.float32) for _ in which)
            step_by = 4 if NT % 4 == 0 else 1

            def several(g, c):
                for j in range(step_by):
                    c = level(step_by * g + j, c, which)
                return c

            accs = lax.fori_loop(0, NT // step_by, several, zero)
            if not final:
                for slot, a in enumerate(which):
                    cs[s + 1, pl.ds(8 * a, 8)] = accs[slot]

        inner = tuple(range(1, tiles - 1))
        outer = tuple(sorted({0, tiles - 1}))
        if inner:
            sweep(inner)

        @pl.when(has_lower)
        def _():
            up.wait_recv()
            install(q, rl.at[s], PAD - 1)

        @pl.when(has_upper)
        def _():
            low.wait_recv()
            install(q, ru.at[s], PAD + R)

        @pl.when(is_last)
        def _():
            for h in range(half):
                face_wait(s, h).wait_recv()

            @pl.loop(0, NT // 2)
            def _(m):
                at = pl.ds(8 * m, 8)
                total = jnp.zeros((8, 128), jnp.float32)
                for k in range(K):
                    picked = jnp.zeros((8, 128), jnp.float32)
                    for h in range(half):
                        got = jnp.take_along_axis(face[s, h, at], lane_ix[k, at], axis=1)
                        picked = jnp.where(blk_ix[k, at] == h, got, picked)
                    total = total + ww[k, at] * picked
                gh[at] = total

            install(q, gh, ghost_row)

        if not final:
            sweep(outer)
            send_halos(s + 1)
        else:
            def finish(t, c):
                p = peer(t)
                for j in range(L):
                    level(p * L + j, (None,) * len(outer), outer)

                @pl.when(t < tm_n - 1)
                def _():
                    out_copy(nq, p, me).start()

                return c

            lax.fori_loop(0, tm_n, finish, 0)
            own_out = pltpu.make_async_copy(nq.at[lev(me), :, pl.ds(PAD, R)], out.at[:, :, rows(me)], loc.at[4])
            own_out.start()

            @pl.loop(0, tm_n - 1)
            def _(t):
                p = peer(t)
                out_copy(nq, p, p).wait_recv()

            own_out.wait()

            @pl.loop(0, tm_n - 1)
            def _(t):
                p = peer(t)
                out_copy(nq, p, me).wait_send()

    @pl.loop(0, tm_n - 1)
    def _(t):
        p = peer(t)
        in_copy(p, me).wait_send()

    @pl.when(jnp.logical_not(is_far))
    def _():
        far_copy(me).wait_send()

    @pl.when(jnp.logical_not(is_last))
    def _():
        wt_copy(me).wait_send()
        ix_copy(me).wait_send()

    for s in range(nsec):
        low, up, jl, ju = halo_copies(s)

        @pl.when(has_lower)
        def _():
            low.wait_send()

        @pl.when(has_upper)
        def _():
            up.wait_send()

        jl.wait_send()
        ju.wait_send()

        @pl.when(is_last)
        def _():
            for h in range(half):
                face_wait(s, h).wait_send()


def shards(dims, state, far_field, face_index, face_weight, mean_flow):
    tm_n, half = dims
    L, _, rows, width = state.shape
    K = face_weight.shape[1]
    R = rows // tm_n
    NT = L * tm_n
    assert width == 128 and NT % 4 == 0 and R % 8 == 0 and 8 * NT <= width
    n = len(SECTION_FACTORS)
    f32 = jnp.float32
    hbm = pl.BlockSpec(memory_space=pl.ANY)
    dma = pltpu.SemaphoreType.DMA
    V = pltpu.VMEM
    return pl.pallas_call(
        functools.partial(kernel, (tm_n, half, L, R, K)),
        out_shape=jax.ShapeDtypeStruct(state.shape, f32),
        in_specs=[hbm, hbm, hbm, hbm, pl.BlockSpec(memory_space=pltpu.SMEM)],
        out_specs=hbm,
        scratch_shapes=[
            V((NT, 4, R, width), f32),
            V((NT, 4, R + 2 * PAD, width), f32),
            V((NT, 4, R + 2 * PAD, width), f32),
            V((n, 4 * NT, width), f32),
            V((n, 4 * NT, width), f32),
            V((n, 4 * NT, width), f32),
            V((n, 4 * NT, width), f32),
            V((n, R, width), f32),
            V((n, R, width), f32),
            V((n, R, width), f32),
            V((n, half, 4 * NT, width), f32),
            V((NT, 4, width), f32),
            V((NT, K, width), f32),
            V((tm_n, L, width), jnp.int32),
            V((K, 4 * NT, width), jnp.int32),
            V((K, 4 * NT, width), jnp.int32),
            V((K, 4 * NT, width), f32),
            V((4 * NT, width), f32),
            dma((tm_n,)), dma((tm_n,)), dma((tm_n,)), dma((tm_n,)),
            dma((3,)), dma((3, tm_n)),
            dma((n, 4)), dma((n, 4)),
            dma((n, half)), dma((n, half)),
            dma((5,)),
        ],
        compiler_params=pltpu.CompilerParams(
            collective_id=0, has_side_effects=True, vmem_limit_bytes=40 * 1024 * 1024),
    )(state, far_field, face_index, face_weight, mean_flow)


def skew_part(o, coef):
    half = len(o)
    quarter = half // 2

    def at(n):
        return o[n % half], -1.0 if (n // half) % 2 else 1.0

    res = []
    for n in range(half):
        total = None
        for m in range(1, quarter):
            (a, sa), (b, sb) = at(n - m), at(n + m)
            term = (coef[m] * sa) * (a - b if sa == sb else a + b)
            total = term if total is None else total + term
        a, sa = at(n - quarter)
        term = (coef[quarter] * sa) * a
        res.append(term if total is None else total + term)
    return res


def cyclic_part(e, coef):
    half = len(e)
    res = []
    for n in range(half):
        total = None
        for m in range(1, half // 2):
            term = coef[m] * (e[(n - m) % half] - e[(n + m) % half])
            total = term if total is None else total + term
        res.append(total)
    return res


def time_term_split(q, even, odd):
    half = len(q) // 2
    quarter = half // 2
    e = [q[n] + q[n + half] for n in range(half)]
    o = [q[n] - q[n + half] for n in range(half)]
    ee = [e[n] + e[n + quarter] for n in range(quarter)]
    eo = [e[n] - e[n + quarter] for n in range(quarter)]
    low = [0.0] + [0.5 * (even[m] - even[quarter - m]) for m in range(1, quarter)]
    high = [0.0] + [0.5 * (even[m] + even[quarter - m]) for m in range(1, quarter)]
    cyc = cyclic_part(ee, low)
    skw = skew_part(eo, high)
    ev = [cyc[n] + skw[n] for n in range(quarter)] + [cyc[n] - skw[n] for n in range(quarter)]
    od = skew_part(o, odd)
    return [ev[n] + od[n] for n in range(half)] + [ev[n] - od[n] for n in range(half)]


def ring_kernel(dims, state, far, fidx, fw, mf, out, q, tt, dd, ff, wts, fi, lane_ix, blk_ix, ww, gg, fo, mfs,
                info, in_s, in_r, dup_s, dup_r, out_s, out_r, p_s, p_r, h_s, h_r, loc):
    tm_n, half, L, R, K = dims
    NT = tm_n * L
    G = tm_n * half
    Z = tm_n // 2
    cycle = half * 128
    nsec = len(SECTION_FACTORS)
    reach = 2 * nsec
    groups = 4 * NT // 8
    me = lax.axis_index("tm")
    blk = lax.axis_index("block")
    side = lax.div(blk, half)
    place = lax.rem(blk, half)

    def slab(t, b, sd):
        z = lax.div(t, 2)
        c = lax.rem(t, 2)
        zo = jnp.where(sd == 0, z, Z - 1 - z)
        return 4 * zo + jnp.where(lax.rem(b + zo, 2) == 0, c, 3 - c)

    def owner(g, sd):
        zo = g // 4 if isinstance(g, int) else lax.div(g, 4)
        k = g % 4 if isinstance(g, int) else lax.rem(g, 4)
        xo = jnp.where(k >= 2, 1, 0)
        c = jnp.where(k >= 2, 3 - k, k)
        b = lax.rem(xo + zo, 2)
        return 2 * jnp.where(sd == 0, zo, Z - 1 - zo) + c, b

    def device(g, sd):
        t, b = owner(g, sd)
        return {"tm": t, "block": sd * half + b}

    g = slab(me, place, side)
    here = me * half + place
    seam = g == G - 1
    mixes = seam & (side == 0)
    ends = seam & (side == 1)
    mix_dev = device(G - 1, 0)
    end_dev = device(G - 1, 1)
    dup_list = [4 * z + 3 for z in range(1, Z - 1)]

    def is_dup(x):
        hit = x < -1
        for d in dup_list:
            hit = hit | (x == d)
        return hit

    takes_dup = is_dup(g)
    feeds_prev = jnp.logical_not(is_dup(g - 1))
    prev_side = jnp.where(g == 0, 1 - side, side)
    prev_dev = device(lax.rem(g + G - 1, G), prev_side)
    next_side = jnp.where(seam, 1 - side, side)

    def peer(t):
        return lax.rem(here + 1 + t, G)

    def dev(j, sd):
        return {"tm": lax.div(j, half), "block": sd * half + lax.rem(j, half)}

    def slab_of(j):
        return slab(lax.div(j, half), lax.rem(j, half), side)

    def lev(t):
        return pl.ds(t * L, L)

    def rc(src, dst, ss, rs, to):
        return pltpu.make_async_remote_copy(src_ref=src, dst_ref=dst, send_sem=ss, recv_sem=rs,
                                            device_id=to, device_id_type=MESH)

    def gather_of(n, whole=False):
        return q[0].at[:, pl.ds(0, NT if whole else NT - L // half), :, pl.ds(0, n)]

    def received(view, sem):
        rc(view, view, p_s.at[0], sem, end_dev).wait_recv()

    def sent(view, sem):
        rc(view, view, sem, p_r.at[0], end_dev).wait_send()

    z = lax.div(me, 2)

    def near(j):
        return jnp.abs(lax.div(lax.div(j, half), 2) - z) <= 1

    partner = {"block": (1 - side) * half + place}
    bar = pltpu.get_barrier_semaphore()

    @pl.loop(0, G - 1)
    def _(t):
        @pl.when(near(peer(t)))
        def _():
            pl.semaphore_signal(bar, inc=1, device_id=dev(peer(t), side), device_id_type=MESH)

    pl.semaphore_signal(bar, inc=1, device_id=partner, device_id_type=MESH)

    own = pltpu.make_async_copy(state.at[:, :, pl.ds(pl.multiple_of(g * R, R), R)],
                                q[0].at[place, lev(me), :, pl.ds(0, R)], loc.at[0])
    own.start()
    own_mf = pltpu.make_async_copy(mf, mfs, loc.at[4])
    own_mf.start()

    first = FIRST_ROWS
    ahead = ((0, first - 8), (first - 8, reach + 8 - first), (0, reach))

    def ahead_rows(d, k):
        lo, n = ahead[k]
        return state.at[:, :, pl.ds((d + 1) * R + lo, n)]

    def ahead_spot(j, k):
        lo, n = ahead[k]
        return q[0].at[lax.rem(j, half), lev(lax.div(j, half)), :, pl.ds(R + lo, n)]

    def dup_copy(i, k, j):
        return rc(ahead_rows(dup_list[i], k), ahead_spot(j, k), dup_s.at[i, k], dup_r.at[k],
                  device(dup_list[i], side))

    def own_dup(i):
        return pltpu.make_async_copy(ahead_rows(dup_list[i], 2), ahead_spot(here, 2), loc.at[5])

    def send_dup(k):
        for i, d in enumerate(dup_list):
            @pl.when(g != d)
            def _():
                dup_copy(i, k, here).start()

    for i, d in enumerate(dup_list):
        @pl.when(g == d)
        def _():
            own_dup(i).start()

    pl.semaphore_wait(bar, 2 * half * (1 + jnp.where(z > 0, 1, 0) + jnp.where(z < Z - 1, 1, 0)))

    parts = ((0, first), (first, R - first))

    def in_copy(i, j, src):
        lo, n = parts[i]
        return rc(state.at[:, :, pl.ds(slab_of(j) * R + lo, n)],
                  q[0].at[lax.rem(src, half), lev(lax.div(src, half)), :, pl.ds(lo, n)],
                  in_s.at[i], in_r.at[i], dev(j, side))

    def send_in(i, which=None):
        @pl.loop(0, G - 1)
        def _(t):
            if which is None:
                in_copy(i, peer(t), here).start()
            else:
                @pl.when(near(peer(t)) == which)
                def _():
                    in_copy(i, peer(t), here).start()

    send_in(0, True)

    for r in range(1, Z - 1):
        @pl.when((z >= 1) & (z + r <= Z - 1))
        def _():
            pl.semaphore_signal(info.at[r], inc=1, device_id={"tm": me - 2}, device_id_type=MESH)

        @pl.when((z <= Z - 2) & (z - r >= 0))
        def _():
            pl.semaphore_signal(info.at[Z + r], inc=1, device_id={"tm": me + 2}, device_id_type=MESH)

        @pl.when(z + r + 1 <= Z - 1)
        def _():
            pl.semaphore_wait(info.at[r], 1)

        @pl.when(z - r - 1 >= 0)
        def _():
            pl.semaphore_wait(info.at[Z + r], 1)

    send_in(0, False)
    pl.semaphore_signal(info.at[0], inc=1, device_id=partner, device_id_type=MESH)
    pl.semaphore_wait(info.at[0], 1)

    def far_copy(j, sd):
        return rc(far, ff.at[sd, lax.rem(j, half), lev(lax.div(j, half))], p_s.at[0], p_r.at[0], end_dev)

    def wt_copy(j, sd):
        return rc(fw, wts.at[sd, lax.rem(j, half), lev(lax.div(j, half))], p_s.at[1], p_r.at[1], mix_dev)

    def ix_copy(j, sd):
        return rc(fidx, fi.at[sd, lax.rem(j, half), lax.div(j, half)], p_s.at[2], p_r.at[2], mix_dev)

    own_far = pltpu.make_async_copy(far, ff.at[side, place, lev(me)], loc.at[1])
    own_wt = pltpu.make_async_copy(fw, wts.at[side, place, lev(me)], loc.at[2])
    own_ix = pltpu.make_async_copy(fidx, fi.at[side, place, me], loc.at[3])

    @pl.when(ends)
    def _():
        own_far.start()

    @pl.when(jnp.logical_not(ends))
    def _():
        far_copy(here, side).start()

    @pl.when(mixes)
    def _():
        own_wt.start()
        own_ix.start()

    @pl.when(jnp.logical_not(mixes))
    def _():
        wt_copy(here, side).start()
        ix_copy(here, side).start()

    send_dup(0)
    send_in(1)
    send_dup(1)

    lane = lax.broadcasted_iota(jnp.int32, (8, 128), 1)
    sub = lax.broadcasted_iota(jnp.int32, (8, 128), 0)
    first_lane, last_lane = lane == 0, lane == 127

    @pl.when(ends)
    def _():
        own_far.wait()

        received(q[0].at[:, pl.ds(0, L // half), :, pl.ds(0, 2 * G - 1)], p_r.at[0])

        for k in range(2):
            for b in range(half):
                @pl.loop(0, NT)
                def _(l):
                    for v in range(4):
                        gg[k, b, pl.ds(4 * l + v, 1)] = ff[1 - k, b, l, pl.ds(v, 1)]

    @pl.when(mixes)
    def _():
        own_wt.wait()
        own_ix.wait()

        received(q[0].at[:, pl.ds(0, L // half), :, pl.ds(0, 2 * G - 1)], p_r.at[1])
        received(q[0].at[0, 0, pl.ds(0, L), pl.ds(0, 2 * G - 1)], p_r.at[2])

        for r in range(2):
            for b in range(half):
                @pl.loop(0, NT // 2)
                def _(m):
                    def ix(l):
                        return jnp.broadcast_to(fi[r, b, lax.div(l, L), pl.ds(lax.rem(l, L), 1)], (8, 128))

                    def wt(l, k):
                        return jnp.broadcast_to(wts[r, b, l, pl.ds(k, 1)], (8, 128))

                    start = jnp.where(sub < 4, ix(2 * m), ix(2 * m + 1))
                    at = pl.ds(8 * m, 8)
                    for k in range(K):
                        src = start + k
                        src = jnp.where(src >= cycle, src - cycle, src)
                        lane_ix[r, k, b, at] = jnp.bitwise_and(src, 127)
                        blk_ix[r, k, b, at] = lax.shift_right_logical(src, 7)
                        ww[r, k, b, at] = jnp.where(sub < 4, wt(2 * m, k), wt(2 * m + 1, k))

    own_mf.wait()

    def speeds(sd):
        return jnp.where(sd == 0, mfs[0, 0], mfs[1, 0]), jnp.where(sd == 0, mfs[0, 1], mfs[1, 1])

    own_speed = speeds(side)
    next_speed = speeds(next_side)

    def feed(k):
        lo, n = ahead[k]
        return rc(q[0].at[:, :, :, pl.ds(lo, n)], q[0].at[:, :, :, pl.ds(R + lo, n)], h_s.at[k], h_r.at[k], prev_dev)

    def wait_ahead(k):
        @pl.when(takes_dup)
        def _():
            received(gather_of(ahead[k][1]), dup_r.at[k])

        @pl.when(jnp.logical_not(takes_dup))
        def _():
            feed(k).wait_recv()

    span = range(half)

    def window(s, w, lo, hi):
        old, new = q[s - 1], q[s]
        c = SECTION_FACTORS[s - 1]
        even, odd = split_coefficients(NT, -OMEGA * c)
        at = pl.ds(w, 8)
        up_row, dn_row = lo <= R - 1 < hi, lo <= R < hi
        hh = 0.5 * c
        near = DISSIPATION * c

        def weights(uv):
            return near - hh * uv[0], near + hh * uv[0], near - hh * uv[1], near + hh * uv[1]

        cu, cd, cr, cl = weights(own_speed)
        if hi > R:
            beyond = sub >= R - w
            cu, cd, cr, cl = [jnp.where(beyond, n, o) for n, o in zip(weights(next_speed), (cu, cd, cr, cl))]
        up_at = sub == jnp.where(seam, R - 1 - w, 8)
        dn_at = sub == jnp.where(seam, R - w, 8)

        @pl.loop(0, 4)
        def _(v):
            for b in span:
                xs = [old[b, l, v, at] for l in range(NT)]
                terms = time_term_split(xs, even, odd)
                for l in range(NT):
                    tt[b, l, v] = (q[0][b, l, v, at] + terms[l]) - (4.0 * DISSIPATION * c) * xs[l]
            for l in range(NT):
                x = [old[b, l, v, at] for b in span]
                rr = [pltpu.roll(x[b], 127, 1) for b in span]
                rl = [pltpu.roll(x[b], 1, 1) for b in span]
                for b in span:
                    up = old[b, l, v, pl.ds(w + 1, 8)]
                    dn = old[b, l, v, pl.ds(w - 1, 8)]
                    row = pl.ds(4 * l + v, 1)
                    if up_row:
                        up = jnp.where(up_at, jnp.broadcast_to(gg[0, b, row], (8, 128)), up)
                    if dn_row:
                        dn = jnp.where(dn_at, jnp.broadcast_to(gg[1, b, row], (8, 128)), dn)
                    right = jnp.where(last_lane, rr[(b + 1) % half], rr[b])
                    left = jnp.where(first_lane, rl[(b - 1) % half], rl[b])
                    tt[b, l, v] = (tt[b, l, v] + (cu * up + cd * dn)) + (cr * right + cl * left)
                    dd[0, b, l, v] = hh * (up - dn)
                    dd[1, b, l, v] = hh * (right - left)

        @pl.loop(0, NT // 4)
        def _(i):
            for j in range(4):
                l = 4 * i + j
                for b in span:
                    cross = dd[0, b, l, 1] + dd[1, b, l, 2]
                    drop = [cross, dd[0, b, l, 3], dd[1, b, l, 3], cross]
                    for v in range(4):
                        value = tt[b, l, v] - drop[v]
                        new[b, l, v, pl.ds(lo, hi - lo)] = value[lo - w:hi - w]
                        for k, hit in enumerate((up_row, dn_row)):
                            if hit and s < nsec:
                                row = R - 1 + k - w
                                fo[k, b, pl.ds(4 * l + v, 1)] = value[row:row + 1]

    own.wait()

    received(gather_of(parts[0][1]), in_r.at[0])

    @pl.when(feeds_prev)
    def _():
        feed(0).start()
        feed(1).start()

    early = first - reach
    following = lax.rem(g + 1, G)
    takes_own = jnp.logical_not(seam)
    turn = nsec + early + 8
    spans = [(nsec, early), (nsec + early, 8), (turn, R - turn), (R, nsec)]
    spans = [(lo, n) for lo, n in spans if n > 0]
    last = len(spans) - 1
    inner = 1 if early else 0

    def result(i, j):
        lo, n = spans[i]
        return q[nsec].at[lax.rem(j, half), lev(lax.div(j, half)), :, pl.ds(lo, n)]

    def spot(i, gs):
        lo, n = spans[i]
        return out.at[:, :, pl.ds(gs * R + (lo if i < last else 0), n)]

    def out_copy(i, j, gs):
        return rc(result(i, j), spot(i, gs), out_s.at[i], out_r.at[i], dev(j, side if i < last else next_side))

    def own_out(i, gs):
        return pltpu.make_async_copy(result(i, here), spot(i, gs), loc.at[6 + i])

    def send_out(i):
        @pl.loop(0, G - 1)
        def _(t):
            out_copy(i, peer(t), g).start()

        own_out(i, g).start()

    for s in range(1, nsec + 1):
        lo, hi = s, first - s
        if hi - lo > 8:
            window(s, lo, lo, lo + 8)
            window(s, hi - 8, lo + 8, hi)
        elif hi > lo:
            window(s, min(lo, first - 8 - (s == 1)), lo, hi)
    if early:
        send_out(0)

    received(gather_of(parts[1][1]), in_r.at[1])

    for i, d in enumerate(dup_list):
        @pl.when(g == d)
        def _():
            own_dup(i).wait()

    wait_ahead(0)

    @pl.when(mixes)
    def _():
        @pl.loop(0, NT)
        def _(l):
            for b in range(half):
                for v in range(4):
                    for k in range(2):
                        fo[k, b, pl.ds(4 * l + v, 1)] = q[0][b, l, v, pl.ds(R - 1 + k, 1)]

    def mix():
        @pl.when(mixes)
        def _():
            @pl.loop(0, groups)
            def _(m):
                at = pl.ds(pl.multiple_of(8 * m, 8), 8)
                for r in range(2):
                    for b in range(half):
                        total = jnp.zeros((8, 128), jnp.float32)
                        for k in range(K):
                            picked = jnp.zeros((8, 128), jnp.float32)
                            for h in range(half):
                                got = jnp.take_along_axis(fo[1 - r, h, at], lane_ix[r, k, b, at], axis=1)
                                picked = jnp.where(blk_ix[r, k, b, at] == h, got, picked)
                            total = total + ww[r, k, b, at] * picked
                        gg[r, b, at] = total

    for s in range(1, nsec + 1):
        if s <= first - 8:
            mix()
        window(s, first - s, first - s, first - s + 8)
    send_out(inner)
    wait_ahead(1)

    for s in range(1, nsec + 1):
        if s > first - 8:
            mix()
        window(s, R + 2 - s, first + 8 - s, R + reach - s)

    @pl.loop(0, G - 1)
    def _(t):
        for i in range(inner + 1, last):
            out_copy(i, peer(t), g).start()
        out_copy(last, peer(t), following).start()

    for i in range(inner + 1, last):
        own_out(i, g).start()

    @pl.when(takes_own)
    def _():
        own_out(last, following).start()

    @pl.when(seam)
    def _():
        out_copy(last, here, following).start()

    for i in range(2):
        sent(gather_of(parts[i][1]), in_s.at[i])

    for i, d in enumerate(dup_list):
        @pl.when(g != d)
        def _():
            for k in range(2):
                dup_copy(i, k, here).wait_send()

    @pl.when(feeds_prev)
    def _():
        feed(0).wait_send()
        feed(1).wait_send()

    @pl.when(jnp.logical_not(ends))
    def _():
        far_copy(here, side).wait_send()

    @pl.when(jnp.logical_not(mixes))
    def _():
        wt_copy(here, side).wait_send()
        ix_copy(here, side).wait_send()

    for i in range(last):
        own_out(i, g).wait()
        sent(gather_of(spans[i][1]), out_s.at[i])
        received(gather_of(spans[i][1]), out_r.at[i])

    @pl.when(takes_own)
    def _():
        own_out(last, following).wait()
        sent(gather_of(nsec), out_s.at[last])
        received(gather_of(nsec), out_r.at[last])

    @pl.when(seam)
    def _():
        sent(gather_of(nsec, True), out_s.at[last])
        received(gather_of(nsec, True), out_r.at[last])


def ring_shards(dims, state, far_field, face_index, face_weight, mean_flow):
    tm_n, half = dims
    L, _, rows, width = state.shape
    K = face_weight.shape[1]
    G = tm_n * half
    R = rows // G
    NT = L * tm_n
    n = len(SECTION_FACTORS)
    f32 = jnp.float32
    hbm = pl.BlockSpec(memory_space=pl.ANY)
    dma = pltpu.SemaphoreType.DMA
    V = pltpu.VMEM
    args = [pltpu.with_memory_space_constraint(a, pltpu.HBM)
            for a in (state, far_field, face_index, face_weight, mean_flow)]
    return pl.pallas_call(
        functools.partial(ring_kernel, (tm_n, half, L, R, K)),
        out_shape=jax.ShapeDtypeStruct(state.shape, f32),
        in_specs=[hbm] * 5,
        out_specs=hbm,
        scratch_shapes=[
            [V((half, NT, 4, R + 16, width), f32) for _ in range(n + 1)],
            V((half, NT, 4, 8, width), f32),
            V((2, half, NT, 4, 8, width), f32),
            V((2, half, NT, 4, width), f32),
            V((2, half, NT, K, width), f32),
            V((2, half, tm_n, L, width), jnp.int32),
            V((2, K, half, 4 * NT, width), jnp.int32),
            V((2, K, half, 4 * NT, width), jnp.int32),
            V((2, K, half, 4 * NT, width), f32),
            V((2, half, 4 * NT, width), f32),
            V((2, half, 4 * NT, width), f32),
            pltpu.SMEM((2, 2), f32),
            pltpu.SemaphoreType.REGULAR((tm_n,)),
            dma((2,)), dma((2,)),
            dma((tm_n // 2 - 2, 2)), dma((2,)),
            dma((4,)), dma((4,)),
            dma((3,)), dma((3,)),
            dma((2,)), dma((2,)),
            dma((10,)),
        ],
        compiler_params=pltpu.CompilerParams(
            collective_id=0, has_side_effects=True, vmem_limit_bytes=48 * 1024 * 1024),
    )(*args)


def solution(mesh):
    dims = (mesh.shape["tm"], mesh.shape["block"] // 2)
    in_specs = (
        P("tm", None, None, "block"),
        P("tm", None, "block"),
        P("tm", "block"),
        P("tm", None, "block"),
        P(),
    )
    out_specs = P("tm", None, None, "block")

    def body(state, *rest):
        tm_n, half = dims
        fits = (half == 2 and tm_n in (6, 8) and state.shape[0] % 2 == 0 and state.shape[0] * tm_n % 8 == 0
                and rest[2].shape[1] == 4 and state.shape[2] == 16 * tm_n * half and state.shape[3] == 128)
        return (ring_shards if fits else shards)(dims, state, *rest)

    return jax.shard_map(body, mesh=mesh, in_specs=in_specs, out_specs=out_specs, check_vma=False)
```

```python
import functools
import math

import jax
import jax.numpy as jnp
from jax import lax
from jax.experimental import pallas as pl
from jax.experimental.pallas import tpu as pltpu
from jax.sharding import PartitionSpec as P

SECTION_FACTORS = (0.075, 0.05, 0.1125, 0.15, 0.3)
OMEGA = 1.0
DISSIPATION = 0.2
PAD = 8
FIRST_ROWS = 13
MESH = pl.DeviceIdType.MESH


def split_coefficients(count, scale):
    half = count // 2
    d = [0.0] + [0.5 * (-1) ** k / math.tan(math.pi * k / count) for k in range(1, half)] + [0.0]
    even = [0.5 * scale * (d[m] - d[half - m]) for m in range(half)]
    odd = [0.5 * scale * (d[m] + d[half - m]) for m in range(half)]
    even[0] = odd[0] = 0.0
    return even, odd


def time_term(q, even, odd):
    half = len(q) // 2
    quarter = half // 2
    e = [q[n] + q[n + half] for n in range(half)]
    o = [q[n] - q[n + half] for n in range(half)]

    def odd_at(n):
        return (o[n % half], -1.0 if (n // half) % 2 else 1.0)

    low, high = [], []
    for n in range(half):
        ev = None
        od = None
        for m in range(1, quarter):
            term = even[m] * (e[(n - m) % half] - e[(n + m) % half])
            ev = term if ev is None else ev + term
            (a, sa), (b, sb) = odd_at(n - m), odd_at(n + m)
            pair = a - b if sa == sb else a + b
            term = (odd[m] * sa) * pair
            od = term if od is None else od + term
        a, sa = odd_at(n - quarter)
        od = od + (odd[quarter] * sa) * a
        low.append(ev + od)
        high.append(ev - od)
    return low + high


def kernel(dims, state, far, fidx, fw, mf, out, x0, qa, qb, ef, el, rl, ru, cs, cl, cu,
           face, ff, wts, fi, lane_ix, blk_ix, ww, gh,
           in_s, in_r, out_s, out_r, p_s, p_r, h_s, h_r, f_s, f_r, loc):
    tm_n, half, L, R, K = dims
    NT = tm_n * L
    cycle = half * 128
    tiles = R // 8
    nsec = len(SECTION_FACTORS)
    me = lax.axis_index("tm")
    blk = lax.axis_index("block")
    side = lax.div(blk, half)
    place = lax.rem(blk, half)
    row0 = side * half
    lower_b = row0 + lax.rem(place + half - 1, half)
    upper_b = row0 + lax.rem(place + 1, half)
    other0 = (1 - side) * half
    step = 1 - 2 * side
    is_last = me == tm_n - 1
    is_far = me == 0
    rchunk = side * (tm_n - 1) + step * me
    has_lower = rchunk > 0
    has_upper = rchunk < tm_n - 1
    ghost_row = jnp.where(side == 0, PAD + R, PAD - 1)
    far_row = jnp.where(side == 0, PAD - 1, PAD + R)

    def rc(src, dst, ss, rs, dev):
        return pltpu.make_async_remote_copy(src_ref=src, dst_ref=dst, send_sem=ss, recv_sem=rs,
                                            device_id=dev, device_id_type=MESH)

    def rows(p):
        return pl.ds(pl.multiple_of((side * (tm_n - 1) + step * p) * R, R), R)

    def lev(p):
        return pl.ds(p * L, L)

    def peer(t):
        return lax.rem(me + 1 + t, tm_n)

    bar = pltpu.get_barrier_semaphore()

    @pl.loop(0, tm_n - 1)
    def _(t):
        pl.semaphore_signal(bar, inc=1, device_id={"tm": peer(t)}, device_id_type=MESH)

    pl.semaphore_signal(bar, inc=1, device_id={"block": lower_b}, device_id_type=MESH)
    pl.semaphore_signal(bar, inc=1, device_id={"block": upper_b}, device_id_type=MESH)

    @pl.when(is_last)
    def _():
        for h in range(half):
            pl.semaphore_signal(bar, inc=1, device_id={"block": other0 + h}, device_id_type=MESH)

    own = pltpu.make_async_copy(state.at[:, :, rows(me)], x0.at[lev(me)], loc.at[0])
    own.start()
    pl.semaphore_wait(bar, tm_n + 1 + jnp.where(is_last, half, 0))

    def in_copy(p, src_tm):
        return rc(state.at[:, :, rows(p)], x0.at[lev(src_tm)], in_s.at[p], in_r.at[src_tm], {"tm": p})

    @pl.loop(0, tm_n - 1)
    def _(t):
        p = peer(t)
        in_copy(p, me).start()

    def far_copy(src_tm):
        return rc(far, ff.at[lev(src_tm)], p_s.at[0], p_r.at[0, src_tm], {"tm": 0})

    def wt_copy(src_tm):
        return rc(fw, wts.at[lev(src_tm)], p_s.at[1], p_r.at[1, src_tm], {"tm": tm_n - 1})

    def ix_copy(src_tm):
        return rc(fidx, fi.at[src_tm], p_s.at[2], p_r.at[2, src_tm], {"tm": tm_n - 1})

    own_far = pltpu.make_async_copy(far, ff.at[lev(me)], loc.at[1])
    own_wt = pltpu.make_async_copy(fw, wts.at[lev(me)], loc.at[2])
    own_ix = pltpu.make_async_copy(fidx, fi.at[me], loc.at[3])

    @pl.when(is_far)
    def _():
        own_far.start()

    @pl.when(jnp.logical_not(is_far))
    def _():
        far_copy(me).start()

    @pl.when(is_last)
    def _():
        own_wt.start()
        own_ix.start()

    @pl.when(jnp.logical_not(is_last))
    def _():
        wt_copy(me).start()
        ix_copy(me).start()

    lane = lax.broadcasted_iota(jnp.int32, (8, 128), 1)
    lane_pair = jnp.bitwise_or(lane, 1)
    sub = lax.broadcasted_iota(jnp.int32, (8, 128), 0)

    def pack(acc, value, k):
        return jnp.where(lane_pair == k, pltpu.roll(value, k, 1), acc)

    def key(l, v):
        return 2 * (4 * l + v) + 1

    def halo_copies(s):
        low = rc(ef.at[s], ru.at[s], h_s.at[s, 0], h_r.at[s, 0], {"tm": me - step})
        up = rc(el.at[s], rl.at[s], h_s.at[s, 1], h_r.at[s, 1], {"tm": me + step})
        jl = rc(cs.at[s], cu.at[s], h_s.at[s, 2], h_r.at[s, 2], {"block": lower_b})
        ju = rc(cs.at[s], cl.at[s], h_s.at[s, 3], h_r.at[s, 3], {"block": upper_b})
        return low, up, jl, ju

    def face_copy(s, h, edge):
        return rc(edge.at[s], face.at[s, place], f_s.at[s, h], f_r.at[s, place], {"block": other0 + h})

    def face_wait(s, h):
        return rc(ef.at[s], face.at[s, h], f_s.at[s, h], f_r.at[s, h], {"block": other0 + h})

    def send_halos(s):
        low, up, jl, ju = halo_copies(s)

        @pl.when(is_last & (side == 0))
        def _():
            for h in range(half):
                face_copy(s, h, el).start()

        @pl.when(is_last & (side == 1))
        def _():
            for h in range(half):
                face_copy(s, h, ef).start()

        @pl.when(has_lower)
        def _():
            low.start()

        @pl.when(has_upper)
        def _():
            up.start()

        jl.start()
        ju.start()

    def take_level(l, accs):
        accs = list(accs)
        for v in range(4):
            for a in range(tiles):
                value = x0[l, v, pl.ds(8 * a, 8)]
                qa[l, v, pl.ds(PAD + 8 * a, 8)] = value
                accs[a] = pack(accs[a], value, key(l, v))
                if a == 0:
                    ef[0, pl.ds(4 * l + v, 1)] = value[0:1]
                if a == tiles - 1:
                    el[0, pl.ds(4 * l + v, 1)] = value[7:8]
        return tuple(accs)

    own.wait()
    accs = tuple(jnp.zeros((8, 128), jnp.float32) for _ in range(tiles))
    accs = lax.fori_loop(0, L, lambda j, c: take_level(me * L + j, c), accs)

    def arrive(t, c):
        p = peer(tm_n - 2 - t)
        in_copy(p, p).wait_recv()
        return lax.fori_loop(0, L, lambda j, d: take_level(p * L + j, d), c)

    accs = lax.fori_loop(0, tm_n - 1, arrive, accs)
    for a in range(tiles):
        cs[0, pl.ds(8 * a, 8)] = accs[a]
    send_halos(0)

    @pl.when(is_far)
    def _():
        own_far.wait()

        @pl.loop(1, tm_n)
        def _(p):
            far_copy(p).wait_recv()

        @pl.loop(0, NT)
        def _(l):
            for v in range(4):
                row = ff[l, pl.ds(v, 1)]
                qa[l, v, pl.ds(far_row, 1)] = row
                qb[l, v, pl.ds(far_row, 1)] = row

    @pl.when(is_last)
    def _():
        own_wt.wait()
        own_ix.wait()

        @pl.loop(0, tm_n - 1)
        def _(p):
            wt_copy(p).wait_recv()
            ix_copy(p).wait_recv()

        @pl.loop(0, NT // 2)
        def _(m):
            def ix(l):
                return jnp.broadcast_to(fi[lax.div(l, L), pl.ds(lax.rem(l, L), 1)], (8, 128))

            def wt(l, k):
                return jnp.broadcast_to(wts[l, pl.ds(k, 1)], (8, 128))

            start = jnp.where(sub < 4, ix(2 * m), ix(2 * m + 1))
            at = pl.ds(8 * m, 8)
            for k in range(K):
                src = start + k
                src = jnp.where(src >= cycle, src - cycle, src)
                lane_ix[k, at] = jnp.bitwise_and(src, 127)
                blk_ix[k, at] = lax.shift_right_logical(src, 7)
                ww[k, at] = jnp.where(sub < 4, wt(2 * m, k), wt(2 * m + 1, k))

    speed_u = jnp.where(side == 0, mf[0, 0], mf[1, 0])
    speed_v = jnp.where(side == 0, mf[0, 1], mf[1, 1])
    odd_lane = jnp.bitwise_and(lane, 1) == 1
    edge_lane = {0: lane == 0, 127: lane == 127}

    def install(dst, src, at):
        @pl.loop(0, NT)
        def _(l):
            for v in range(4):
                dst[l, v, pl.ds(at, 1)] = src[pl.ds(4 * l + v, 1)]

    def out_copy(q, p, src_tm):
        return rc(q.at[lev(p), :, pl.ds(PAD, R)], out.at[:, :, rows(src_tm)],
                  out_s.at[p], out_r.at[src_tm], {"tm": p})

    for s, factor in enumerate(SECTION_FACTORS):
        q, nq = (qa, qb) if s % 2 == 0 else (qb, qa)
        final = s == nsec - 1
        even, odd = split_coefficients(NT, OMEGA * factor)
        hu, hv, hh = (0.5 * factor) * speed_u, (0.5 * factor) * speed_v, 0.5 * factor

        @pl.loop(0, 4)
        def _(v):
            @pl.loop(0, tiles)
            def _(a):
                at = pl.ds(pl.multiple_of(PAD + 8 * a, 8), 8)
                xs = [q[l, v, at] for l in range(NT)]
                terms = time_term(xs, even, odd)
                for l in range(NT):
                    first = x0[l, v, pl.ds(pl.multiple_of(8 * a, 8), 8)]
                    nq[l, v, at] = first - (terms[l] + (4.0 * DISSIPATION * factor) * xs[l])

        low, up, jl, ju = halo_copies(s)
        jl.wait_recv()
        ju.wait_recv()
        mixed = []
        for a in range(tiles):
            at = pl.ds(8 * a, 8)
            mixed.append(jnp.where(odd_lane, pltpu.roll(cl[s, at], 1, 1), pltpu.roll(cu[s, at], 127, 1)))

        def level(l, accs, which):
            accs = list(accs)
            for slot, a in enumerate(which):
                base = PAD + 8 * a
                di, dj, near = [], [], []
                for v in range(4):
                    x = q[l, v, pl.ds(base, 8)]
                    upx = q[l, v, pl.ds(base + 1, 8)]
                    dnx = q[l, v, pl.ds(base - 1, 8)]
                    border = pltpu.roll(mixed[a], 128 - key(l, v), 1)
                    left = jnp.where(edge_lane[0], border, pltpu.roll(x, 1, 1))
                    right = jnp.where(edge_lane[127], border, pltpu.roll(x, 127, 1))
                    di.append(upx - dnx)
                    dj.append(right - left)
                    near.append((DISSIPATION * factor) * ((upx + dnx) + (right + left)))
                flux = [
                    hu * di[0] + hv * dj[0] + hh * (di[1] + dj[2]),
                    hu * di[1] + hv * dj[1] + hh * di[3],
                    hu * di[2] + hv * dj[2] + hh * dj[3],
                    hu * di[3] + hv * dj[3] + hh * (di[1] + dj[2]),
                ]
                for v in range(4):
                    new = nq[l, v, pl.ds(base, 8)] + (near[v] - flux[v])
                    nq[l, v, pl.ds(base, 8)] = new
                    if not final:
                        accs[slot] = pack(accs[slot], new, key(l, v))
                        if a == 0:
                            ef[s + 1, pl.ds(4 * l + v, 1)] = new[0:1]
                        if a == tiles - 1:
                            el[s + 1, pl.ds(4 * l + v, 1)] = new[7:8]
            return tuple(accs)

        def sweep(which):
            zero = tuple(jnp.zeros((8, 128), jnp.float32) for _ in which)
            step_by = 4 if NT % 4 == 0 else 1

            def several(g, c):
                for j in range(step_by):
                    c = level(step_by * g + j, c, which)
                return c

            accs = lax.fori_loop(0, NT // step_by, several, zero)
            if not final:
                for slot, a in enumerate(which):
                    cs[s + 1, pl.ds(8 * a, 8)] = accs[slot]

        inner = tuple(range(1, tiles - 1))
        outer = tuple(sorted({0, tiles - 1}))
        if inner:
            sweep(inner)

        @pl.when(has_lower)
        def _():
            up.wait_recv()
            install(q, rl.at[s], PAD - 1)

        @pl.when(has_upper)
        def _():
            low.wait_recv()
            install(q, ru.at[s], PAD + R)

        @pl.when(is_last)
        def _():
            for h in range(half):
                face_wait(s, h).wait_recv()

            @pl.loop(0, NT // 2)
            def _(m):
                at = pl.ds(8 * m, 8)
                total = jnp.zeros((8, 128), jnp.float32)
                for k in range(K):
                    picked = jnp.zeros((8, 128), jnp.float32)
                    for h in range(half):
                        got = jnp.take_along_axis(face[s, h, at], lane_ix[k, at], axis=1)
                        picked = jnp.where(blk_ix[k, at] == h, got, picked)
                    total = total + ww[k, at] * picked
                gh[at] = total

            install(q, gh, ghost_row)

        if not final:
            sweep(outer)
            send_halos(s + 1)
        else:
            def finish(t, c):
                p = peer(t)
                for j in range(L):
                    level(p * L + j, (None,) * len(outer), outer)

                @pl.when(t < tm_n - 1)
                def _():
                    out_copy(nq, p, me).start()

                return c

            lax.fori_loop(0, tm_n, finish, 0)
            own_out = pltpu.make_async_copy(nq.at[lev(me), :, pl.ds(PAD, R)], out.at[:, :, rows(me)], loc.at[4])
            own_out.start()

            @pl.loop(0, tm_n - 1)
            def _(t):
                p = peer(t)
                out_copy(nq, p, p).wait_recv()

            own_out.wait()

            @pl.loop(0, tm_n - 1)
            def _(t):
                p = peer(t)
                out_copy(nq, p, me).wait_send()

    @pl.loop(0, tm_n - 1)
    def _(t):
        p = peer(t)
        in_copy(p, me).wait_send()

    @pl.when(jnp.logical_not(is_far))
    def _():
        far_copy(me).wait_send()

    @pl.when(jnp.logical_not(is_last))
    def _():
        wt_copy(me).wait_send()
        ix_copy(me).wait_send()

    for s in range(nsec):
        low, up, jl, ju = halo_copies(s)

        @pl.when(has_lower)
        def _():
            low.wait_send()

        @pl.when(has_upper)
        def _():
            up.wait_send()

        jl.wait_send()
        ju.wait_send()

        @pl.when(is_last)
        def _():
            for h in range(half):
                face_wait(s, h).wait_send()


def shards(dims, state, far_field, face_index, face_weight, mean_flow):
    tm_n, half = dims
    L, _, rows, width = state.shape
    K = face_weight.shape[1]
    R = rows // tm_n
    NT = L * tm_n
    assert width == 128 and NT % 4 == 0 and R % 8 == 0 and 8 * NT <= width
    n = len(SECTION_FACTORS)
    f32 = jnp.float32
    hbm = pl.BlockSpec(memory_space=pl.ANY)
    dma = pltpu.SemaphoreType.DMA
    V = pltpu.VMEM
    return pl.pallas_call(
        functools.partial(kernel, (tm_n, half, L, R, K)),
        out_shape=jax.ShapeDtypeStruct(state.shape, f32),
        in_specs=[hbm, hbm, hbm, hbm, pl.BlockSpec(memory_space=pltpu.SMEM)],
        out_specs=hbm,
        scratch_shapes=[
            V((NT, 4, R, width), f32),
            V((NT, 4, R + 2 * PAD, width), f32),
            V((NT, 4, R + 2 * PAD, width), f32),
            V((n, 4 * NT, width), f32),
            V((n, 4 * NT, width), f32),
            V((n, 4 * NT, width), f32),
            V((n, 4 * NT, width), f32),
            V((n, R, width), f32),
            V((n, R, width), f32),
            V((n, R, width), f32),
            V((n, half, 4 * NT, width), f32),
            V((NT, 4, width), f32),
            V((NT, K, width), f32),
            V((tm_n, L, width), jnp.int32),
            V((K, 4 * NT, width), jnp.int32),
            V((K, 4 * NT, width), jnp.int32),
            V((K, 4 * NT, width), f32),
            V((4 * NT, width), f32),
            dma((tm_n,)), dma((tm_n,)), dma((tm_n,)), dma((tm_n,)),
            dma((3,)), dma((3, tm_n)),
            dma((n, 4)), dma((n, 4)),
            dma((n, half)), dma((n, half)),
            dma((5,)),
        ],
        compiler_params=pltpu.CompilerParams(
            collective_id=0, has_side_effects=True, vmem_limit_bytes=40 * 1024 * 1024),
    )(state, far_field, face_index, face_weight, mean_flow)


def skew_part(o, coef):
    half = len(o)
    quarter = half // 2

    def at(n):
        return o[n % half], -1.0 if (n // half) % 2 else 1.0

    res = []
    for n in range(half):
        total = None
        for m in range(1, quarter):
            (a, sa), (b, sb) = at(n - m), at(n + m)
            term = (coef[m] * sa) * (a - b if sa == sb else a + b)
            total = term if total is None else total + term
        a, sa = at(n - quarter)
        term = (coef[quarter] * sa) * a
        res.append(term if total is None else total + term)
    return res


def cyclic_part(e, coef):
    half = len(e)
    res = []
    for n in range(half):
        total = None
        for m in range(1, half // 2):
            term = coef[m] * (e[(n - m) % half] - e[(n + m) % half])
            total = term if total is None else total + term
        res.append(total)
    return res


def time_term_split(q, even, odd):
    half = len(q) // 2
    quarter = half // 2
    e = [q[n] + q[n + half] for n in range(half)]
    o = [q[n] - q[n + half] for n in range(half)]
    ee = [e[n] + e[n + quarter] for n in range(quarter)]
    eo = [e[n] - e[n + quarter] for n in range(quarter)]
    low = [0.0] + [0.5 * (even[m] - even[quarter - m]) for m in range(1, quarter)]
    high = [0.0] + [0.5 * (even[m] + even[quarter - m]) for m in range(1, quarter)]
    cyc = cyclic_part(ee, low)
    skw = skew_part(eo, high)
    ev = [cyc[n] + skw[n] for n in range(quarter)] + [cyc[n] - skw[n] for n in range(quarter)]
    od = skew_part(o, odd)
    return [ev[n] + od[n] for n in range(half)] + [ev[n] - od[n] for n in range(half)]


def ring_kernel(dims, state, far, fidx, fw, mf, out, q, tt, dd, ff, wts, fi, lane_ix, blk_ix, ww, gg, fo, mfs,
                info, in_s, in_r, dup_s, dup_r, out_s, out_r, p_s, p_r, h_s, h_r, loc):
    tm_n, half, L, R, K = dims
    NT = tm_n * L
    G = tm_n * half
    Z = tm_n // 2
    cycle = half * 128
    nsec = len(SECTION_FACTORS)
    reach = 2 * nsec
    groups = 4 * NT // 8
    me = lax.axis_index("tm")
    blk = lax.axis_index("block")
    side = lax.div(blk, half)
    place = lax.rem(blk, half)

    def slab(t, b, sd):
        z = lax.div(t, 2)
        c = lax.rem(t, 2)
        zo = jnp.where(sd == 0, z, Z - 1 - z)
        return 4 * zo + jnp.where(lax.rem(b + zo, 2) == 0, c, 3 - c)

    def owner(g, sd):
        zo = g // 4 if isinstance(g, int) else lax.div(g, 4)
        k = g % 4 if isinstance(g, int) else lax.rem(g, 4)
        xo = jnp.where(k >= 2, 1, 0)
        c = jnp.where(k >= 2, 3 - k, k)
        b = lax.rem(xo + zo, 2)
        return 2 * jnp.where(sd == 0, zo, Z - 1 - zo) + c, b

    def device(g, sd):
        t, b = owner(g, sd)
        return {"tm": t, "block": sd * half + b}

    g = slab(me, place, side)
    here = me * half + place
    seam = g == G - 1
    mixes = seam & (side == 0)
    ends = seam & (side == 1)
    mix_dev = device(G - 1, 0)
    end_dev = device(G - 1, 1)
    dup_list = [4 * z + 3 for z in range(1, Z - 1)]

    def is_dup(x):
        hit = x < -1
        for d in dup_list:
            hit = hit | (x == d)
        return hit

    takes_dup = is_dup(g)
    feeds_prev = jnp.logical_not(is_dup(g - 1))
    prev_side = jnp.where(g == 0, 1 - side, side)
    prev_dev = device(lax.rem(g + G - 1, G), prev_side)
    next_side = jnp.where(seam, 1 - side, side)

    def peer(t):
        return lax.rem(here + 1 + t, G)

    def dev(j, sd):
        return {"tm": lax.div(j, half), "block": sd * half + lax.rem(j, half)}

    def slab_of(j):
        return slab(lax.div(j, half), lax.rem(j, half), side)

    def lev(t):
        return pl.ds(t * L, L)

    def rc(src, dst, ss, rs, to):
        return pltpu.make_async_remote_copy(src_ref=src, dst_ref=dst, send_sem=ss, recv_sem=rs,
                                            device_id=to, device_id_type=MESH)

    def gather_of(n, whole=False):
        return q[0].at[:, pl.ds(0, NT if whole else NT - L // half), :, pl.ds(0, n)]

    def received(view, sem):
        rc(view, view, p_s.at[0], sem, end_dev).wait_recv()

    def sent(view, sem):
        rc(view, view, sem, p_r.at[0], end_dev).wait_send()

    z = lax.div(me, 2)

    def near(j):
        return jnp.abs(lax.div(lax.div(j, half), 2) - z) <= 1

    partner = {"block": (1 - side) * half + place}
    bar = pltpu.get_barrier_semaphore()

    @pl.loop(0, G - 1)
    def _(t):
        @pl.when(near(peer(t)))
        def _():
            pl.semaphore_signal(bar, inc=1, device_id=dev(peer(t), side), device_id_type=MESH)

    pl.semaphore_signal(bar, inc=1, device_id=partner, device_id_type=MESH)

    own = pltpu.make_async_copy(state.at[:, :, pl.ds(pl.multiple_of(g * R, R), R)],
                                q[0].at[place, lev(me), :, pl.ds(0, R)], loc.at[0])
    own.start()
    own_mf = pltpu.make_async_copy(mf, mfs, loc.at[4])
    own_mf.start()

    first = FIRST_ROWS
    ahead = ((0, first - 8), (first - 8, reach + 8 - first), (0, reach))

    def ahead_rows(d, k):
        lo, n = ahead[k]
        return state.at[:, :, pl.ds((d + 1) * R + lo, n)]

    def ahead_spot(j, k):
        lo, n = ahead[k]
        return q[0].at[lax.rem(j, half), lev(lax.div(j, half)), :, pl.ds(R + lo, n)]

    def dup_copy(i, k, j):
        return rc(ahead_rows(dup_list[i], k), ahead_spot(j, k), dup_s.at[i, k], dup_r.at[k],
                  device(dup_list[i], side))

    def own_dup(i):
        return pltpu.make_async_copy(ahead_rows(dup_list[i], 2), ahead_spot(here, 2), loc.at[5])

    def send_dup(k):
        for i, d in enumerate(dup_list):
            @pl.when(g != d)
            def _():
                dup_copy(i, k, here).start()

    for i, d in enumerate(dup_list):
        @pl.when(g == d)
        def _():
            own_dup(i).start()

    pl.semaphore_wait(bar, 2 * half * (1 + jnp.where(z > 0, 1, 0) + jnp.where(z < Z - 1, 1, 0)))

    parts = ((0, first), (first, R - first))

    def in_copy(i, j, src):
        lo, n = parts[i]
        return rc(state.at[:, :, pl.ds(slab_of(j) * R + lo, n)],
                  q[0].at[lax.rem(src, half), lev(lax.div(src, half)), :, pl.ds(lo, n)],
                  in_s.at[i], in_r.at[i], dev(j, side))

    def send_in(i, which=None):
        @pl.loop(0, G - 1)
        def _(t):
            if which is None:
                in_copy(i, peer(t), here).start()
            else:
                @pl.when(near(peer(t)) == which)
                def _():
                    in_copy(i, peer(t), here).start()

    send_in(0, True)

    for r in range(1, Z - 1):
        @pl.when((z >= 1) & (z + r <= Z - 1))
        def _():
            pl.semaphore_signal(info.at[r], inc=1, device_id={"tm": me - 2}, device_id_type=MESH)

        @pl.when((z <= Z - 2) & (z - r >= 0))
        def _():
            pl.semaphore_signal(info.at[Z + r], inc=1, device_id={"tm": me + 2}, device_id_type=MESH)

        @pl.when(z + r + 1 <= Z - 1)
        def _():
            pl.semaphore_wait(info.at[r], 1)

        @pl.when(z - r - 1 >= 0)
        def _():
            pl.semaphore_wait(info.at[Z + r], 1)

    send_in(0, False)
    pl.semaphore_signal(info.at[0], inc=1, device_id=partner, device_id_type=MESH)
    pl.semaphore_wait(info.at[0], 1)

    def far_copy(j, sd):
        return rc(far, ff.at[sd, lax.rem(j, half), lev(lax.div(j, half))], p_s.at[0], p_r.at[0], end_dev)

    def wt_copy(j, sd):
        return rc(fw, wts.at[sd, lax.rem(j, half), lev(lax.div(j, half))], p_s.at[1], p_r.at[1], mix_dev)

    def ix_copy(j, sd):
        return rc(fidx, fi.at[sd, lax.rem(j, half), lax.div(j, half)], p_s.at[2], p_r.at[2], mix_dev)

    own_far = pltpu.make_async_copy(far, ff.at[side, place, lev(me)], loc.at[1])
    own_wt = pltpu.make_async_copy(fw, wts.at[side, place, lev(me)], loc.at[2])
    own_ix = pltpu.make_async_copy(fidx, fi.at[side, place, me], loc.at[3])

    @pl.when(ends)
    def _():
        own_far.start()

    @pl.when(jnp.logical_not(ends))
    def _():
        far_copy(here, side).start()

    @pl.when(mixes)
    def _():
        own_wt.start()
        own_ix.start()

    @pl.when(jnp.logical_not(mixes))
    def _():
        wt_copy(here, side).start()
        ix_copy(here, side).start()

    send_dup(0)
    send_in(1, True)
    send_in(1, False)
    send_dup(1)

    lane = lax.broadcasted_iota(jnp.int32, (8, 128), 1)
    sub = lax.broadcasted_iota(jnp.int32, (8, 128), 0)
    first_lane, last_lane = lane == 0, lane == 127

    @pl.when(ends)
    def _():
        own_far.wait()

        received(q[0].at[:, pl.ds(0, L // half), :, pl.ds(0, 2 * G - 1)], p_r.at[0])

        for k in range(2):
            for b in range(half):
                @pl.loop(0, NT)
                def _(l):
                    for v in range(4):
                        gg[k, b, pl.ds(4 * l + v, 1)] = ff[1 - k, b, l, pl.ds(v, 1)]

    @pl.when(mixes)
    def _():
        own_wt.wait()
        own_ix.wait()

        received(q[0].at[:, pl.ds(0, L // half), :, pl.ds(0, 2 * G - 1)], p_r.at[1])
        received(q[0].at[0, 0, pl.ds(0, L), pl.ds(0, 2 * G - 1)], p_r.at[2])

        for r in range(2):
            for b in range(half):
                @pl.loop(0, NT // 2)
                def _(m):
                    def ix(l):
                        return jnp.broadcast_to(fi[r, b, lax.div(l, L), pl.ds(lax.rem(l, L), 1)], (8, 128))

                    def wt(l, k):
                        return jnp.broadcast_to(wts[r, b, l, pl.ds(k, 1)], (8, 128))

                    start = jnp.where(sub < 4, ix(2 * m), ix(2 * m + 1))
                    at = pl.ds(8 * m, 8)
                    for k in range(K):
                        src = start + k
                        src = jnp.where(src >= cycle, src - cycle, src)
                        lane_ix[r, k, b, at] = jnp.bitwise_and(src, 127)
                        blk_ix[r, k, b, at] = lax.shift_right_logical(src, 7)
                        ww[r, k, b, at] = jnp.where(sub < 4, wt(2 * m, k), wt(2 * m + 1, k))

    own_mf.wait()

    def speeds(sd):
        return jnp.where(sd == 0, mfs[0, 0], mfs[1, 0]), jnp.where(sd == 0, mfs[0, 1], mfs[1, 1])

    own_speed = speeds(side)
    next_speed = speeds(next_side)

    def feed(k):
        lo, n = ahead[k]
        return rc(q[0].at[:, :, :, pl.ds(lo, n)], q[0].at[:, :, :, pl.ds(R + lo, n)], h_s.at[k], h_r.at[k], prev_dev)

    def wait_ahead(k):
        @pl.when(takes_dup)
        def _():
            received(gather_of(ahead[k][1]), dup_r.at[k])

        @pl.when(jnp.logical_not(takes_dup))
        def _():
            feed(k).wait_recv()

    span = range(half)

    def window(s, w, lo, hi):
        old, new = q[s - 1], q[s]
        c = SECTION_FACTORS[s - 1]
        even, odd = split_coefficients(NT, -OMEGA * c)
        at = pl.ds(w, 8)
        up_row, dn_row = lo <= R - 1 < hi, lo <= R < hi
        hh = 0.5 * c
        near = DISSIPATION * c

        def weights(uv):
            return near - hh * uv[0], near + hh * uv[0], near - hh * uv[1], near + hh * uv[1]

        cu, cd, cr, cl = weights(own_speed)
        if hi > R:
            beyond = sub >= R - w
            cu, cd, cr, cl = [jnp.where(beyond, n, o) for n, o in zip(weights(next_speed), (cu, cd, cr, cl))]
        up_at = sub == jnp.where(seam, R - 1 - w, 8)
        dn_at = sub == jnp.where(seam, R - w, 8)

        @pl.loop(0, 4)
        def _(v):
            for b in span:
                xs = [old[b, l, v, at] for l in range(NT)]
                terms = time_term_split(xs, even, odd)
                for l in range(NT):
                    tt[b, l, v] = (q[0][b, l, v, at] + terms[l]) - (4.0 * DISSIPATION * c) * xs[l]
            for l in range(NT):
                x = [old[b, l, v, at] for b in span]
                rr = [pltpu.roll(x[b], 127, 1) for b in span]
                rl = [pltpu.roll(x[b], 1, 1) for b in span]
                for b in span:
                    up = old[b, l, v, pl.ds(w + 1, 8)]
                    dn = old[b, l, v, pl.ds(w - 1, 8)]
                    row = pl.ds(4 * l + v, 1)
                    if up_row:
                        up = jnp.where(up_at, jnp.broadcast_to(gg[0, b, row], (8, 128)), up)
                    if dn_row:
                        dn = jnp.where(dn_at, jnp.broadcast_to(gg[1, b, row], (8, 128)), dn)
                    right = jnp.where(last_lane, rr[(b + 1) % half], rr[b])
                    left = jnp.where(first_lane, rl[(b - 1) % half], rl[b])
                    tt[b, l, v] = (tt[b, l, v] + (cu * up + cd * dn)) + (cr * right + cl * left)
                    dd[0, b, l, v] = hh * (up - dn)
                    dd[1, b, l, v] = hh * (right - left)

        @pl.loop(0, NT // 4)
        def _(i):
            for j in range(4):
                l = 4 * i + j
                for b in span:
                    cross = dd[0, b, l, 1] + dd[1, b, l, 2]
                    drop = [cross, dd[0, b, l, 3], dd[1, b, l, 3], cross]
                    for v in range(4):
                        value = tt[b, l, v] - drop[v]
                        new[b, l, v, pl.ds(lo, hi - lo)] = value[lo - w:hi - w]
                        for k, hit in enumerate((up_row, dn_row)):
                            if hit and s < nsec:
                                row = R - 1 + k - w
                                fo[k, b, pl.ds(4 * l + v, 1)] = value[row:row + 1]

    own.wait()

    received(gather_of(parts[0][1]), in_r.at[0])

    @pl.when(feeds_prev)
    def _():
        feed(0).start()
        feed(1).start()

    early = first - reach
    following = lax.rem(g + 1, G)
    takes_own = jnp.logical_not(seam)
    turn = nsec + early + 8
    spans = [(nsec, early), (nsec + early, 8), (turn, R - turn), (R, nsec)]
    spans = [(lo, n) for lo, n in spans if n > 0]
    last = len(spans) - 1
    inner = 1 if early else 0

    def result(i, j):
        lo, n = spans[i]
        return q[nsec].at[lax.rem(j, half), lev(lax.div(j, half)), :, pl.ds(lo, n)]

    def spot(i, gs):
        lo, n = spans[i]
        return out.at[:, :, pl.ds(gs * R + (lo if i < last else 0), n)]

    def out_copy(i, j, gs):
        return rc(result(i, j), spot(i, gs), out_s.at[i], out_r.at[i], dev(j, side if i < last else next_side))

    def own_out(i, gs):
        return pltpu.make_async_copy(result(i, here), spot(i, gs), loc.at[6 + i])

    def send_out(i):
        @pl.loop(0, G - 1)
        def _(t):
            out_copy(i, peer(t), g).start()

        own_out(i, g).start()

    for s in range(1, nsec + 1):
        lo, hi = s, first - s
        if hi - lo > 8:
            window(s, lo, lo, lo + 8)
            window(s, hi - 8, lo + 8, hi)
        elif hi > lo:
            window(s, min(lo, first - 8 - (s == 1)), lo, hi)
    if early:
        send_out(0)

    received(gather_of(parts[1][1]), in_r.at[1])

    for i, d in enumerate(dup_list):
        @pl.when(g == d)
        def _():
            own_dup(i).wait()

    wait_ahead(0)

    @pl.when(mixes)
    def _():
        @pl.loop(0, NT)
        def _(l):
            for b in range(half):
                for v in range(4):
                    for k in range(2):
                        fo[k, b, pl.ds(4 * l + v, 1)] = q[0][b, l, v, pl.ds(R - 1 + k, 1)]

    def mix():
        @pl.when(mixes)
        def _():
            @pl.loop(0, groups)
            def _(m):
                at = pl.ds(pl.multiple_of(8 * m, 8), 8)
                for r in range(2):
                    for b in range(half):
                        total = jnp.zeros((8, 128), jnp.float32)
                        for k in range(K):
                            picked = jnp.zeros((8, 128), jnp.float32)
                            for h in range(half):
                                got = jnp.take_along_axis(fo[1 - r, h, at], lane_ix[r, k, b, at], axis=1)
                                picked = jnp.where(blk_ix[r, k, b, at] == h, got, picked)
                            total = total + ww[r, k, b, at] * picked
                        gg[r, b, at] = total

    for s in range(1, nsec + 1):
        if s <= first - 8:
            mix()
        window(s, first - s, first - s, first - s + 8)
    send_out(inner)
    wait_ahead(1)

    for s in range(1, nsec + 1):
        if s > first - 8:
            mix()
        window(s, R + 2 - s, first + 8 - s, R + reach - s)

    @pl.loop(0, G - 1)
    def _(t):
        for i in range(inner + 1, last):
            out_copy(i, peer(t), g).start()
        out_copy(last, peer(t), following).start()

    for i in range(inner + 1, last):
        own_out(i, g).start()

    @pl.when(takes_own)
    def _():
        own_out(last, following).start()

    @pl.when(seam)
    def _():
        out_copy(last, here, following).start()

    for i in range(2):
        sent(gather_of(parts[i][1]), in_s.at[i])

    for i, d in enumerate(dup_list):
        @pl.when(g != d)
        def _():
            for k in range(2):
                dup_copy(i, k, here).wait_send()

    @pl.when(feeds_prev)
    def _():
        feed(0).wait_send()
        feed(1).wait_send()

    @pl.when(jnp.logical_not(ends))
    def _():
        far_copy(here, side).wait_send()

    @pl.when(jnp.logical_not(mixes))
    def _():
        wt_copy(here, side).wait_send()
        ix_copy(here, side).wait_send()

    for i in range(last):
        own_out(i, g).wait()
        sent(gather_of(spans[i][1]), out_s.at[i])
        received(gather_of(spans[i][1]), out_r.at[i])

    @pl.when(takes_own)
    def _():
        own_out(last, following).wait()
        sent(gather_of(nsec), out_s.at[last])
        received(gather_of(nsec), out_r.at[last])

    @pl.when(seam)
    def _():
        sent(gather_of(nsec, True), out_s.at[last])
        received(gather_of(nsec, True), out_r.at[last])


def ring_shards(dims, state, far_field, face_index, face_weight, mean_flow):
    tm_n, half = dims
    L, _, rows, width = state.shape
    K = face_weight.shape[1]
    G = tm_n * half
    R = rows // G
    NT = L * tm_n
    n = len(SECTION_FACTORS)
    f32 = jnp.float32
    hbm = pl.BlockSpec(memory_space=pl.ANY)
    dma = pltpu.SemaphoreType.DMA
    V = pltpu.VMEM
    args = [pltpu.with_memory_space_constraint(a, pltpu.HBM)
            for a in (state, far_field, face_index, face_weight, mean_flow)]
    return pl.pallas_call(
        functools.partial(ring_kernel, (tm_n, half, L, R, K)),
        out_shape=jax.ShapeDtypeStruct(state.shape, f32),
        in_specs=[hbm] * 5,
        out_specs=hbm,
        scratch_shapes=[
            [V((half, NT, 4, R + 16, width), f32) for _ in range(n + 1)],
            V((half, NT, 4, 8, width), f32),
            V((2, half, NT, 4, 8, width), f32),
            V((2, half, NT, 4, width), f32),
            V((2, half, NT, K, width), f32),
            V((2, half, tm_n, L, width), jnp.int32),
            V((2, K, half, 4 * NT, width), jnp.int32),
            V((2, K, half, 4 * NT, width), jnp.int32),
            V((2, K, half, 4 * NT, width), f32),
            V((2, half, 4 * NT, width), f32),
            V((2, half, 4 * NT, width), f32),
            pltpu.SMEM((2, 2), f32),
            pltpu.SemaphoreType.REGULAR((tm_n,)),
            dma((2,)), dma((2,)),
            dma((tm_n // 2 - 2, 2)), dma((2,)),
            dma((4,)), dma((4,)),
            dma((3,)), dma((3,)),
            dma((2,)), dma((2,)),
            dma((10,)),
        ],
        compiler_params=pltpu.CompilerParams(
            collective_id=0, has_side_effects=True, vmem_limit_bytes=48 * 1024 * 1024),
    )(*args)


def solution(mesh):
    dims = (mesh.shape["tm"], mesh.shape["block"] // 2)
    in_specs = (
        P("tm", None, None, "block"),
        P("tm", None, "block"),
        P("tm", "block"),
        P("tm", None, "block"),
        P(),
    )
    out_specs = P("tm", None, None, "block")

    def body(state, *rest):
        tm_n, half = dims
        fits = (half == 2 and tm_n in (6, 8) and state.shape[0] % 2 == 0 and state.shape[0] * tm_n % 8 == 0
                and rest[2].shape[1] == 4 and state.shape[2] == 16 * tm_n * half and state.shape[3] == 128)
        return (ring_shards if fits else shards)(dims, state, *rest)

    return jax.shard_map(body, mesh=mesh, in_specs=in_specs, out_specs=out_specs, check_vma=False)
```

```python
import functools
import math

import jax
import jax.numpy as jnp
from jax import lax
from jax.experimental import pallas as pl
from jax.experimental.pallas import tpu as pltpu
from jax.sharding import PartitionSpec as P

SECTION_FACTORS = (0.075, 0.05, 0.1125, 0.15, 0.3)
OMEGA = 1.0
DISSIPATION = 0.2
PAD = 8
FIRST_ROWS = 13
MESH = pl.DeviceIdType.MESH


def split_coefficients(count, scale):
    half = count // 2
    d = [0.0] + [0.5 * (-1) ** k / math.tan(math.pi * k / count) for k in range(1, half)] + [0.0]
    even = [0.5 * scale * (d[m] - d[half - m]) for m in range(half)]
    odd = [0.5 * scale * (d[m] + d[half - m]) for m in range(half)]
    even[0] = odd[0] = 0.0
    return even, odd


def time_term(q, even, odd):
    half = len(q) // 2
    quarter = half // 2
    e = [q[n] + q[n + half] for n in range(half)]
    o = [q[n] - q[n + half] for n in range(half)]

    def odd_at(n):
        return (o[n % half], -1.0 if (n // half) % 2 else 1.0)

    low, high = [], []
    for n in range(half):
        ev = None
        od = None
        for m in range(1, quarter):
            term = even[m] * (e[(n - m) % half] - e[(n + m) % half])
            ev = term if ev is None else ev + term
            (a, sa), (b, sb) = odd_at(n - m), odd_at(n + m)
            pair = a - b if sa == sb else a + b
            term = (odd[m] * sa) * pair
            od = term if od is None else od + term
        a, sa = odd_at(n - quarter)
        od = od + (odd[quarter] * sa) * a
        low.append(ev + od)
        high.append(ev - od)
    return low + high


def kernel(dims, state, far, fidx, fw, mf, out, x0, qa, qb, ef, el, rl, ru, cs, cl, cu,
           face, ff, wts, fi, lane_ix, blk_ix, ww, gh,
           in_s, in_r, out_s, out_r, p_s, p_r, h_s, h_r, f_s, f_r, loc):
    tm_n, half, L, R, K = dims
    NT = tm_n * L
    cycle = half * 128
    tiles = R // 8
    nsec = len(SECTION_FACTORS)
    me = lax.axis_index("tm")
    blk = lax.axis_index("block")
    side = lax.div(blk, half)
    place = lax.rem(blk, half)
    row0 = side * half
    lower_b = row0 + lax.rem(place + half - 1, half)
    upper_b = row0 + lax.rem(place + 1, half)
    other0 = (1 - side) * half
    step = 1 - 2 * side
    is_last = me == tm_n - 1
    is_far = me == 0
    rchunk = side * (tm_n - 1) + step * me
    has_lower = rchunk > 0
    has_upper = rchunk < tm_n - 1
    ghost_row = jnp.where(side == 0, PAD + R, PAD - 1)
    far_row = jnp.where(side == 0, PAD - 1, PAD + R)

    def rc(src, dst, ss, rs, dev):
        return pltpu.make_async_remote_copy(src_ref=src, dst_ref=dst, send_sem=ss, recv_sem=rs,
                                            device_id=dev, device_id_type=MESH)

    def rows(p):
        return pl.ds(pl.multiple_of((side * (tm_n - 1) + step * p) * R, R), R)

    def lev(p):
        return pl.ds(p * L, L)

    def peer(t):
        return lax.rem(me + 1 + t, tm_n)

    bar = pltpu.get_barrier_semaphore()

    @pl.loop(0, tm_n - 1)
    def _(t):
        pl.semaphore_signal(bar, inc=1, device_id={"tm": peer(t)}, device_id_type=MESH)

    pl.semaphore_signal(bar, inc=1, device_id={"block": lower_b}, device_id_type=MESH)
    pl.semaphore_signal(bar, inc=1, device_id={"block": upper_b}, device_id_type=MESH)

    @pl.when(is_last)
    def _():
        for h in range(half):
            pl.semaphore_signal(bar, inc=1, device_id={"block": other0 + h}, device_id_type=MESH)

    own = pltpu.make_async_copy(state.at[:, :, rows(me)], x0.at[lev(me)], loc.at[0])
    own.start()
    pl.semaphore_wait(bar, tm_n + 1 + jnp.where(is_last, half, 0))

    def in_copy(p, src_tm):
        return rc(state.at[:, :, rows(p)], x0.at[lev(src_tm)], in_s.at[p], in_r.at[src_tm], {"tm": p})

    @pl.loop(0, tm_n - 1)
    def _(t):
        p = peer(t)
        in_copy(p, me).start()

    def far_copy(src_tm):
        return rc(far, ff.at[lev(src_tm)], p_s.at[0], p_r.at[0, src_tm], {"tm": 0})

    def wt_copy(src_tm):
        return rc(fw, wts.at[lev(src_tm)], p_s.at[1], p_r.at[1, src_tm], {"tm": tm_n - 1})

    def ix_copy(src_tm):
        return rc(fidx, fi.at[src_tm], p_s.at[2], p_r.at[2, src_tm], {"tm": tm_n - 1})

    own_far = pltpu.make_async_copy(far, ff.at[lev(me)], loc.at[1])
    own_wt = pltpu.make_async_copy(fw, wts.at[lev(me)], loc.at[2])
    own_ix = pltpu.make_async_copy(fidx, fi.at[me], loc.at[3])

    @pl.when(is_far)
    def _():
        own_far.start()

    @pl.when(jnp.logical_not(is_far))
    def _():
        far_copy(me).start()

    @pl.when(is_last)
    def _():
        own_wt.start()
        own_ix.start()

    @pl.when(jnp.logical_not(is_last))
    def _():
        wt_copy(me).start()
        ix_copy(me).start()

    lane = lax.broadcasted_iota(jnp.int32, (8, 128), 1)
    lane_pair = jnp.bitwise_or(lane, 1)
    sub = lax.broadcasted_iota(jnp.int32, (8, 128), 0)

    def pack(acc, value, k):
        return jnp.where(lane_pair == k, pltpu.roll(value, k, 1), acc)

    def key(l, v):
        return 2 * (4 * l + v) + 1

    def halo_copies(s):
        low = rc(ef.at[s], ru.at[s], h_s.at[s, 0], h_r.at[s, 0], {"tm": me - step})
        up = rc(el.at[s], rl.at[s], h_s.at[s, 1], h_r.at[s, 1], {"tm": me + step})
        jl = rc(cs.at[s], cu.at[s], h_s.at[s, 2], h_r.at[s, 2], {"block": lower_b})
        ju = rc(cs.at[s], cl.at[s], h_s.at[s, 3], h_r.at[s, 3], {"block": upper_b})
        return low, up, jl, ju

    def face_copy(s, h, edge):
        return rc(edge.at[s], face.at[s, place], f_s.at[s, h], f_r.at[s, place], {"block": other0 + h})

    def face_wait(s, h):
        return rc(ef.at[s], face.at[s, h], f_s.at[s, h], f_r.at[s, h], {"block": other0 + h})

    def send_halos(s):
        low, up, jl, ju = halo_copies(s)

        @pl.when(is_last & (side == 0))
        def _():
            for h in range(half):
                face_copy(s, h, el).start()

        @pl.when(is_last & (side == 1))
        def _():
            for h in range(half):
                face_copy(s, h, ef).start()

        @pl.when(has_lower)
        def _():
            low.start()

        @pl.when(has_upper)
        def _():
            up.start()

        jl.start()
        ju.start()

    def take_level(l, accs):
        accs = list(accs)
        for v in range(4):
            for a in range(tiles):
                value = x0[l, v, pl.ds(8 * a, 8)]
                qa[l, v, pl.ds(PAD + 8 * a, 8)] = value
                accs[a] = pack(accs[a], value, key(l, v))
                if a == 0:
                    ef[0, pl.ds(4 * l + v, 1)] = value[0:1]
                if a == tiles - 1:
                    el[0, pl.ds(4 * l + v, 1)] = value[7:8]
        return tuple(accs)

    own.wait()
    accs = tuple(jnp.zeros((8, 128), jnp.float32) for _ in range(tiles))
    accs = lax.fori_loop(0, L, lambda j, c: take_level(me * L + j, c), accs)

    def arrive(t, c):
        p = peer(tm_n - 2 - t)
        in_copy(p, p).wait_recv()
        return lax.fori_loop(0, L, lambda j, d: take_level(p * L + j, d), c)

    accs = lax.fori_loop(0, tm_n - 1, arrive, accs)
    for a in range(tiles):
        cs[0, pl.ds(8 * a, 8)] = accs[a]
    send_halos(0)

    @pl.when(is_far)
    def _():
        own_far.wait()

        @pl.loop(1, tm_n)
        def _(p):
            far_copy(p).wait_recv()

        @pl.loop(0, NT)
        def _(l):
            for v in range(4):
                row = ff[l, pl.ds(v, 1)]
                qa[l, v, pl.ds(far_row, 1)] = row
                qb[l, v, pl.ds(far_row, 1)] = row

    @pl.when(is_last)
    def _():
        own_wt.wait()
        own_ix.wait()

        @pl.loop(0, tm_n - 1)
        def _(p):
            wt_copy(p).wait_recv()
            ix_copy(p).wait_recv()

        @pl.loop(0, NT // 2)
        def _(m):
            def ix(l):
                return jnp.broadcast_to(fi[lax.div(l, L), pl.ds(lax.rem(l, L), 1)], (8, 128))

            def wt(l, k):
                return jnp.broadcast_to(wts[l, pl.ds(k, 1)], (8, 128))

            start = jnp.where(sub < 4, ix(2 * m), ix(2 * m + 1))
            at = pl.ds(8 * m, 8)
            for k in range(K):
                src = start + k
                src = jnp.where(src >= cycle, src - cycle, src)
                lane_ix[k, at] = jnp.bitwise_and(src, 127)
                blk_ix[k, at] = lax.shift_right_logical(src, 7)
                ww[k, at] = jnp.where(sub < 4, wt(2 * m, k), wt(2 * m + 1, k))

    speed_u = jnp.where(side == 0, mf[0, 0], mf[1, 0])
    speed_v = jnp.where(side == 0, mf[0, 1], mf[1, 1])
    odd_lane = jnp.bitwise_and(lane, 1) == 1
    edge_lane = {0: lane == 0, 127: lane == 127}

    def install(dst, src, at):
        @pl.loop(0, NT)
        def _(l):
            for v in range(4):
                dst[l, v, pl.ds(at, 1)] = src[pl.ds(4 * l + v, 1)]

    def out_copy(q, p, src_tm):
        return rc(q.at[lev(p), :, pl.ds(PAD, R)], out.at[:, :, rows(src_tm)],
                  out_s.at[p], out_r.at[src_tm], {"tm": p})

    for s, factor in enumerate(SECTION_FACTORS):
        q, nq = (qa, qb) if s % 2 == 0 else (qb, qa)
        final = s == nsec - 1
        even, odd = split_coefficients(NT, OMEGA * factor)
        hu, hv, hh = (0.5 * factor) * speed_u, (0.5 * factor) * speed_v, 0.5 * factor

        @pl.loop(0, 4)
        def _(v):
            @pl.loop(0, tiles)
            def _(a):
                at = pl.ds(pl.multiple_of(PAD + 8 * a, 8), 8)
                xs = [q[l, v, at] for l in range(NT)]
                terms = time_term(xs, even, odd)
                for l in range(NT):
                    first = x0[l, v, pl.ds(pl.multiple_of(8 * a, 8), 8)]
                    nq[l, v, at] = first - (terms[l] + (4.0 * DISSIPATION * factor) * xs[l])

        low, up, jl, ju = halo_copies(s)
        jl.wait_recv()
        ju.wait_recv()
        mixed = []
        for a in range(tiles):
            at = pl.ds(8 * a, 8)
            mixed.append(jnp.where(odd_lane, pltpu.roll(cl[s, at], 1, 1), pltpu.roll(cu[s, at], 127, 1)))

        def level(l, accs, which):
            accs = list(accs)
            for slot, a in enumerate(which):
                base = PAD + 8 * a
                di, dj, near = [], [], []
                for v in range(4):
                    x = q[l, v, pl.ds(base, 8)]
                    upx = q[l, v, pl.ds(base + 1, 8)]
                    dnx = q[l, v, pl.ds(base - 1, 8)]
                    border = pltpu.roll(mixed[a], 128 - key(l, v), 1)
                    left = jnp.where(edge_lane[0], border, pltpu.roll(x, 1, 1))
                    right = jnp.where(edge_lane[127], border, pltpu.roll(x, 127, 1))
                    di.append(upx - dnx)
                    dj.append(right - left)
                    near.append((DISSIPATION * factor) * ((upx + dnx) + (right + left)))
                flux = [
                    hu * di[0] + hv * dj[0] + hh * (di[1] + dj[2]),
                    hu * di[1] + hv * dj[1] + hh * di[3],
                    hu * di[2] + hv * dj[2] + hh * dj[3],
                    hu * di[3] + hv * dj[3] + hh * (di[1] + dj[2]),
                ]
                for v in range(4):
                    new = nq[l, v, pl.ds(base, 8)] + (near[v] - flux[v])
                    nq[l, v, pl.ds(base, 8)] = new
                    if not final:
                        accs[slot] = pack(accs[slot], new, key(l, v))
                        if a == 0:
                            ef[s + 1, pl.ds(4 * l + v, 1)] = new[0:1]
                        if a == tiles - 1:
                            el[s + 1, pl.ds(4 * l + v, 1)] = new[7:8]
            return tuple(accs)

        def sweep(which):
            zero = tuple(jnp.zeros((8, 128), jnp.float32) for _ in which)
            step_by = 4 if NT % 4 == 0 else 1

            def several(g, c):
                for j in range(step_by):
                    c = level(step_by * g + j, c, which)
                return c

            accs = lax.fori_loop(0, NT // step_by, several, zero)
            if not final:
                for slot, a in enumerate(which):
                    cs[s + 1, pl.ds(8 * a, 8)] = accs[slot]

        inner = tuple(range(1, tiles - 1))
        outer = tuple(sorted({0, tiles - 1}))
        if inner:
            sweep(inner)

        @pl.when(has_lower)
        def _():
            up.wait_recv()
            install(q, rl.at[s], PAD - 1)

        @pl.when(has_upper)
        def _():
            low.wait_recv()
            install(q, ru.at[s], PAD + R)

        @pl.when(is_last)
        def _():
            for h in range(half):
                face_wait(s, h).wait_recv()

            @pl.loop(0, NT // 2)
            def _(m):
                at = pl.ds(8 * m, 8)
                total = jnp.zeros((8, 128), jnp.float32)
                for k in range(K):
                    picked = jnp.zeros((8, 128), jnp.float32)
                    for h in range(half):
                        got = jnp.take_along_axis(face[s, h, at], lane_ix[k, at], axis=1)
                        picked = jnp.where(blk_ix[k, at] == h, got, picked)
                    total = total + ww[k, at] * picked
                gh[at] = total

            install(q, gh, ghost_row)

        if not final:
            sweep(outer)
            send_halos(s + 1)
        else:
            def finish(t, c):
                p = peer(t)
                for j in range(L):
                    level(p * L + j, (None,) * len(outer), outer)

                @pl.when(t < tm_n - 1)
                def _():
                    out_copy(nq, p, me).start()

                return c

            lax.fori_loop(0, tm_n, finish, 0)
            own_out = pltpu.make_async_copy(nq.at[lev(me), :, pl.ds(PAD, R)], out.at[:, :, rows(me)], loc.at[4])
            own_out.start()

            @pl.loop(0, tm_n - 1)
            def _(t):
                p = peer(t)
                out_copy(nq, p, p).wait_recv()

            own_out.wait()

            @pl.loop(0, tm_n - 1)
            def _(t):
                p = peer(t)
                out_copy(nq, p, me).wait_send()

    @pl.loop(0, tm_n - 1)
    def _(t):
        p = peer(t)
        in_copy(p, me).wait_send()

    @pl.when(jnp.logical_not(is_far))
    def _():
        far_copy(me).wait_send()

    @pl.when(jnp.logical_not(is_last))
    def _():
        wt_copy(me).wait_send()
        ix_copy(me).wait_send()

    for s in range(nsec):
        low, up, jl, ju = halo_copies(s)

        @pl.when(has_lower)
        def _():
            low.wait_send()

        @pl.when(has_upper)
        def _():
            up.wait_send()

        jl.wait_send()
        ju.wait_send()

        @pl.when(is_last)
        def _():
            for h in range(half):
                face_wait(s, h).wait_send()


def shards(dims, state, far_field, face_index, face_weight, mean_flow):
    tm_n, half = dims
    L, _, rows, width = state.shape
    K = face_weight.shape[1]
    R = rows // tm_n
    NT = L * tm_n
    assert width == 128 and NT % 4 == 0 and R % 8 == 0 and 8 * NT <= width
    n = len(SECTION_FACTORS)
    f32 = jnp.float32
    hbm = pl.BlockSpec(memory_space=pl.ANY)
    dma = pltpu.SemaphoreType.DMA
    V = pltpu.VMEM
    return pl.pallas_call(
        functools.partial(kernel, (tm_n, half, L, R, K)),
        out_shape=jax.ShapeDtypeStruct(state.shape, f32),
        in_specs=[hbm, hbm, hbm, hbm, pl.BlockSpec(memory_space=pltpu.SMEM)],
        out_specs=hbm,
        scratch_shapes=[
            V((NT, 4, R, width), f32),
            V((NT, 4, R + 2 * PAD, width), f32),
            V((NT, 4, R + 2 * PAD, width), f32),
            V((n, 4 * NT, width), f32),
            V((n, 4 * NT, width), f32),
            V((n, 4 * NT, width), f32),
            V((n, 4 * NT, width), f32),
            V((n, R, width), f32),
            V((n, R, width), f32),
            V((n, R, width), f32),
            V((n, half, 4 * NT, width), f32),
            V((NT, 4, width), f32),
            V((NT, K, width), f32),
            V((tm_n, L, width), jnp.int32),
            V((K, 4 * NT, width), jnp.int32),
            V((K, 4 * NT, width), jnp.int32),
            V((K, 4 * NT, width), f32),
            V((4 * NT, width), f32),
            dma((tm_n,)), dma((tm_n,)), dma((tm_n,)), dma((tm_n,)),
            dma((3,)), dma((3, tm_n)),
            dma((n, 4)), dma((n, 4)),
            dma((n, half)), dma((n, half)),
            dma((5,)),
        ],
        compiler_params=pltpu.CompilerParams(
            collective_id=0, has_side_effects=True, vmem_limit_bytes=40 * 1024 * 1024),
    )(state, far_field, face_index, face_weight, mean_flow)


def skew_part(o, coef):
    half = len(o)
    quarter = half // 2

    def at(n):
        return o[n % half], -1.0 if (n // half) % 2 else 1.0

    res = []
    for n in range(half):
        total = None
        for m in range(1, quarter):
            (a, sa), (b, sb) = at(n - m), at(n + m)
            term = (coef[m] * sa) * (a - b if sa == sb else a + b)
            total = term if total is None else total + term
        a, sa = at(n - quarter)
        term = (coef[quarter] * sa) * a
        res.append(term if total is None else total + term)
    return res


def cyclic_part(e, coef):
    half = len(e)
    res = []
    for n in range(half):
        total = None
        for m in range(1, half // 2):
            term = coef[m] * (e[(n - m) % half] - e[(n + m) % half])
            total = term if total is None else total + term
        res.append(total)
    return res


def time_term_split(q, even, odd):
    half = len(q) // 2
    quarter = half // 2
    e = [q[n] + q[n + half] for n in range(half)]
    o = [q[n] - q[n + half] for n in range(half)]
    ee = [e[n] + e[n + quarter] for n in range(quarter)]
    eo = [e[n] - e[n + quarter] for n in range(quarter)]
    low = [0.0] + [0.5 * (even[m] - even[quarter - m]) for m in range(1, quarter)]
    high = [0.0] + [0.5 * (even[m] + even[quarter - m]) for m in range(1, quarter)]
    cyc = cyclic_part(ee, low)
    skw = skew_part(eo, high)
    ev = [cyc[n] + skw[n] for n in range(quarter)] + [cyc[n] - skw[n] for n in range(quarter)]
    od = skew_part(o, odd)
    return [ev[n] + od[n] for n in range(half)] + [ev[n] - od[n] for n in range(half)]


def ring_kernel(dims, state, far, fidx, fw, mf, out, q, tt, dd, ff, wts, fi, lane_ix, blk_ix, ww, gg, fo, mfs,
                info, in_s, in_r, dup_s, dup_r, out_s, out_r, p_s, p_r, h_s, h_r, loc):
    tm_n, half, L, R, K = dims
    NT = tm_n * L
    G = tm_n * half
    Z = tm_n // 2
    cycle = half * 128
    nsec = len(SECTION_FACTORS)
    reach = 2 * nsec
    groups = 4 * NT // 8
    me = lax.axis_index("tm")
    blk = lax.axis_index("block")
    side = lax.div(blk, half)
    place = lax.rem(blk, half)

    def slab(t, b, sd):
        z = lax.div(t, 2)
        c = lax.rem(t, 2)
        zo = jnp.where(sd == 0, z, Z - 1 - z)
        return 4 * zo + jnp.where(lax.rem(b + zo, 2) == 0, c, 3 - c)

    def owner(g, sd):
        zo = g // 4 if isinstance(g, int) else lax.div(g, 4)
        k = g % 4 if isinstance(g, int) else lax.rem(g, 4)
        xo = jnp.where(k >= 2, 1, 0)
        c = jnp.where(k >= 2, 3 - k, k)
        b = lax.rem(xo + zo, 2)
        return 2 * jnp.where(sd == 0, zo, Z - 1 - zo) + c, b

    def device(g, sd):
        t, b = owner(g, sd)
        return {"tm": t, "block": sd * half + b}

    g = slab(me, place, side)
    here = me * half + place
    seam = g == G - 1
    mixes = seam & (side == 0)
    ends = seam & (side == 1)
    mix_dev = device(G - 1, 0)
    end_dev = device(G - 1, 1)
    dup_list = [4 * z + 3 for z in range(1, Z - 1)]

    def is_dup(x):
        hit = x < -1
        for d in dup_list:
            hit = hit | (x == d)
        return hit

    takes_dup = is_dup(g)
    feeds_prev = jnp.logical_not(is_dup(g - 1))
    prev_side = jnp.where(g == 0, 1 - side, side)
    prev_dev = device(lax.rem(g + G - 1, G), prev_side)
    next_side = jnp.where(seam, 1 - side, side)

    def peer(t):
        return lax.rem(here + 1 + t, G)

    def dev(j, sd):
        return {"tm": lax.div(j, half), "block": sd * half + lax.rem(j, half)}

    def slab_of(j):
        return slab(lax.div(j, half), lax.rem(j, half), side)

    def lev(t):
        return pl.ds(t * L, L)

    def rc(src, dst, ss, rs, to):
        return pltpu.make_async_remote_copy(src_ref=src, dst_ref=dst, send_sem=ss, recv_sem=rs,
                                            device_id=to, device_id_type=MESH)

    def gather_of(n, whole=False):
        return q[0].at[:, pl.ds(0, NT if whole else NT - L // half), :, pl.ds(0, n)]

    def received(view, sem):
        rc(view, view, p_s.at[0], sem, end_dev).wait_recv()

    def sent(view, sem):
        rc(view, view, sem, p_r.at[0], end_dev).wait_send()

    z = lax.div(me, 2)

    def near(j):
        return jnp.abs(lax.div(lax.div(j, half), 2) - z) <= 1

    partner = {"block": (1 - side) * half + place}
    bar = pltpu.get_barrier_semaphore()

    @pl.loop(0, G - 1)
    def _(t):
        @pl.when(near(peer(t)))
        def _():
            pl.semaphore_signal(bar, inc=1, device_id=dev(peer(t), side), device_id_type=MESH)

    pl.semaphore_signal(bar, inc=1, device_id=partner, device_id_type=MESH)

    own = pltpu.make_async_copy(state.at[:, :, pl.ds(pl.multiple_of(g * R, R), R)],
                                q[0].at[place, lev(me), :, pl.ds(0, R)], loc.at[0])
    own.start()
    own_mf = pltpu.make_async_copy(mf, mfs, loc.at[4])
    own_mf.start()

    first = FIRST_ROWS
    ahead = ((0, first - 8), (first - 8, reach + 8 - first), (0, reach))

    def ahead_rows(d, k):
        lo, n = ahead[k]
        return state.at[:, :, pl.ds((d + 1) * R + lo, n)]

    def ahead_spot(j, k):
        lo, n = ahead[k]
        return q[0].at[lax.rem(j, half), lev(lax.div(j, half)), :, pl.ds(R + lo, n)]

    def dup_copy(i, k, j):
        return rc(ahead_rows(dup_list[i], k), ahead_spot(j, k), dup_s.at[i, k], dup_r.at[k],
                  device(dup_list[i], side))

    def own_dup(i):
        return pltpu.make_async_copy(ahead_rows(dup_list[i], 2), ahead_spot(here, 2), loc.at[5])

    def send_dup(k):
        for i, d in enumerate(dup_list):
            @pl.when(g != d)
            def _():
                dup_copy(i, k, here).start()

    for i, d in enumerate(dup_list):
        @pl.when(g == d)
        def _():
            own_dup(i).start()

    pl.semaphore_wait(bar, 2 * half * (1 + jnp.where(z > 0, 1, 0) + jnp.where(z < Z - 1, 1, 0)))

    parts = ((0, first), (first, R - first))

    def in_copy(i, j, src):
        lo, n = parts[i]
        return rc(state.at[:, :, pl.ds(slab_of(j) * R + lo, n)],
                  q[0].at[lax.rem(src, half), lev(lax.div(src, half)), :, pl.ds(lo, n)],
                  in_s.at[i], in_r.at[i], dev(j, side))

    def send_in(i, which=None):
        @pl.loop(0, G - 1)
        def _(t):
            if which is None:
                in_copy(i, peer(t), here).start()
            else:
                @pl.when(near(peer(t)) == which)
                def _():
                    in_copy(i, peer(t), here).start()

    send_in(0, True)

    for r in range(1, Z - 1):
        @pl.when((z >= 1) & (z + r <= Z - 1))
        def _():
            pl.semaphore_signal(info.at[r], inc=1, device_id={"tm": me - 2}, device_id_type=MESH)

        @pl.when((z <= Z - 2) & (z - r >= 0))
        def _():
            pl.semaphore_signal(info.at[Z - 2 + r], inc=1, device_id={"tm": me + 2}, device_id_type=MESH)

        @pl.when(z + r + 1 <= Z - 1)
        def _():
            pl.semaphore_wait(info.at[r], 1)

        @pl.when(z - r - 1 >= 0)
        def _():
            pl.semaphore_wait(info.at[Z - 2 + r], 1)

    send_in(0, False)
    pl.semaphore_signal(info.at[0], inc=1, device_id=partner, device_id_type=MESH)
    pl.semaphore_wait(info.at[0], 1)

    def far_copy(j, sd):
        return rc(far, ff.at[sd, lax.rem(j, half), lev(lax.div(j, half))], p_s.at[0], p_r.at[0], end_dev)

    def wt_copy(j, sd):
        return rc(fw, wts.at[sd, lax.rem(j, half), lev(lax.div(j, half))], p_s.at[1], p_r.at[1], mix_dev)

    def ix_copy(j, sd):
        return rc(fidx, fi.at[sd, lax.rem(j, half), lax.div(j, half)], p_s.at[2], p_r.at[2], mix_dev)

    own_far = pltpu.make_async_copy(far, ff.at[side, place, lev(me)], loc.at[1])
    own_wt = pltpu.make_async_copy(fw, wts.at[side, place, lev(me)], loc.at[2])
    own_ix = pltpu.make_async_copy(fidx, fi.at[side, place, me], loc.at[3])

    @pl.when(ends)
    def _():
        own_far.start()

    @pl.when(jnp.logical_not(ends))
    def _():
        far_copy(here, side).start()

    @pl.when(mixes)
    def _():
        own_wt.start()
        own_ix.start()

    @pl.when(jnp.logical_not(mixes))
    def _():
        wt_copy(here, side).start()
        ix_copy(here, side).start()

    send_dup(0)
    send_in(1, True)
    send_in(1, False)
    send_dup(1)

    lane = lax.broadcasted_iota(jnp.int32, (8, 128), 1)
    sub = lax.broadcasted_iota(jnp.int32, (8, 128), 0)
    first_lane, last_lane = lane == 0, lane == 127

    @pl.when(ends)
    def _():
        own_far.wait()

        received(q[0].at[:, pl.ds(0, L // half), :, pl.ds(0, 2 * G - 1)], p_r.at[0])

        for k in range(2):
            for b in range(half):
                @pl.loop(0, NT)
                def _(l):
                    for v in range(4):
                        gg[k, b, pl.ds(4 * l + v, 1)] = ff[1 - k, b, l, pl.ds(v, 1)]

    @pl.when(mixes)
    def _():
        own_wt.wait()
        own_ix.wait()

        received(q[0].at[:, pl.ds(0, L // half), :, pl.ds(0, 2 * G - 1)], p_r.at[1])
        received(q[0].at[0, 0, pl.ds(0, L), pl.ds(0, 2 * G - 1)], p_r.at[2])

        for r in range(2):
            for b in range(half):
                @pl.loop(0, NT // 2)
                def _(m):
                    def ix(l):
                        return jnp.broadcast_to(fi[r, b, lax.div(l, L), pl.ds(lax.rem(l, L), 1)], (8, 128))

                    def wt(l, k):
                        return jnp.broadcast_to(wts[r, b, l, pl.ds(k, 1)], (8, 128))

                    start = jnp.where(sub < 4, ix(2 * m), ix(2 * m + 1))
                    at = pl.ds(8 * m, 8)
                    for k in range(K):
                        src = start + k
                        src = jnp.where(src >= cycle, src - cycle, src)
                        lane_ix[r, k, b, at] = jnp.bitwise_and(src, 127)
                        blk_ix[r, k, b, at] = lax.shift_right_logical(src, 7)
                        ww[r, k, b, at] = jnp.where(sub < 4, wt(2 * m, k), wt(2 * m + 1, k))

    own_mf.wait()

    def speeds(sd):
        return jnp.where(sd == 0, mfs[0, 0], mfs[1, 0]), jnp.where(sd == 0, mfs[0, 1], mfs[1, 1])

    own_speed = speeds(side)
    next_speed = speeds(next_side)

    def feed(k):
        lo, n = ahead[k]
        return rc(q[0].at[:, :, :, pl.ds(lo, n)], q[0].at[:, :, :, pl.ds(R + lo, n)], h_s.at[k], h_r.at[k], prev_dev)

    def wait_ahead(k):
        @pl.when(takes_dup)
        def _():
            received(gather_of(ahead[k][1]), dup_r.at[k])

        @pl.when(jnp.logical_not(takes_dup))
        def _():
            feed(k).wait_recv()

    span = range(half)

    def window(s, w, lo, hi):
        old, new = q[s - 1], q[s]
        c = SECTION_FACTORS[s - 1]
        even, odd = split_coefficients(NT, -OMEGA * c)
        at = pl.ds(w, 8)
        up_row, dn_row = lo <= R - 1 < hi, lo <= R < hi
        hh = 0.5 * c
        near = DISSIPATION * c

        def weights(uv):
            return near - hh * uv[0], near + hh * uv[0], near - hh * uv[1], near + hh * uv[1]

        cu, cd, cr, cl = weights(own_speed)
        if hi > R:
            beyond = sub >= R - w
            cu, cd, cr, cl = [jnp.where(beyond, n, o) for n, o in zip(weights(next_speed), (cu, cd, cr, cl))]
        up_at = sub == jnp.where(seam, R - 1 - w, 8)
        dn_at = sub == jnp.where(seam, R - w, 8)

        @pl.loop(0, 4)
        def _(v):
            for b in span:
                xs = [old[b, l, v, at] for l in range(NT)]
                terms = time_term_split(xs, even, odd)
                for l in range(NT):
                    tt[b, l, v] = (q[0][b, l, v, at] + terms[l]) - (4.0 * DISSIPATION * c) * xs[l]
            for l in range(NT):
                x = [old[b, l, v, at] for b in span]
                rr = [pltpu.roll(x[b], 127, 1) for b in span]
                rl = [pltpu.roll(x[b], 1, 1) for b in span]
                for b in span:
                    up = old[b, l, v, pl.ds(w + 1, 8)]
                    dn = old[b, l, v, pl.ds(w - 1, 8)]
                    row = pl.ds(4 * l + v, 1)
                    if up_row:
                        up = jnp.where(up_at, jnp.broadcast_to(gg[0, b, row], (8, 128)), up)
                    if dn_row:
                        dn = jnp.where(dn_at, jnp.broadcast_to(gg[1, b, row], (8, 128)), dn)
                    right = jnp.where(last_lane, rr[(b + 1) % half], rr[b])
                    left = jnp.where(first_lane, rl[(b - 1) % half], rl[b])
                    tt[b, l, v] = (tt[b, l, v] + (cu * up + cd * dn)) + (cr * right + cl * left)
                    dd[0, b, l, v] = hh * (up - dn)
                    dd[1, b, l, v] = hh * (right - left)

        @pl.loop(0, NT // 4)
        def _(i):
            for j in range(4):
                l = 4 * i + j
                for b in span:
                    cross = dd[0, b, l, 1] + dd[1, b, l, 2]
                    drop = [cross, dd[0, b, l, 3], dd[1, b, l, 3], cross]
                    for v in range(4):
                        value = tt[b, l, v] - drop[v]
                        new[b, l, v, pl.ds(lo, hi - lo)] = value[lo - w:hi - w]
                        for k, hit in enumerate((up_row, dn_row)):
                            if hit and s < nsec:
                                row = R - 1 + k - w
                                fo[k, b, pl.ds(4 * l + v, 1)] = value[row:row + 1]

    own.wait()

    received(gather_of(parts[0][1]), in_r.at[0])

    @pl.when(feeds_prev)
    def _():
        feed(0).start()
        feed(1).start()

    early = first - reach
    following = lax.rem(g + 1, G)
    takes_own = jnp.logical_not(seam)
    turn = nsec + early + 8
    spans = [(nsec, early), (nsec + early, 8), (turn, R - turn), (R, nsec)]
    spans = [(lo, n) for lo, n in spans if n > 0]
    last = len(spans) - 1
    inner = 1 if early else 0

    def result(i, j):
        lo, n = spans[i]
        return q[nsec].at[lax.rem(j, half), lev(lax.div(j, half)), :, pl.ds(lo, n)]

    def spot(i, gs):
        lo, n = spans[i]
        return out.at[:, :, pl.ds(gs * R + (lo if i < last else 0), n)]

    def out_copy(i, j, gs):
        return rc(result(i, j), spot(i, gs), out_s.at[i], out_r.at[i], dev(j, side if i < last else next_side))

    def own_out(i, gs):
        return pltpu.make_async_copy(result(i, here), spot(i, gs), loc.at[6 + i])

    def send_out(i):
        @pl.loop(0, G - 1)
        def _(t):
            out_copy(i, peer(lax.rem(t + 3, G - 1)), g).start()

        own_out(i, g).start()

    for s in range(1, nsec + 1):
        lo, hi = s, first - s
        if hi - lo > 8:
            window(s, lo, lo, lo + 8)
            window(s, hi - 8, lo + 8, hi)
        elif hi > lo:
            window(s, min(lo, first - 8 - (s == 1)), lo, hi)
    if early:
        send_out(0)

    received(gather_of(parts[1][1]), in_r.at[1])

    for i, d in enumerate(dup_list):
        @pl.when(g == d)
        def _():
            own_dup(i).wait()

    wait_ahead(0)

    @pl.when(mixes)
    def _():
        @pl.loop(0, NT)
        def _(l):
            for b in range(half):
                for v in range(4):
                    for k in range(2):
                        fo[k, b, pl.ds(4 * l + v, 1)] = q[0][b, l, v, pl.ds(R - 1 + k, 1)]

    def mix():
        @pl.when(mixes)
        def _():
            @pl.loop(0, groups)
            def _(m):
                at = pl.ds(pl.multiple_of(8 * m, 8), 8)
                for r in range(2):
                    for b in range(half):
                        total = jnp.zeros((8, 128), jnp.float32)
                        for k in range(K):
                            picked = jnp.zeros((8, 128), jnp.float32)
                            for h in range(half):
                                got = jnp.take_along_axis(fo[1 - r, h, at], lane_ix[r, k, b, at], axis=1)
                                picked = jnp.where(blk_ix[r, k, b, at] == h, got, picked)
                            total = total + ww[r, k, b, at] * picked
                        gg[r, b, at] = total

    for s in range(1, nsec + 1):
        if s <= first - 8:
            mix()
        window(s, first - s, first - s, first - s + 8)
    send_out(inner)
    wait_ahead(1)

    for s in range(1, nsec + 1):
        if s > first - 8:
            mix()
        window(s, R + 2 - s, first + 8 - s, R + reach - s)

    @pl.loop(0, G - 1)
    def _(t):
        for i in range(inner + 1, last):
            out_copy(i, peer(t), g).start()
        out_copy(last, peer(t), following).start()

    for i in range(inner + 1, last):
        own_out(i, g).start()

    @pl.when(takes_own)
    def _():
        own_out(last, following).start()

    @pl.when(seam)
    def _():
        out_copy(last, here, following).start()

    for i in range(2):
        sent(gather_of(parts[i][1]), in_s.at[i])

    for i, d in enumerate(dup_list):
        @pl.when(g != d)
        def _():
            for k in range(2):
                dup_copy(i, k, here).wait_send()

    @pl.when(feeds_prev)
    def _():
        feed(0).wait_send()
        feed(1).wait_send()

    @pl.when(jnp.logical_not(ends))
    def _():
        far_copy(here, side).wait_send()

    @pl.when(jnp.logical_not(mixes))
    def _():
        wt_copy(here, side).wait_send()
        ix_copy(here, side).wait_send()

    for i in range(last):
        own_out(i, g).wait()
        sent(gather_of(spans[i][1]), out_s.at[i])
        received(gather_of(spans[i][1]), out_r.at[i])

    @pl.when(takes_own)
    def _():
        own_out(last, following).wait()
        sent(gather_of(nsec), out_s.at[last])
        received(gather_of(nsec), out_r.at[last])

    @pl.when(seam)
    def _():
        sent(gather_of(nsec, True), out_s.at[last])
        received(gather_of(nsec, True), out_r.at[last])


def ring_shards(dims, state, far_field, face_index, face_weight, mean_flow):
    tm_n, half = dims
    L, _, rows, width = state.shape
    K = face_weight.shape[1]
    G = tm_n * half
    R = rows // G
    NT = L * tm_n
    n = len(SECTION_FACTORS)
    f32 = jnp.float32
    hbm = pl.BlockSpec(memory_space=pl.ANY)
    dma = pltpu.SemaphoreType.DMA
    V = pltpu.VMEM
    args = [pltpu.with_memory_space_constraint(a, pltpu.HBM)
            for a in (state, far_field, face_index, face_weight, mean_flow)]
    return pl.pallas_call(
        functools.partial(ring_kernel, (tm_n, half, L, R, K)),
        out_shape=jax.ShapeDtypeStruct(state.shape, f32),
        in_specs=[hbm] * 5,
        out_specs=hbm,
        scratch_shapes=[
            [V((half, NT, 4, R + 16, width), f32) for _ in range(n + 1)],
            V((half, NT, 4, 8, width), f32),
            V((2, half, NT, 4, 8, width), f32),
            V((2, half, NT, 4, width), f32),
            V((2, half, NT, K, width), f32),
            V((2, half, tm_n, L, width), jnp.int32),
            V((2, K, half, 4 * NT, width), jnp.int32),
            V((2, K, half, 4 * NT, width), jnp.int32),
            V((2, K, half, 4 * NT, width), f32),
            V((2, half, 4 * NT, width), f32),
            V((2, half, 4 * NT, width), f32),
            pltpu.SMEM((2, 2), f32),
            pltpu.SemaphoreType.REGULAR((tm_n - 3,)),
            dma((2,)), dma((2,)),
            dma((tm_n // 2 - 2, 2)), dma((2,)),
            dma((4,)), dma((4,)),
            dma((3,)), dma((3,)),
            dma((2,)), dma((2,)),
            dma((10,)),
        ],
        compiler_params=pltpu.CompilerParams(
            collective_id=0, has_side_effects=True, vmem_limit_bytes=48 * 1024 * 1024),
    )(*args)


def solution(mesh):
    dims = (mesh.shape["tm"], mesh.shape["block"] // 2)
    in_specs = (
        P("tm", None, None, "block"),
        P("tm", None, "block"),
        P("tm", "block"),
        P("tm", None, "block"),
        P(),
    )
    out_specs = P("tm", None, None, "block")

    def body(state, *rest):
        tm_n, half = dims
        fits = (half == 2 and tm_n in (6, 8) and state.shape[0] % 2 == 0 and state.shape[0] * tm_n % 8 == 0
                and rest[2].shape[1] == 4 and state.shape[2] == 16 * tm_n * half and state.shape[3] == 128)
        return (ring_shards if fits else shards)(dims, state, *rest)

    return jax.shard_map(body, mesh=mesh, in_specs=in_specs, out_specs=out_specs, check_vma=False)
```
